32 devices in a mesh: gx: 4 (over z), gy: 4 (over y, core), gz: 2 (over x).
Axes of the slice: x: 2, y: 2, z: 4, core: 2. Of those that a mesh axis runs over, the one named last changes fastest.
Arguments:
- right_side: float32 [128, 128, 256], P('gx', 'gy', 'gz'), may hold values from -8 to 8
- guess: float32 [128, 128, 256], P('gx', 'gy', 'gz'), may hold values from -4 to 4
Outputs:
- solution_field: float32 [128, 128, 256], P('gx', 'gy', 'gz')
- residual: float32 [128, 128, 256], P('gx', 'gy', 'gz')
The draws below stay inside these ranges and needn't reach their ends.
All inputs are finite; a program needn't handle non-finite values.
Results may differ from the reference program's by a relative error of at most 0.0001.
Values sent between devices are 32-bit elements; how exact they have to be, the bound alone decides.
A program may use at most 128 MiB of HBM per device.

```python
import jax
import jax.numpy as jnp

LEVELS = 6
SWEEPS = 4
STEPS = 2
NX = 128
NY = 128
NZ = 256


def level_of(stream_key, dims, cuts, low, largest):
    level = 1.0
    for position, shards_of in cuts:
        heights = jax.random.uniform(jax.random.fold_in(jax.random.fold_in(stream_key, 6), position), (shards_of,), jnp.float32, low / len(cuts), largest / len(cuts))
        level = level * jnp.repeat(jnp.exp(heights), dims[position] // shards_of).reshape((-1,) + (1,) * (len(dims) - 1 - position))
    return level


def centred(own_key, shape, width, limit, pieces=(), kind=jnp.bfloat16):
    drawn = width * jax.random.normal(own_key, shape, jnp.float32)
    if pieces:
        drawn = drawn * level_of(own_key, shape, pieces, -0.22, 0.18)
    return jnp.clip(drawn, -limit, limit).astype(kind)


def setup_inputs(seed: int = 0) -> dict:
    keys = jax.random.split(jax.random.key(seed), 3)
    return {
        "right_side": centred(keys[0], (NX, NY, NZ), 1.0, 8.0, ((0, 4), (1, 4), (2, 2)), jnp.float32),
        "guess": centred(keys[1], (NX, NY, NZ), 0.5, 4.0, ((0, 4), (1, 4), (2, 2)), jnp.float32),
    }


damping = 2.0 / 3.0


def stencil(field):
    padded = jnp.pad(field, 1)
    beside = padded[2:, 1:-1, 1:-1] + padded[:-2, 1:-1, 1:-1]
    beside = beside + padded[1:-1, 2:, 1:-1] + padded[1:-1, :-2, 1:-1]
    beside = beside + padded[1:-1, 1:-1, 2:] + padded[1:-1, 1:-1, :-2]
    return 6.0 * field - beside


def restrict(field):
    first, second, third = field.shape
    blocks = field.reshape(first // 2, 2, second // 2, 2, third // 2, 2)
    return jnp.mean(blocks, axis=(1, 3, 5))


def prolong(field):
    first, second, third = field.shape
    spread = jnp.broadcast_to(field[:, None, :, None, :, None], (first, 2, second, 2, third, 2))
    return spread.reshape(first * 2, second * 2, third * 2)


def smooth(rhs, level_index):
    scaling = 0.25 ** level_index
    diagonal_value = 6.0 * scaling
    approx = damping * rhs / diagonal_value
    for sweep_index in range(SWEEPS - 1):
        approx = approx + damping * (rhs - scaling * stencil(approx)) / diagonal_value
    return approx


def precondition(residual):
    chain = [residual]
    for level_index in range(1, LEVELS):
        chain.append(restrict(chain[-1]))
    correction = smooth(chain[LEVELS - 1], LEVELS - 1)
    for level_index in range(LEVELS - 2, -1, -1):
        correction = prolong(correction) + smooth(chain[level_index], level_index)
    return correction


def reference(right_side, guess):
    solution_field = guess
    residual = right_side - stencil(guess)
    for step_index in range(STEPS):
        direction = precondition(residual)
        image = stencil(direction)
        alpha = jnp.sum(residual * direction) / jnp.sum(direction * image)
        solution_field = solution_field + alpha * direction
        residual = residual - alpha * image
    return solution_field, residual
```

```python
import functools

import jax
import jax.numpy as jnp
from jax import lax
from jax.experimental import pallas as pl
from jax.experimental.pallas import tpu as pltpu
from jax.sharding import PartitionSpec as P

LEVELS = 6
SWEEPS = 4
STEPS = 2
HALOED = 3
AXES = ("gx", "gy", "gz")
LANES = 128
TOP = 8
DEPTH = SWEEPS
SPAN = 8 * DEPTH
PER = LANES // SPAN
MESH = pl.DeviceIdType.MESH
HIGH = lax.Precision.HIGHEST
AROUND = [(a, b) for a in (-1, 0, 1) for b in (-1, 0, 1) if (a, b) != (0, 0)]
FACES = [(d, s) for d in range(3) for s in (-1, 1)]


def iota(shape, dim):
    return lax.broadcasted_iota(jnp.int32, shape, dim)


def lanes_dot(x, matrix):
    first, second, _ = x.shape
    if second % 8 == 0:
        out = jnp.dot(x.reshape(first * second, LANES), matrix, precision=HIGH, preferred_element_type=jnp.float32)
        return out.reshape(first, second, LANES)
    planes = [jnp.dot(x[i], matrix, precision=HIGH, preferred_element_type=jnp.float32)[None] for i in range(first)]
    return jnp.concatenate(planes, axis=0)


def halve_matrix(width, start):
    source, target = iota((LANES, LANES), 0), iota((LANES, LANES), 1) - start
    keep = (target >= 0) & (target < width) & ((source == 2 * target) | (source == 2 * target + 1))
    return jnp.where(keep, 0.125, 0.0)


def double_matrix(width, start):
    source, target = iota((LANES, LANES), 0) - start, iota((LANES, LANES), 1)
    keep = (source >= 0) & (source < width) & ((target == 2 * source) | (target == 2 * source + 1))
    return jnp.where(keep, 1.0, 0.0)


def wrapped(lane):
    return jnp.where(lane >= LANES - DEPTH, lane - LANES, lane)


def double_around(coarse_start, coarse_total, fine_width):
    source, target = iota((LANES, LANES), 0), wrapped(iota((LANES, LANES), 1))
    at = (target >> 1) + coarse_start
    if coarse_total is None:
        at = at & (LANES - 1)
        keep = (source == at) & (target < fine_width + DEPTH)
    else:
        keep = (source == at) & (target < fine_width + DEPTH) & (source < coarse_total)
    return jnp.where(keep, 1.0, 0.0)


def ends_matrix(width):
    source, target = iota((LANES, LANES), 0), iota((LANES, LANES), 1)
    keep = ((target == 0) & (source == LANES - 1)) | ((target == LANES - 1) & (source == width))
    return jnp.where(keep, 1.0, 0.0)


def plane_groups(shape, width):
    return max(1, LANES // width // shape[1])


def own_group(shape, width):
    group = iota(shape, 0) % plane_groups(shape, width) * shape[1] + iota(shape, 1)
    return iota(shape, 2) // width == group


def tile_matrix(width):
    source, target = iota((LANES, LANES), 0), iota((LANES, LANES), 1) % width
    return jnp.where((source == 2 * target) | (source == 2 * target + 1), 0.125, 0.0)


def gather_matrix(width, start):
    source, target = iota((LANES, LANES), 0) % width, iota((LANES, LANES), 1) - start
    return jnp.where(source == target, 1.0, 0.0)


def turn(x, shift):
    shift = shift % LANES
    return pltpu.roll(x, shift, x.ndim - 1) if shift else x


def kernel(sizes, block, b_hbm, x_hbm, sol_ref, res_ref, *rest):
    (ux, bb, g0, g1, g2, gs, f0a, f0b, f1a, f1b, f2a, f2b, fsa, fsb, z0, z1, wv, sc, sd, pd, pe,
     m0, m1, m2, ms, wref, wide, fold, spread, ze, zi, zs, zr, cs, cr, ds, dr,
     isem, xsend, xrecv, zsend, zrecv, msend, mrecv, fsend, frecv, csend, crecv, dsend, drecv) = rest
    nx, ny, nz = sizes
    n = nx * ny * nz
    at = tuple(lax.axis_index(a) for a in AXES)
    me = (at[0] * ny + at[1]) * nz + at[2]
    dims = [tuple(d >> l for d in block) for l in range(LEVELS)]
    X, Y, Z = block
    fields = (g0, g1, g2)
    ping = ((f0a, f0b), (f1a, f1b), (f2a, f2b))
    masks = (m0, m1, m2)
    groups = X // PER
    lower = [at[d] > 0 for d in range(3)]
    upper = [at[d] < sizes[d] - 1 for d in range(3)]
    inlow = [jnp.where(c, 1.0, 0.0) for c in lower]
    inup = [jnp.where(c, 1.0, 0.0) for c in upper]

    load_x = pltpu.make_async_copy(x_hbm, ux.at[1:X + 1, TOP:TOP + Y], isem.at[0])
    load_b = pltpu.make_async_copy(b_hbm, bb, isem.at[1])
    load_x.start()
    load_b.start()

    def others():
        moved = [[lax.rem(at[d] + k, sizes[d]) if k else at[d] for k in range(sizes[d])] for d in range(3)]
        return [(a, b, c) for a in moved[0] for b in moved[1] for c in moved[2]][1:]

    def clear(ref, lead, planes, depth, rows, own):
        zero = jnp.float32(0)
        for i in lead:
            head = (i,) if i is not None else ()
            for a, b in ((0, depth), (planes - depth, planes)):
                ref[head + (slice(a, b),)] = jnp.full((b - a,) + ref.shape[-2:], zero)
            for a, b in ((0, TOP), (TOP + own, rows)):
                ref[head + (slice(depth, planes - depth), slice(a, b))] = jnp.full((planes - 2 * depth, b - a, LANES), zero)

    clear(ux, (None,), X + 2, 1, Y + 2 * TOP, Y)
    for l in range(HALOED):
        clear(fields[l], range(STEPS), dims[l][0] + 2 * DEPTH, DEPTH, dims[l][1] + 2 * TOP, dims[l][1])
    clear(gs, range(STEPS), groups + 2, 1, Y + 2 * TOP, Y)
    zi[...] = jnp.zeros_like(zi)
    zr[...] = jnp.zeros_like(zr)

    barrier = pltpu.get_barrier_semaphore()
    for target in others():
        pl.semaphore_signal(barrier, inc=1, device_id=target, device_id_type=MESH)

    for ref in (f0a, f0b, f1a, f1b, f2a, f2b, fsa, fsb):
        ref[...] = jnp.zeros_like(ref)
    wref[...] = jnp.zeros_like(wref)
    wide[...] = jnp.zeros_like(wide)

    def mask(rows, z, depth_z):
        y = iota((rows + 2 * DEPTH, LANES), 0) - DEPTH
        part = jnp.where(y < 0, inlow[1], jnp.where(y >= rows, inup[1], 1.0))
        return part * jnp.where(z < 0, inlow[2], jnp.where(z >= depth_z, inup[2], 1.0)) * (1.0 / 9.0)

    for l in range(HALOED):
        lane = iota((dims[l][1] + 2 * DEPTH, LANES), 1)
        masks[l][...] = mask(dims[l][1], lane if l == 0 else wrapped(lane), dims[l][2])
    lane = iota((Y + 2 * DEPTH, LANES), 1) % SPAN
    ms[...] = mask(Y, jnp.where(lane < SPAN // 2, lane + Z - SPAN // 4, lane - 3 * SPAN // 4), Z)

    def face_copies():
        out = []
        for i, (d, s) in enumerate(FACES):
            target = list(at)
            target[d] = at[d] + s
            if d == 0:
                src, dst = (X, 0) if s > 0 else (1, X + 1)
                src, dst = ux.at[src:src + 1, TOP:TOP + Y], ux.at[dst:dst + 1, TOP:TOP + Y]
            elif d == 1:
                src, dst = (TOP + Y - 1, TOP - 1) if s > 0 else (TOP, TOP + Y)
                src, dst = ux.at[1:X + 1, src:src + 1], ux.at[1:X + 1, dst:dst + 1]
            else:
                src, dst = ze, zi.at[0 if s > 0 else 1]
            copy = pltpu.make_async_remote_copy(
                src_ref=src, dst_ref=dst, send_sem=xsend.at[i], recv_sem=xrecv.at[i],
                device_id=tuple(target), device_id_type=MESH,
            )
            out.append((copy, upper[d] if s > 0 else lower[d], lower[d] if s > 0 else upper[d]))
        return out

    def z_copies(k):
        out = []
        for side in (0, 1):
            copy = pltpu.make_async_remote_copy(
                src_ref=zs.at[k, side], dst_ref=zr.at[k, side], send_sem=zsend.at[k, side], recv_sem=zrecv.at[k, side],
                device_id=(at[0], at[1], at[2] + (1 if side else -1)), device_id_type=MESH,
            )
            out.append((copy, upper[2] if side else lower[2], lower[2] if side else upper[2]))
        return out

    def span(step, depth, start, own, other):
        if step > 0:
            return (start + own - depth, depth), (start - depth, depth)
        if step < 0:
            return (start, depth), (start + own, depth)
        return (start, own), (start, own)

    def around_copies(ref, k, depth, planes, rows, ssem, rsem):
        out = []
        for i, (dx, dy) in enumerate(AROUND):
            (sx, lx), (tx, _) = span(dx, depth, depth, planes, None)
            (sy, ly), (ty, _) = span(dy, DEPTH, TOP, rows, None)
            copy = pltpu.make_async_remote_copy(
                src_ref=ref.at[k, sx:sx + lx, sy:sy + ly], dst_ref=ref.at[k, tx:tx + lx, ty:ty + ly],
                send_sem=ssem(i), recv_sem=rsem(i),
                device_id=(at[0] + dx, at[1] + dy, at[2]), device_id_type=MESH,
            )
            to, fro = None, None
            for d, s in ((0, dx), (1, dy)):
                if s:
                    a, b = (upper[d], lower[d]) if s > 0 else (lower[d], upper[d])
                    to = a if to is None else jnp.logical_and(to, a)
                    fro = b if fro is None else jnp.logical_and(fro, b)
            out.append((copy, to, fro))
        return out

    def main_copies(k):
        return around_copies(g0, k, DEPTH, X, Y, lambda i: msend.at[k, i], lambda i: mrecv.at[k, i])

    def more_copies(k):
        out = [around_copies(gs, k, 1, groups, Y, lambda i: fsend.at[k, 0, i], lambda i: frecv.at[k, 0, i])]
        for l in range(1, HALOED):
            out.append(around_copies(
                fields[l], k, DEPTH, dims[l][0], dims[l][1],
                lambda i, l=l: fsend.at[k, l, i], lambda i, l=l: frecv.at[k, l, i]))
        return [[kind[i] for kind in out] for i in range(len(AROUND))]

    def start_all(copies):
        for copy, cond, _ in copies:
            pl.when(cond)(copy.start)

    def wait_all(copies):
        for copy, _, cond in copies:
            pl.when(cond)(copy.wait_recv)

    def sent_all(copies):
        for copy, cond, _ in copies:
            pl.when(cond)(copy.wait_send)

    def start_more(k):
        for same in more_copies(k):
            @pl.when(same[0][1])
            def _(same=same):
                for copy, _, _ in same:
                    copy.start()

    def wait_more(k):
        for same in more_copies(k):
            @pl.when(same[0][2])
            def _(same=same):
                for copy, _, _ in same:
                    copy.wait_recv()

    def sent_more(k):
        for same in more_copies(k):
            @pl.when(same[0][1])
            def _(same=same):
                for copy, _, _ in same:
                    copy.wait_send()

    def to_all(src, dst, s_sem, r_sem):
        for target in others():
            pltpu.make_async_remote_copy(
                src_ref=src, dst_ref=dst.at[me], send_sem=s_sem, recv_sem=r_sem,
                device_id=target, device_id_type=MESH,
            ).start()

    def all_done(dst, sem):
        part = dst.at[pl.ds(0, n - 1)]
        pltpu.make_async_copy(part, part, sem).wait()

    def fold_xy(field):
        A, B, _ = field.shape
        pairs = field.reshape(A // 2, 2, B, LANES)
        fold[0:A // 2, 0:B, :] = pairs[:, 0] + pairs[:, 1]
        return fold[0:A // 2, pl.ds(0, B // 2, 2), :] + fold[0:A // 2, pl.ds(1, B // 2, 2), :]

    def spread_y(field, into, first=0):
        A, B, _ = field.shape
        into[0:A, pl.ds(first, B, 2), :] = field
        into[0:A, pl.ds(first + 1, B, 2), :] = field

    def twice(field):
        A, B, _ = field.shape
        return jnp.broadcast_to(field[:, None], (A, 2, B, LANES)).reshape(2 * A, B, LANES)

    def own(ref, l, k=None):
        A, B, _ = dims[l]
        return ref[(k,) * (k is not None) + (slice(DEPTH, DEPTH + A), slice(TOP, TOP + B))]

    def beside(ref, a, c, low, rows):
        mid = ref[a:a + c, low:low + rows, :]
        total = ref[a - 1:a - 1 + c, low:low + rows, :] + ref[a + 1:a + 1 + c, low:low + rows, :]
        total = total + ref[a:a + c, low - 1:low - 1 + rows, :] + ref[a:a + c, low + 1:low + 1 + rows, :]
        return mid, total

    def sweep(l, src, rhs, dst, k):
        A, B, _ = dims[l]
        low, rows = TOP - DEPTH, B + 2 * DEPTH
        m = masks[l][...]
        parts = [(k, DEPTH - k, inlow[0])]
        parts += [(a, min(4, DEPTH + A - a), None) for a in range(DEPTH, DEPTH + A, 4)]
        parts += [(DEPTH + A, DEPTH - k, inup[0])]
        for a, c, flag in parts:
            mid, total = beside(src, a, c, low, rows)
            total = total + turn(mid, 1) + turn(mid, -1)
            scale = m if flag is None else m * flag
            dst[a:a + c, low:low + rows, :] = rhs[a:a + c, low:low + rows, :] + (3.0 * mid + total) * scale[None]

    def sweep_slab(src, rhs, dst):
        low, rows = TOP - DEPTH, Y + 2 * DEPTH
        lane = iota((rows, LANES), 1)
        m = ms[...]
        for g in range(groups + 2):
            mid = src[g, low:low + rows, :]
            total = src[g, low - 1:low - 1 + rows, :] + src[g, low + 1:low + 1 + rows, :]
            total = total + turn(mid, 1) + turn(mid, -1)
            before = mid if g == 0 else jnp.where(lane >= LANES - SPAN, src[g - 1, low:low + rows, :], mid)
            after = mid if g == groups + 1 else jnp.where(lane < SPAN, src[g + 1, low:low + rows, :], mid)
            total = total + turn(before, SPAN) + turn(after, -SPAN)
            scale = m * inlow[0] if g == 0 else m * inup[0] if g == groups + 1 else m
            dst[g, low:low + rows, :] = rhs[g, low:low + rows, :] + (3.0 * mid + total) * scale

    def smooth_whole(rhs, width, l):
        A, B, _ = rhs.shape
        lane = iota(rhs.shape, 2)
        e = rhs
        for _ in range(SWEEPS - 1):
            px, py = jnp.zeros((1, B, LANES), jnp.float32), jnp.zeros((A, 1, LANES), jnp.float32)
            total = jnp.concatenate([px, e[:-1]], axis=0) + jnp.concatenate([e[1:], px], axis=0)
            total = total + jnp.concatenate([py, e[:, :-1]], axis=1) + jnp.concatenate([e[:, 1:], py], axis=1)
            total = total + jnp.where(lane == 0, 0.0, turn(e, 1))
            total = total + jnp.where(lane == width - 1, 0.0, turn(e, -1))
            e = rhs + (3.0 * e + total) * (1.0 / 9.0)
        return e * (4.0 ** l / 9.0)

    half, quarter = SPAN // 2, SPAN // 4

    def pack_slab(k):
        lane = iota((Y, LANES), 1)
        line, spot = lane // SPAN, lane % SPAN
        low = high = jnp.zeros((Y, LANES), jnp.float32)
        for g in range(groups):
            both = jnp.zeros((Y, LANES), jnp.float32)
            for i in range(PER):
                field = g0[k, DEPTH + g * PER + i, TOP:TOP + Y, :]
                both = jnp.where((line == i) & (spot < half), turn(field, SPAN * i + quarter), both)
            gs[k, g + 1, TOP:TOP + Y, :] = jnp.where(
                spot < quarter, both, jnp.where(spot >= 3 * quarter, turn(both, half), 0.0))
            here = spot // DEPTH == g
            low = jnp.where(here, turn(both, DEPTH * g - quarter), low)
            high = jnp.where(here, turn(both, DEPTH * g - quarter + DEPTH), high)
        zs[k, 0, 0:Y, :] = low
        zs[k, 1, 0:Y, :] = high

    def pack_level(k, l, first):
        A, B, C = dims[l]
        lane = iota((B, LANES), 1)
        out = jnp.zeros((B, LANES), jnp.float32)
        for i in range(A):
            field = fields[l][k, DEPTH + i, TOP:TOP + B, :]
            out = jnp.where(lane // DEPTH == i, turn(field, DEPTH * i), out)
            out = jnp.where(lane // DEPTH == A + i, turn(field, DEPTH * (A + i) - C + DEPTH), out)
        for side in (0, 1):
            zs[k, side, first:first + B, :] = out

    def unpack_slab(k):
        spot = iota((Y, LANES), 1) % SPAN
        above, below = zr[k, 0, 0:Y, :], zr[k, 1, 0:Y, :]
        for g in range(groups):
            held = gs[k, g + 1, TOP:TOP + Y, :]
            held = jnp.where(spot // DEPTH == 2, turn(above, 2 * DEPTH - DEPTH * g), held)
            gs[k, g + 1, TOP:TOP + Y, :] = jnp.where(spot // DEPTH == 5, turn(below, 5 * DEPTH - DEPTH * g), held)

    def unpack_level(k, l, first):
        A, B, C = dims[l]
        lane = iota((B, LANES), 1)
        above, below = zr[k, 0, first:first + B, :], zr[k, 1, first:first + B, :]
        for i in range(A):
            held = fields[l][k, DEPTH + i, TOP:TOP + B, :]
            held = jnp.where(lane // DEPTH == C // DEPTH, turn(above, C - DEPTH * i), held)
            fields[l][k, DEPTH + i, TOP:TOP + B, :] = jnp.where(
                lane >= LANES - DEPTH, turn(below, -DEPTH - DEPTH * (A + i)), held)

    width = dims[HALOED][2]
    cx, cy, _ = dims[HALOED]
    starts = [0, Y, Y + dims[1][1]]
    packed = cx // plane_groups((cx, cy), width)

    def coarse(k):
        per = plane_groups((cx, cy), width)
        fine = None
        for c in range(nz):
            rows = []
            for i in range(nx):
                columns = []
                for j in range(ny):
                    part = cr[k, (i * ny + j) * nz + c, 0:packed][:, None]
                    part = jnp.broadcast_to(part, (cx // per, per, cy, LANES)).reshape(cx, cy, LANES)
                    columns.append(jnp.where(own_group((cx, cy, LANES), width), part, 0.0))
                rows.append(jnp.concatenate(columns, axis=1))
            spot = lanes_dot(jnp.concatenate(rows, axis=0), gather_matrix(width, c * width))
            fine = spot if fine is None else fine + spot
        chain = [fine]
        widths = [width * nz]
        for l in range(HALOED + 1, LEVELS):
            widths.append(widths[-1] // 2)
            chain.append(lanes_dot(fold_xy(chain[-1]), halve_matrix(widths[-1], 0)))
        whole = smooth_whole(chain[-1], widths[-1], LEVELS - 1)
        for l in range(LEVELS - 2, HALOED - 1, -1):
            i = l - HALOED
            spread_y(whole, spread)
            grown = spread[0:whole.shape[0], 0:2 * whole.shape[1], :]
            grown = twice(lanes_dot(grown, double_matrix(widths[i + 1], 0)))
            whole = grown + smooth_whole(chain[i], widths[i], l)
        wref[DEPTH // 2:DEPTH // 2 + nx * cx, :, :] = whole

    def precondition(k, z, extra):
        start_all(main_copies(k))
        pack_slab(k)
        for l in range(HALOED - 1):
            A, B, C = dims[l + 1]
            fields[l + 1][k, DEPTH:DEPTH + A, TOP:TOP + B, :] = lanes_dot(fold_xy(own(fields[l], l, k)), halve_matrix(C, 0))
            pack_level(k, l + 1, starts[l + 1])
        start_all(z_copies(k))
        mine = lanes_dot(fold_xy(own(fields[HALOED - 1], HALOED - 1, k)), tile_matrix(width))
        mine = jnp.where(own_group(mine.shape, width), mine, 0.0)
        mine = jnp.sum(mine.reshape(-1, plane_groups(mine.shape, width), *mine.shape[1:]), axis=1)
        mine = jnp.sum(mine, axis=1, keepdims=True)
        mine = jnp.concatenate([mine, extra], axis=0)
        cs[k] = mine
        cr[k, me] = mine
        to_all(cs.at[k], cr.at[k], csend.at[k], crecv.at[k])
        wait_all(z_copies(k))
        unpack_slab(k)
        for l in range(1, HALOED):
            unpack_level(k, l, starts[l])
        start_more(k)
        wait_all(main_copies(k))
        for s in range(1, SWEEPS):
            src = g0.at[k] if s == 1 else ping[0][s % 2]
            sweep(0, src, g0.at[k], ping[0][(s + 1) % 2], s)
        wait_more(k)
        for s in range(1, SWEEPS):
            src = gs.at[k] if s == 1 else (fsa, fsb)[s % 2]
            sweep_slab(src, gs.at[k], (fsa, fsb)[(s + 1) % 2])
            for l in range(1, HALOED):
                src = fields[l].at[k] if s == 1 else ping[l][s % 2]
                sweep(l, src, fields[l].at[k], ping[l][(s + 1) % 2], s)
        all_done(cr.at[k], crecv.at[k])
        coarse(k)
        last = SWEEPS % 2
        spread_y(wref[pl.ds(at[0] * cx, cx + DEPTH)], wide, DEPTH)
        part = wide[:, pl.ds(pl.multiple_of(at[1] * 2 * cy, 8), 2 * cy + 2 * DEPTH), :]
        part = lanes_dot(part, double_around(at[2] * width, width * nz, dims[HALOED - 1][2]))
        part = twice(part)[DEPTH - 1:DEPTH + dims[HALOED - 1][0] + 1]
        for l in range(HALOED - 1, 0, -1):
            A, B, C = dims[l]
            end = ping[l][last][DEPTH - 1:DEPTH + A + 1, TOP - DEPTH:TOP + B + DEPTH, :]
            full = end * (4.0 ** l / 9.0) + part
            if l > 1:
                spread_y(lanes_dot(full, double_around(0, None, dims[l - 1][2])), spread)
                part = twice(spread[0:A + 2, DEPTH:DEPTH + 2 * B + 2 * DEPTH, :])[1:2 * A + 3]
            else:
                spread_y(lanes_dot(full, double_matrix(C, 0)), pd)
                spread_y(lanes_dot(full, ends_matrix(C)), pe)
        low, rows = TOP - DEPTH, Y + 2 * DEPTH
        slab = (fsa, fsb)[last]
        spot = iota((rows, LANES), 1) % SPAN
        for g in range(groups + 2):
            s = slab[g, low:low + rows, :]
            sc[g] = jnp.where(spot < quarter, s, turn(s, -half))
            sd[g] = jnp.where(spot <= quarter, s, turn(s, quarter + 1 - (3 * quarter - 1)))
        lane = iota((rows, LANES), 1)
        near = (lane < DEPTH - 1) | (lane > LANES - DEPTH)
        end = ping[0][last]
        for p in range(DEPTH - 1, DEPTH + X + 1):
            g, i = p // PER, p % PER
            f = jnp.where(near, turn(sc[g], -quarter - SPAN * i), end[p, low:low + rows, :])
            z[p, low:low + rows, :] = f * (1.0 / 9.0) + pd[(p - DEPTH + 2) // 2, low:low + rows, :]

    def operator(z, p):
        lane = iota((Y, LANES), 1)
        mid, total = beside(z, p, 1, TOP, Y)
        mid, total = mid[0], total[0]
        g, i = p // PER, p % PER
        ghost = turn(sd[g, DEPTH:DEPTH + Y, :], LANES - 1 - quarter - SPAN * i) * (1.0 / 9.0)
        ghost = ghost + pe[(p - DEPTH + 2) // 2, TOP:TOP + Y, :]
        total = total + jnp.where(lane == 0, ghost, turn(mid, 1))
        total = total + jnp.where(lane == LANES - 1, ghost, turn(mid, -1))
        return mid, 6.0 * mid - total

    load_x.wait()
    lane = iota((Y, LANES), 1)
    out = jnp.zeros((Y, LANES), jnp.float32)
    for i in range(X):
        out = jnp.where(lane // 2 == i, turn(ux[1 + i, TOP:TOP + Y, :], 2 * i + 1), out)
    ze[...] = out
    pl.semaphore_wait(barrier, n - 1)
    start_all(face_copies())
    load_b.wait()
    wait_all(face_copies())
    ghosts = jnp.where(lane % 2 == 0, turn(zi[1], -1), turn(zi[0], 1))
    for i in range(X):
        mid, total = beside(ux, 1 + i, 1, TOP, Y)
        mid, total = mid[0], total[0]
        ghost = turn(ghosts, -2 * i - 1)
        total = total + jnp.where(lane == 0, ghost, turn(mid, 1))
        total = total + jnp.where(lane == LANES - 1, ghost, turn(mid, -1))
        g0[0, DEPTH + i, TOP:TOP + Y, :] = bb[i] - (6.0 * mid - total)

    def sums_of(a, b):
        return jnp.concatenate([jnp.sum(a, axis=0, keepdims=True), jnp.sum(b, axis=0, keepdims=True)], axis=0)

    def ratio(parts):
        both = jnp.sum(parts, axis=0)
        both = jnp.sum(both, axis=1, keepdims=True)
        return both[0:1] / both[1:2]

    nothing = jnp.zeros((Y, LANES), jnp.float32)
    precondition(0, z0, jnp.zeros((2, 1, LANES), jnp.float32))
    rz, zw = nothing, nothing
    for i in range(X):
        mid, image = operator(z0, DEPTH + i)
        g0[1, DEPTH + i, TOP:TOP + Y, :] = image
        rz = rz + g0[0, DEPTH + i, TOP:TOP + Y, :] * mid
        zw = zw + mid * image
    precondition(1, z1, sums_of(rz, zw)[:, None, :])
    alpha = ratio(cr[1, :, packed:packed + 2, 0, :])
    rz, zw = nothing, nothing
    for i in range(X):
        mid, image = operator(z1, DEPTH + i)
        here = (DEPTH + i, slice(TOP, TOP + Y))
        zi0, w0 = z0[here], g0[(1,) + here]
        r = g0[(0,) + here] - alpha * w0
        zi1 = zi0 - alpha * mid
        w1 = w0 - alpha * image
        rz = rz + r * zi1
        zw = zw + zi1 * w1
        sol_ref[i] = ux[1 + i, TOP:TOP + Y, :] + alpha * zi0
        res_ref[i] = r
        bb[i] = zi1
        wv[i] = w1
    sums = sums_of(rz, zw)
    ds[...] = sums
    dr[me] = sums
    to_all(ds, dr, dsend.at[0], drecv.at[0])
    sent_all(face_copies())
    for k in range(STEPS):
        sent_all(z_copies(k))
        sent_all(main_copies(k))
        sent_more(k)
        all_done(cr.at[k], csend.at[k])
    all_done(dr, drecv.at[0])
    alpha = ratio(dr[...])
    for i in range(X):
        sol_ref[i] = sol_ref[i] + alpha * bb[i]
        res_ref[i] = res_ref[i] - alpha * wv[i]
    all_done(dr, dsend.at[0])


def solution(mesh):
    sizes = tuple(mesh.shape[a] for a in AXES)
    n = sizes[0] * sizes[1] * sizes[2]

    def run(right_side, guess):
        X, Y, Z = block = guess.shape
        assert Z == LANES and PER == DEPTH and X % PER == 0 and X * DEPTH <= LANES
        dims = [tuple(d >> l for d in block) for l in range(LEVELS)]
        f32 = jnp.float32
        vm = lambda *s: pltpu.VMEM(s, f32)
        ext = [(dims[l][0] + 2 * DEPTH, dims[l][1] + 2 * TOP, LANES) for l in range(HALOED)]
        slab = (X // PER + 2, Y + 2 * TOP, LANES)
        tall = [(dims[l][1] + 2 * DEPTH, LANES) for l in range(HALOED)]
        cx, cy, width = dims[HALOED]
        packed = cx // plane_groups((cx, cy), width) + 2
        zrows = sum(dims[l][1] for l in range(HALOED))
        dma = lambda *s: pltpu.SemaphoreType.DMA(s)
        scratch = [
            vm(X + 2, Y + 2 * TOP, LANES), vm(*block),
            *(vm(STEPS, *e) for e in ext), vm(STEPS, *slab),
            *(vm(*e) for e in ext for _ in range(2)), vm(*slab), vm(*slab),
            vm(*ext[0]), vm(*ext[0]), vm(*block),
            vm(slab[0], *tall[0]), vm(slab[0], *tall[0]),
            vm(dims[1][0] + 2, 2 * tall[1][0], LANES), vm(dims[1][0] + 2, 2 * tall[1][0], LANES),
            *(vm(*t) for t in tall), vm(*tall[0]),
            vm(cx * sizes[0] + DEPTH, cy * sizes[1], LANES),
            vm(cx + DEPTH, 2 * cy * sizes[1] + 2 * DEPTH, LANES),
            vm(X // 2, Y, LANES), vm(X // 2, 2 * Y, LANES),
            vm(Y, LANES), vm(2, Y, LANES),
            vm(STEPS, 2, zrows, LANES), vm(STEPS, 2, zrows, LANES),
            vm(STEPS, packed, 1, LANES), vm(STEPS, n, packed, 1, LANES),
            vm(2, LANES), vm(n, 2, LANES),
            dma(2), dma(6), dma(6), dma(STEPS, 2), dma(STEPS, 2),
            dma(STEPS, 8), dma(STEPS, 8), dma(STEPS, HALOED, 8), dma(STEPS, HALOED, 8),
            dma(STEPS), dma(STEPS), dma(1), dma(1),
        ]
        return tuple(pl.pallas_call(
            functools.partial(kernel, sizes, block),
            out_shape=(pltpu.VMEM(block, f32), pltpu.VMEM(block, f32)),
            in_specs=[pl.BlockSpec(memory_space=pl.ANY)] * 2,
            out_specs=[pl.BlockSpec(memory_space=pltpu.VMEM)] * 2,
            scratch_shapes=scratch,
            compiler_params=pltpu.CompilerParams(collective_id=0, has_side_effects=True),
        )(right_side, guess))

    spec = P(*AXES)
    return jax.shard_map(run, mesh=mesh, in_specs=(spec, spec), out_specs=(spec, spec), check_vma=False)
```

```python
import functools

import jax
import jax.numpy as jnp
from jax import lax
from jax.experimental import pallas as pl
from jax.experimental.pallas import tpu as pltpu
from jax.sharding import PartitionSpec as P

LEVELS = 6
SWEEPS = 4
STEPS = 2
HALOED = 3
AXES = ("gx", "gy", "gz")
LANES = 128
TOP = 8
DEPTH = SWEEPS
SPAN = 8 * DEPTH
PER = LANES // SPAN
MESH = pl.DeviceIdType.MESH
HIGH = lax.Precision.HIGHEST
AROUND = [(a, b) for a in (-1, 0, 1) for b in (-1, 0, 1) if (a, b) != (0, 0)]
FACES = [(d, s) for d in range(3) for s in (-1, 1)]


def iota(shape, dim):
    return lax.broadcasted_iota(jnp.int32, shape, dim)


def lanes_dot(x, matrix):
    first, second, _ = x.shape
    if second % 8 == 0:
        out = jnp.dot(x.reshape(first * second, LANES), matrix, precision=HIGH, preferred_element_type=jnp.float32)
        return out.reshape(first, second, LANES)
    planes = [jnp.dot(x[i], matrix, precision=HIGH, preferred_element_type=jnp.float32)[None] for i in range(first)]
    return jnp.concatenate(planes, axis=0)


def take(x, index):
    index = jnp.broadcast_to(index[:1], x.shape[-2:])
    if x.ndim == 2:
        return jnp.take_along_axis(x, index, axis=1, mode="promise_in_bounds")
    return jnp.stack([jnp.take_along_axis(x[i], index, axis=1, mode="promise_in_bounds") for i in range(x.shape[0])])


def halve_matrix(width, start):
    source, target = iota((LANES, LANES), 0), iota((LANES, LANES), 1) - start
    keep = (target >= 0) & (target < width) & ((source == 2 * target) | (source == 2 * target + 1))
    return jnp.where(keep, 0.125, 0.0)


def double_matrix(width, start):
    source, target = iota((LANES, LANES), 0) - start, iota((LANES, LANES), 1)
    keep = (source >= 0) & (source < width) & ((target == 2 * source) | (target == 2 * source + 1))
    return jnp.where(keep, 1.0, 0.0)


def wrapped(lane):
    return jnp.where(lane >= LANES - DEPTH, lane - LANES, lane)


def halve(x, width):
    lane = iota((8, LANES), 1)
    return take(x + turn(x, -1), 2 * (lane % width)) * 0.125


def plane_groups(shape, width):
    return max(1, LANES // width // shape[1])


def own_group(shape, width):
    group = iota(shape, 0) % plane_groups(shape, width) * shape[1] + iota(shape, 1)
    return iota(shape, 2) // width == group


def gather_matrix(width, start):
    source, target = iota((LANES, LANES), 0) % width, iota((LANES, LANES), 1) - start
    return jnp.where(source == target, 1.0, 0.0)


def turn(x, shift):
    shift = shift % LANES
    return pltpu.roll(x, shift, x.ndim - 1) if shift else x


def kernel(sizes, block, b_hbm, x_hbm, sol_ref, z_ref, res_ref, w_ref, alpha_ref, *rest):
    (ux, bb, g0, g1, g2, gs, f0a, f0b, f0c, f1a, f1b, f1c, f2a, f2b, f2c, fsa, fsb, fsc, z0, z1, sc, sd, pd, pe,
     m0, m1, m2, ms, wref, wide, fold, spread, xg, yg, ze, zi, zs, zr, cs, cr, ds, dr, blank,
     isem, xsend, xrecv, zsend, zrecv, send, mrecv, frecv, csend, crecv, dsend, drecv) = rest
    nx, ny, nz = sizes
    n = nx * ny * nz
    at = tuple(lax.axis_index(a) for a in AXES)
    me = (at[0] * ny + at[1]) * nz + at[2]
    dims = [tuple(d >> l for d in block) for l in range(LEVELS)]
    X, Y, Z = block
    fields = (g0, g1, g2)
    after = ((f0a, f0b, f0c), (f1a, f1b, f1c), (f2a, f2b, f2c), (fsa, fsb, fsc))
    masks = (m0, m1, m2)
    groups = X // PER
    lower = [at[d] > 0 for d in range(3)]
    upper = [at[d] < sizes[d] - 1 for d in range(3)]
    inlow = [jnp.where(c, 1.0, 0.0) for c in lower]
    inup = [jnp.where(c, 1.0, 0.0) for c in upper]

    load_x = pltpu.make_async_copy(x_hbm, ux.at[1:X + 1, TOP:TOP + Y], isem.at[0])
    load_b = pltpu.make_async_copy(b_hbm, bb, isem.at[1])
    load_x.start()
    load_b.start()

    def others():
        moved = [[lax.rem(at[d] + k, sizes[d]) if k else at[d] for k in range(sizes[d])] for d in range(3)]
        return [(a, b, c) for a in moved[0] for b in moved[1] for c in moved[2]][1:]

    barrier = pltpu.get_barrier_semaphore()
    for target in others():
        pl.semaphore_signal(barrier, inc=1, device_id=target, device_id_type=MESH)

    def outside(dim, side):
        for l in range(HALOED + 1):
            A, B = (groups if l == HALOED else dims[l][0]), (Y if l == HALOED else dims[l][1])
            d, ref = (1, gs) if l == HALOED else (DEPTH, fields[l])
            for k in range(STEPS):
                if dim == 0:
                    a = A + d if side else 0
                    ref[k, a:a + d, TOP - DEPTH:TOP + B + DEPTH, :] = jnp.zeros((d, B + 2 * DEPTH, LANES), jnp.float32)
                else:
                    a = TOP + B if side else TOP - DEPTH
                    ref[k, :, a:a + DEPTH, :] = jnp.zeros((A + 2 * d, DEPTH, LANES), jnp.float32)

    for side in (0, 1):
        for dim in range(2):
            @pl.when(jnp.logical_not((upper if side else lower)[dim]))
            def _(dim=dim, side=side):
                outside(dim, side)
                ref = (xg, yg)[dim]
                ref[1 - side] = jnp.zeros(ref.shape[1:], jnp.float32)
        @pl.when(jnp.logical_not((upper if side else lower)[2]))
        def _(side=side):
            zi[1 if side else 0] = jnp.zeros(zi.shape[1:], jnp.float32)
            for k in range(STEPS):
                zr[k, 0 if side else 1] = jnp.zeros(zr.shape[2:], jnp.float32)

    ux[:, TOP - 1:TOP, :] = jnp.zeros((X + 2, 1, LANES), jnp.float32)
    ux[:, TOP + Y:TOP + Y + 1, :] = jnp.zeros((X + 2, 1, LANES), jnp.float32)
    ux[0, TOP:TOP + Y, :] = jnp.zeros((Y, LANES), jnp.float32)
    ux[X + 1, TOP:TOP + Y, :] = jnp.zeros((Y, LANES), jnp.float32)
    wref[...] = jnp.zeros_like(wref)
    wide[...] = jnp.zeros_like(wide)

    def mask(rows, z, depth_z):
        y = iota((rows + 2 * DEPTH, LANES), 0) - DEPTH
        part = jnp.where(y < 0, inlow[1], jnp.where(y >= rows, inup[1], 1.0))
        return part * jnp.where(z < 0, inlow[2], jnp.where(z >= depth_z, inup[2], 1.0)) * (1.0 / 9.0)

    for l in range(HALOED):
        lane = iota((dims[l][1] + 2 * DEPTH, LANES), 1)
        masks[l][...] = mask(dims[l][1], lane if l == 0 else wrapped(lane), dims[l][2])
    lane = iota((Y + 2 * DEPTH, LANES), 1) % SPAN
    ms[...] = mask(Y, jnp.where(lane < SPAN // 2, lane + Z - SPAN // 4, lane - 3 * SPAN // 4), Z)

    def face_copies():
        out = []
        for i, (d, s) in enumerate(FACES):
            target = list(at)
            target[d] = at[d] + s
            into = 1 if s > 0 else 0
            if d == 0:
                src, dst = ux.at[X if s > 0 else 1, TOP:TOP + Y], xg.at[into]
            elif d == 1:
                a = TOP + Y - 1 if s > 0 else TOP
                src, dst = ux.at[1:X + 1, a:a + 1], yg.at[into]
            else:
                src, dst = ze, zi.at[0 if s > 0 else 1]
            copy = pltpu.make_async_remote_copy(
                src_ref=src, dst_ref=dst, send_sem=xsend.at[i], recv_sem=xrecv.at[i],
                device_id=tuple(target), device_id_type=MESH,
            )
            out.append((copy, upper[d] if s > 0 else lower[d], lower[d] if s > 0 else upper[d]))
        return out

    def z_copies(k):
        out = []
        for side in (0, 1):
            copy = pltpu.make_async_remote_copy(
                src_ref=zs.at[k, side], dst_ref=zr.at[k, side], send_sem=zsend.at[side], recv_sem=zrecv.at[k, side],
                device_id=(at[0], at[1], at[2] + (1 if side else -1)), device_id_type=MESH,
            )
            out.append((copy, upper[2] if side else lower[2], lower[2] if side else upper[2]))
        return out

    def span(step, depth, start, own, other):
        if step > 0:
            return (start + own - depth, depth), (start - depth, depth)
        if step < 0:
            return (start, depth), (start + own, depth)
        return (start, own), (start, own)

    def around_copies(ref, k, depth, planes, rows, rsem):
        out = []
        for i, (dx, dy) in enumerate(AROUND):
            (sx, lx), (tx, _) = span(dx, depth, depth, planes, None)
            (sy, ly), (ty, _) = span(dy, DEPTH, TOP, rows, None)
            copy = pltpu.make_async_remote_copy(
                src_ref=ref.at[k, sx:sx + lx, sy:sy + ly], dst_ref=ref.at[k, tx:tx + lx, ty:ty + ly],
                send_sem=send.at[i], recv_sem=rsem.at[k, i],
                device_id=(at[0] + dx, at[1] + dy, at[2]), device_id_type=MESH,
            )
            to, fro = None, None
            for d, s in ((0, dx), (1, dy)):
                if s:
                    a, b = (upper[d], lower[d]) if s > 0 else (lower[d], upper[d])
                    to = a if to is None else jnp.logical_and(to, a)
                    fro = b if fro is None else jnp.logical_and(fro, b)
            out.append((copy, to, fro, lx * ly))
        return out

    def main_copies(k):
        return around_copies(g0, k, DEPTH, X, Y, mrecv)

    def more_copies(k):
        out = [around_copies(gs, k, 1, groups, Y, frecv)]
        for l in range(1, HALOED):
            out.append(around_copies(fields[l], k, DEPTH, dims[l][0], dims[l][1], frecv))
        return [[kind[i] for kind in out] for i in range(len(AROUND))]

    def lines(copies):
        return sum(entry[3] for entry in copies)

    def bytes_done(count, sem):
        part = blank.at[pl.ds(0, count)]
        pltpu.make_async_copy(part, part, sem).wait()

    def start_all(copies):
        for copy, cond, *_ in copies:
            pl.when(cond)(copy.start)

    def wait_all(copies):
        for copy, _, cond, *_ in copies:
            pl.when(cond)(copy.wait_recv)

    def sent_all(copies):
        for copy, cond, *_ in copies:
            pl.when(cond)(copy.wait_send)

    def start_more(k):
        for same in more_copies(k):
            @pl.when(same[0][1])
            def _(same=same):
                for copy, *_ in same:
                    copy.start()

    def wait_more(k):
        for i, same in enumerate(more_copies(k)):
            pl.when(same[0][2])(lambda i=i, same=same: bytes_done(lines(same), frecv.at[k, i]))

    def sent_around():
        for i, same in enumerate(more_copies(0)):
            count = STEPS * (lines(same) + lines([main_copies(0)[i]]))
            pl.when(same[0][1])(lambda i=i, count=count: bytes_done(count, send.at[i]))
        for side in (0, 1):
            part = zs.at[:, side]
            cond = upper[2] if side else lower[2]
            pl.when(cond)(pltpu.make_async_copy(part, part, zsend.at[side]).wait)

    def to_all(src, dst, s_sem, r_sem):
        for target in others():
            pltpu.make_async_remote_copy(
                src_ref=src, dst_ref=dst.at[me], send_sem=s_sem, recv_sem=r_sem,
                device_id=target, device_id_type=MESH,
            ).start()

    def all_done(dst, sem):
        part = dst.at[pl.ds(0, n - 1)]
        pltpu.make_async_copy(part, part, sem).wait()

    def fold_xy(field):
        A, B, _ = field.shape
        pairs = field.reshape(A // 2, 2, B, LANES)
        fold[0:A // 2, 0:B, :] = pairs[:, 0] + pairs[:, 1]
        return fold[0:A // 2, pl.ds(0, B // 2, 2), :] + fold[0:A // 2, pl.ds(1, B // 2, 2), :]

    def spread_y(field, into, first=0):
        A, B, _ = field.shape
        into[0:A, pl.ds(first, B, 2), :] = field
        into[0:A, pl.ds(first + 1, B, 2), :] = field

    def twice(field):
        A, B, _ = field.shape
        return jnp.broadcast_to(field[:, None], (A, 2, B, LANES)).reshape(2 * A, B, LANES)

    def own(ref, l, k=None):
        A, B, _ = dims[l]
        return ref[(k,) * (k is not None) + (slice(DEPTH, DEPTH + A), slice(TOP, TOP + B))]

    def update(src, rhs, dst, a, c, low, rows, scale):
        at_rows = slice(low, low + rows)
        mid = src[a:a + c, at_rows, :]
        total = src[a - 1:a - 1 + c, at_rows, :] + src[a + 1:a + 1 + c, at_rows, :]
        total = total + src[a:a + c, low - 1:low - 1 + rows, :] + src[a:a + c, low + 1:low + 1 + rows, :]
        total = total + turn(mid, 1) + turn(mid, -1)
        dst[a:a + c, at_rows, :] = rhs[a:a + c, at_rows, :] + (3.0 * mid + total) * scale

    def pieces(a, b):
        return [(p, min(4, b - p)) for p in range(a, b, 4)]

    def sweep(l, src, rhs, dst, k):
        A, B, _ = dims[l]
        low, rows = TOP - DEPTH, B + 2 * DEPTH
        m = masks[l][...]
        update(src, rhs, dst, k, DEPTH - k, low, rows, m * inlow[0])
        for a, c in pieces(DEPTH, DEPTH + A):
            update(src, rhs, dst, a, c, low, rows, m)
        update(src, rhs, dst, DEPTH + A, DEPTH - k, low, rows, m * inup[0])

    def sweep_inside(src, rhs, dst, k):
        for a, c in pieces(DEPTH + k, DEPTH + X - k):
            update(src, rhs, dst, a, c, TOP + k, Y - 2 * k, 1.0 / 9.0)

    def sweep_rim(src, rhs, dst, k):
        low, rows = TOP - DEPTH, Y + 2 * DEPTH
        m = m0[...]
        update(src, rhs, dst, k, DEPTH - k, low, rows, m * inlow[0])
        update(src, rhs, dst, DEPTH, k, low, rows, m)
        update(src, rhs, dst, DEPTH + X - k, k, low, rows, m)
        update(src, rhs, dst, DEPTH + X, DEPTH - k, low, rows, m * inup[0])
        for start in (0, Y):
            edge = m0[start:start + 2 * DEPTH, :]
            for a, c in pieces(DEPTH + k, DEPTH + X - k):
                update(src, rhs, dst, a, c, low + start, 2 * DEPTH, edge)

    def sweep_slab(src, rhs, dst):
        low, rows = TOP - DEPTH, Y + 2 * DEPTH
        lane = iota((rows, LANES), 1)
        m = ms[...]
        for g in range(groups + 2):
            mid = src[g, low:low + rows, :]
            total = src[g, low - 1:low - 1 + rows, :] + src[g, low + 1:low + 1 + rows, :]
            total = total + turn(mid, 1) + turn(mid, -1)
            before = mid if g == 0 else jnp.where(lane >= LANES - SPAN, src[g - 1, low:low + rows, :], mid)
            behind = mid if g == groups + 1 else jnp.where(lane < SPAN, src[g + 1, low:low + rows, :], mid)
            total = total + turn(before, SPAN) + turn(behind, -SPAN)
            scale = m * inlow[0] if g == 0 else m * inup[0] if g == groups + 1 else m
            dst[g, low:low + rows, :] = rhs[g, low:low + rows, :] + (3.0 * mid + total) * scale

    def smooth_whole(rhs, width, l):
        A, B, _ = rhs.shape
        lane = iota(rhs.shape, 2)
        e = rhs
        for _ in range(SWEEPS - 1):
            px, py = jnp.zeros((1, B, LANES), jnp.float32), jnp.zeros((A, 1, LANES), jnp.float32)
            total = jnp.concatenate([px, e[:-1]], axis=0) + jnp.concatenate([e[1:], px], axis=0)
            total = total + jnp.concatenate([py, e[:, :-1]], axis=1) + jnp.concatenate([e[:, 1:], py], axis=1)
            total = total + jnp.where(lane == 0, 0.0, turn(e, 1))
            total = total + jnp.where(lane == width - 1, 0.0, turn(e, -1))
            e = rhs + (3.0 * e + total) * (1.0 / 9.0)
        return e * (4.0 ** l / 9.0)

    half, quarter = SPAN // 2, SPAN // 4

    def pack_slab(k):
        lane = iota((Y, LANES), 1)
        line, spot = lane // SPAN, lane % SPAN
        low = high = jnp.zeros((Y, LANES), jnp.float32)
        for g in range(groups):
            both = jnp.zeros((Y, LANES), jnp.float32)
            for i in range(PER):
                field = g0[k, DEPTH + g * PER + i, TOP:TOP + Y, :]
                both = jnp.where((line == i) & (spot < half), turn(field, SPAN * i + quarter), both)
            gs[k, g + 1, TOP:TOP + Y, :] = jnp.where(
                spot < quarter, both, jnp.where(spot >= 3 * quarter, turn(both, half), 0.0))
            here = spot // DEPTH == g
            low = jnp.where(here, turn(both, DEPTH * g - quarter), low)
            high = jnp.where(here, turn(both, DEPTH * g - quarter + DEPTH), high)
        zs[k, 0, 0:Y, :] = low
        zs[k, 1, 0:Y, :] = high

    def pack_level(k, l, first):
        A, B, C = dims[l]
        lane = iota((B, LANES), 1)
        out = jnp.zeros((B, LANES), jnp.float32)
        for i in range(A):
            field = fields[l][k, DEPTH + i, TOP:TOP + B, :]
            out = jnp.where(lane // DEPTH == i, turn(field, DEPTH * i), out)
            out = jnp.where(lane // DEPTH == A + i, turn(field, DEPTH * (A + i) - C + DEPTH), out)
        for side in (0, 1):
            zs[k, side, first:first + B, :] = out

    def unpack_slab(k):
        spot = iota((Y, LANES), 1) % SPAN
        above, below = zr[k, 0, 0:Y, :], zr[k, 1, 0:Y, :]
        for g in range(groups):
            held = gs[k, g + 1, TOP:TOP + Y, :]
            held = jnp.where(spot // DEPTH == 2, turn(above, 2 * DEPTH - DEPTH * g), held)
            gs[k, g + 1, TOP:TOP + Y, :] = jnp.where(spot // DEPTH == 5, turn(below, 5 * DEPTH - DEPTH * g), held)

    def unpack_level(k, l, first):
        A, B, C = dims[l]
        lane = iota((B, LANES), 1)
        above, below = zr[k, 0, first:first + B, :], zr[k, 1, first:first + B, :]
        for i in range(A):
            held = fields[l][k, DEPTH + i, TOP:TOP + B, :]
            held = jnp.where(lane // DEPTH == C // DEPTH, turn(above, C - DEPTH * i), held)
            fields[l][k, DEPTH + i, TOP:TOP + B, :] = jnp.where(
                lane >= LANES - DEPTH, turn(below, -DEPTH - DEPTH * (A + i)), held)

    width = dims[HALOED][2]
    cx, cy, _ = dims[HALOED]
    starts = [0, Y, Y + dims[1][1]]
    packed = cx // plane_groups((cx, cy), width)

    def coarse(k):
        per = plane_groups((cx, cy), width)
        fine = None
        for c in range(nz):
            rows = []
            for i in range(nx):
                columns = []
                for j in range(ny):
                    part = cr[k, (i * ny + j) * nz + c, 0:packed][:, None]
                    part = jnp.broadcast_to(part, (cx // per, per, cy, LANES)).reshape(cx, cy, LANES)
                    columns.append(jnp.where(own_group((cx, cy, LANES), width), part, 0.0))
                rows.append(jnp.concatenate(columns, axis=1))
            spot = lanes_dot(jnp.concatenate(rows, axis=0), gather_matrix(width, c * width))
            fine = spot if fine is None else fine + spot
        chain = [fine]
        widths = [width * nz]
        for l in range(HALOED + 1, LEVELS):
            widths.append(widths[-1] // 2)
            chain.append(jnp.where(iota((1, 1, LANES), 2) < widths[-1], halve(fold_xy(chain[-1]), LANES // 2), 0.0))
        whole = smooth_whole(chain[-1], widths[-1], LEVELS - 1)
        for l in range(LEVELS - 2, HALOED - 1, -1):
            i = l - HALOED
            spread_y(whole, spread)
            grown = spread[0:whole.shape[0], 0:2 * whole.shape[1], :]
            grown = twice(take(grown, iota((8, LANES), 1) // 2))
            whole = grown + smooth_whole(chain[i], widths[i], l)
        wref[DEPTH // 2:DEPTH // 2 + nx * cx, :, :] = whole

    def precondition(k, z, extra):
        start_all(main_copies(k))
        lane = iota((8, LANES), 1)
        for l in range(HALOED - 1):
            A, B, C = dims[l + 1]
            coarser = jnp.where(iota((1, 1, LANES), 2) < C, halve(fold_xy(own(fields[l], l, k)), LANES // 2), 0.0)
            fields[l + 1][k, DEPTH:DEPTH + A, TOP:TOP + B, :] = coarser
            pack_level(k, l + 1, starts[l + 1])
        pack_slab(k)
        start_all(z_copies(k))
        mine = halve(fold_xy(own(fields[HALOED - 1], HALOED - 1, k)), width)
        mine = jnp.where(own_group(mine.shape, width), mine, 0.0)
        mine = jnp.sum(mine.reshape(-1, plane_groups(mine.shape, width), *mine.shape[1:]), axis=1)
        mine = jnp.sum(mine, axis=1, keepdims=True)
        mine = jnp.concatenate([mine, extra], axis=0)
        cs[k] = mine
        cr[k, me] = mine
        to_all(cs.at[k], cr.at[k], csend.at[k], crecv.at[k])
        for s in range(1, SWEEPS):
            sweep_inside(after[0][s - 2] if s > 1 else g0.at[k], g0.at[k], after[0][s - 1], s)
        wait_all(z_copies(k))
        unpack_slab(k)
        for l in range(1, HALOED):
            unpack_level(k, l, starts[l])
        start_more(k)
        wait_all(main_copies(k))
        for s in range(1, SWEEPS):
            sweep_rim(after[0][s - 2] if s > 1 else g0.at[k], g0.at[k], after[0][s - 1], s)
        all_done(cr.at[k], crecv.at[k])
        coarse(k)
        spread_y(wref[pl.ds(at[0] * cx, cx + DEPTH)], wide, DEPTH)
        part = wide[:, pl.ds(pl.multiple_of(at[1] * 2 * cy, 8), 2 * cy + 2 * DEPTH), :]
        source = (wrapped(lane) >> 1) + at[2] * width
        inside = (source >= 0) & (source < width * nz)
        part = take(part, jnp.where(inside, source, 0))
        part = jnp.where(inside[0:1][None], part, 0.0)
        part = twice(part)[DEPTH - 1:DEPTH + dims[HALOED - 1][0] + 1]
        wait_more(k)
        for s in range(1, SWEEPS):
            sweep_slab(after[3][s - 2] if s > 1 else gs.at[k], gs.at[k], after[3][s - 1])
            for l in range(1, HALOED):
                sweep(l, after[l][s - 2] if s > 1 else fields[l].at[k], fields[l].at[k], after[l][s - 1], s)
        for l in range(HALOED - 1, 0, -1):
            A, B, C = dims[l]
            end = after[l][SWEEPS - 2][DEPTH - 1:DEPTH + A + 1, TOP - DEPTH:TOP + B + DEPTH, :]
            full = end * (4.0 ** l / 9.0) + part
            if l > 1:
                spread_y(take(full, (wrapped(lane) >> 1) & (LANES - 1)), spread)
                part = twice(spread[0:A + 2, DEPTH:DEPTH + 2 * B + 2 * DEPTH, :])[1:2 * A + 3]
            else:
                spread_y(take(full, lane // 2), pd)
                spread_y(take(full, jnp.where(lane == 0, LANES - 1, C)), pe)
        low, rows = TOP - DEPTH, Y + 2 * DEPTH
        slab = after[3][SWEEPS - 2]
        spot = iota((rows, LANES), 1) % SPAN
        for g in range(groups + 2):
            s = slab[g, low:low + rows, :]
            sc[g] = jnp.where(spot < quarter, s, turn(s, -half))
            sd[g] = jnp.where(spot <= quarter, s, turn(s, quarter + 1 - (3 * quarter - 1)))
        lane = iota((rows, LANES), 1)
        near = (lane < DEPTH - 1) | (lane > LANES - DEPTH)
        end = after[0][SWEEPS - 2]
        for p in range(DEPTH - 1, DEPTH + X + 1):
            g, i = p // PER, p % PER
            f = jnp.where(near, turn(sc[g], -quarter - SPAN * i), end[p, low:low + rows, :])
            z[p, low:low + rows, :] = f * (1.0 / 9.0) + pd[(p - DEPTH + 2) // 2, low:low + rows, :]

    def around(ref, p):
        mid = ref[p, TOP:TOP + Y, :]
        total = ref[p - 1, TOP:TOP + Y, :] + ref[p + 1, TOP:TOP + Y, :]
        return mid, total + ref[p, TOP - 1:TOP - 1 + Y, :] + ref[p, TOP + 1:TOP + 1 + Y, :]

    lane = iota((Y, LANES), 1)
    first, last = lane == 0, lane == LANES - 1

    def operator(z, p):
        mid, total = around(z, p)
        g, i = p // PER, p % PER
        ghost = turn(sd[g, DEPTH:DEPTH + Y, :], LANES - 1 - quarter - SPAN * i) * (1.0 / 9.0)
        ghost = ghost + pe[(p - DEPTH + 2) // 2, TOP:TOP + Y, :]
        total = total + jnp.where(first, ghost, turn(mid, 1))
        total = total + jnp.where(last, ghost, turn(mid, -1))
        return mid, 6.0 * mid - total

    load_x.wait()
    out = jnp.zeros((Y, LANES), jnp.float32)
    for i in range(X):
        out = jnp.where(lane // 2 == i, turn(ux[1 + i, TOP:TOP + Y, :], 2 * i + 1), out)
    ze[...] = out
    pl.semaphore_wait(barrier, n - 1)
    start_all(face_copies())
    load_b.wait()
    for i in range(X):
        mid, total = around(ux, 1 + i)
        total = total + jnp.where(first, 0.0, turn(mid, 1))
        total = total + jnp.where(last, 0.0, turn(mid, -1))
        g0[0, DEPTH + i, TOP:TOP + Y, :] = bb[i] - (6.0 * mid - total)
    wait_all(face_copies())
    for i, side in ((0, 1), (X - 1, 0)):
        here = (0, DEPTH + i, slice(TOP, TOP + Y))
        g0[here] = g0[here] + xg[side]
    for j, side in ((0, 1), (Y - 1, 0)):
        here = (0, slice(DEPTH, DEPTH + X), slice(TOP + j, TOP + j + 1))
        g0[here] = g0[here] + yg[side]
    ghosts = jnp.where(lane % 2 == 0, turn(zi[1], -1), turn(zi[0], 1))
    for i in range(X):
        here = (0, DEPTH + i, slice(TOP, TOP + Y))
        g0[here] = g0[here] + jnp.where(first | last, turn(ghosts, -2 * i - 1), 0.0)

    def sums_of(a, b):
        return jnp.concatenate([jnp.sum(a, axis=0, keepdims=True), jnp.sum(b, axis=0, keepdims=True)], axis=0)

    def ratio(parts):
        both = jnp.sum(parts, axis=0)
        both = jnp.sum(both, axis=1, keepdims=True)
        return both[0:1] / both[1:2]

    nothing = jnp.zeros((Y, LANES), jnp.float32)
    precondition(0, z0, jnp.zeros((2, 1, LANES), jnp.float32))
    rz, zw = nothing, nothing
    for i in range(X):
        mid, image = operator(z0, DEPTH + i)
        g0[1, DEPTH + i, TOP:TOP + Y, :] = image
        rz = rz + g0[0, DEPTH + i, TOP:TOP + Y, :] * mid
        zw = zw + mid * image
    precondition(1, z1, sums_of(rz, zw)[:, None, :])
    alpha = ratio(cr[1, :, packed:packed + 2, 0, :])
    rz, zw = nothing, nothing
    for i in range(X):
        mid, image = operator(z1, DEPTH + i)
        here = (DEPTH + i, slice(TOP, TOP + Y))
        before, w = z0[here], g0[(1,) + here]
        r = g0[(0,) + here] - alpha * w
        z = before - alpha * mid
        w = w - alpha * image
        rz = rz + r * z
        zw = zw + z * w
        sol_ref[i] = ux[1 + i, TOP:TOP + Y, :] + alpha * before
        z_ref[i] = z
        res_ref[i] = r
        w_ref[i] = w
    sums = sums_of(rz, zw)
    ds[...] = sums
    dr[me] = sums
    to_all(ds, dr, dsend.at[0], drecv.at[0])
    sent_all(face_copies())
    sent_around()
    for k in range(STEPS):
        all_done(cr.at[k], csend.at[k])
    all_done(dr, dsend.at[0])
    all_done(dr, drecv.at[0])
    alpha_ref[...] = jnp.broadcast_to(ratio(dr[...]), alpha_ref.shape)


def solution(mesh):
    sizes = tuple(mesh.shape[a] for a in AXES)
    n = sizes[0] * sizes[1] * sizes[2]

    def run(right_side, guess):
        X, Y, Z = block = guess.shape
        assert Z == LANES and PER == DEPTH and X % PER == 0 and X * DEPTH <= LANES
        dims = [tuple(d >> l for d in block) for l in range(LEVELS)]
        f32 = jnp.float32
        vm = lambda *s: pltpu.VMEM(s, f32)
        ext = [(dims[l][0] + 2 * DEPTH, dims[l][1] + 2 * TOP, LANES) for l in range(HALOED)]
        slab = (X // PER + 2, Y + 2 * TOP, LANES)
        tall = [(dims[l][1] + 2 * DEPTH, LANES) for l in range(HALOED)]
        cx, cy, width = dims[HALOED]
        packed = cx // plane_groups((cx, cy), width) + 2
        zrows = sum(dims[l][1] for l in range(HALOED))
        dma = lambda *s: pltpu.SemaphoreType.DMA(s)
        scratch = [
            vm(X + 2, Y + 2 * TOP, LANES), vm(*block),
            *(vm(STEPS, *e) for e in ext), vm(STEPS, *slab),
            *(vm(*e) for e in ext + [slab] for _ in range(SWEEPS - 1)),
            vm(*ext[0]), vm(*ext[0]),
            vm(slab[0], *tall[0]), vm(slab[0], *tall[0]),
            vm(dims[1][0] + 2, 2 * tall[1][0], LANES), vm(dims[1][0] + 2, 2 * tall[1][0], LANES),
            *(vm(*t) for t in tall), vm(*tall[0]),
            vm(cx * sizes[0] + DEPTH, cy * sizes[1], LANES),
            vm(cx + DEPTH, 2 * cy * sizes[1] + 2 * DEPTH, LANES),
            vm(X // 2, Y, LANES), vm(X // 2, 2 * Y, LANES),
            vm(2, Y, LANES), vm(2, X, 1, LANES), vm(Y, LANES), vm(2, Y, LANES),
            vm(STEPS, 2, zrows, LANES), vm(STEPS, 2, zrows, LANES),
            vm(STEPS, packed, 1, LANES), vm(STEPS, n, packed, 1, LANES),
            vm(2, LANES), vm(n, 2, LANES), vm(3 * STEPS * DEPTH * max(X, Y), LANES),
            dma(2), dma(6), dma(6), dma(2), dma(STEPS, 2),
            dma(8), dma(STEPS, 8), dma(STEPS, 8),
            dma(STEPS), dma(STEPS), dma(1), dma(1),
        ]
        whole = pltpu.VMEM(block, f32)
        base, z, r, w, alpha = pl.pallas_call(
            functools.partial(kernel, sizes, block),
            out_shape=(whole, whole, whole, whole, pltpu.VMEM((8, LANES), f32)),
            in_specs=[pl.BlockSpec(memory_space=pl.ANY)] * 2,
            out_specs=[pl.BlockSpec(memory_space=pltpu.VMEM)] * 5,
            scratch_shapes=scratch,
            compiler_params=pltpu.CompilerParams(collective_id=0, has_side_effects=True),
        )(right_side, guess)
        return base + alpha[0, 0] * z, r - alpha[0, 0] * w

    spec = P(*AXES)
    return jax.shard_map(run, mesh=mesh, in_specs=(spec, spec), out_specs=(spec, spec), check_vma=False)
```

```python
import functools

import jax
import jax.numpy as jnp
from jax import lax
from jax.experimental import pallas as pl
from jax.experimental.pallas import tpu as pltpu
from jax.sharding import PartitionSpec as P

LEVELS = 6
SWEEPS = 4
STEPS = 2
HALOED = 4
AXES = ("gx", "gy", "gz")
LANES = 128
TOP = 8
DEPTH = SWEEPS
SPAN = 8 * DEPTH
PER = LANES // SPAN
PARTS = 4
MESH = pl.DeviceIdType.MESH
HIGH = lax.Precision.HIGHEST
ROWS = 8
AROUND = [(a, b) for a in (-1, 0, 1) for b in (-1, 0, 1) if (a, b) != (0, 0)]
FACES = [(d, s) for d in range(3) for s in (-1, 1)]


def iota(shape, dim):
    return lax.broadcasted_iota(jnp.int32, shape, dim)


def take(x, index):
    if x.ndim == 3:
        return jnp.stack([take(x[i], index) for i in range(x.shape[0])])
    rows = x.shape[0]
    more = -rows % 8
    if rows == 1:
        x = jnp.broadcast_to(x, (8, LANES))
    elif more:
        x = jnp.concatenate([x, jnp.zeros((more, LANES), x.dtype)], axis=0)
    index = jnp.broadcast_to(index[:1], x.shape)
    out = jnp.take_along_axis(x, index, axis=1, mode="promise_in_bounds")
    return out[:rows] if more else out


def wrapped(lane):
    return jnp.where(lane >= LANES - DEPTH, lane - LANES, lane)


def halve(x, width):
    lane = iota((8, LANES), 1)
    return take(x + turn(x, -1), 2 * (lane % width)) * 0.125


def turn(x, shift):
    shift = shift % LANES
    return pltpu.roll(x, shift, x.ndim - 1) if shift else x


def kernel(sizes, block, b_hbm, x_hbm, sol_ref, z_ref, res_ref, w_ref, alpha_ref, *rest):
    (ux, bb, g0, g1, g2, g3, gs, f0a, f0b, f0c, f1a, f1b, f1c, f2a, f2b, f2c, f3a, f3b, f3c, fsa, fsb, fsc,
     z0, z1, sc, sd, pd, pe, m0, m1, m2, m3, ms, pmat, wref, wide, fold, spread, xg, yg, ze, zi, zs, zr, cs, cr, ds, dr, blank,
     isem, xsend, xrecv, zsend, zrecv, send, mrecv, frecv, csend, crecv, dsend, drecv) = rest
    nx, ny, nz = sizes
    n = nx * ny * nz
    at = tuple(lax.axis_index(a) for a in AXES)
    me = (at[0] * ny + at[1]) * nz + at[2]
    dims = [tuple(d >> l for d in block) for l in range(LEVELS)]
    X, Y, Z = block
    fields = (g0, g1, g2, g3)
    after = ((f0a, f0b, f0c), (f1a, f1b, f1c), (f2a, f2b, f2c), (f3a, f3b, f3c), (fsa, fsb, fsc))
    masks = (m0, m1, m2, m3)
    groups = X // PER
    lower = [at[d] > 0 for d in range(3)]
    upper = [at[d] < sizes[d] - 1 for d in range(3)]
    inlow = [jnp.where(c, 1.0, 0.0) for c in lower]
    inup = [jnp.where(c, 1.0, 0.0) for c in upper]

    load_x = pltpu.make_async_copy(x_hbm, ux.at[1:X + 1, TOP:TOP + Y], isem.at[0])
    load_b = pltpu.make_async_copy(b_hbm, bb, isem.at[1])
    load_x.start()
    load_b.start()

    def others():
        out = []
        for b in range(ny - 1, -1, -1):
            for c in range(nz - 1, -1, -1):
                for a in range(nx):
                    if b or c:
                        first = jnp.where(at[0] < nx // 2, nx - 1 - a, a)
                    elif a:
                        first = lax.rem(at[0] + a, nx)
                    else:
                        continue
                    out.append((first, lax.rem(at[1] + b, ny), lax.rem(at[2] + c, nz)))
        return out

    barrier = pltpu.get_barrier_semaphore()
    for target in others():
        pl.semaphore_signal(barrier, inc=1, device_id=target, device_id_type=MESH)

    def outside(dim, side):
        for l in range(HALOED + 1):
            A, B = (groups if l == HALOED else dims[l][0]), (Y if l == HALOED else dims[l][1])
            d, ref = (1, gs) if l == HALOED else (DEPTH, fields[l])
            for k in range(STEPS):
                if dim == 0:
                    a = A + d if side else 0
                    ref[k, a:a + d, TOP - DEPTH:TOP + B + DEPTH, :] = jnp.zeros((d, B + 2 * DEPTH, LANES), jnp.float32)
                else:
                    a = TOP + B if side else TOP - DEPTH
                    ref[k, :, a:a + DEPTH, :] = jnp.zeros((A + 2 * d, DEPTH, LANES), jnp.float32)

    for side in (0, 1):
        for dim in range(2):
            @pl.when(jnp.logical_not((upper if side else lower)[dim]))
            def _(dim=dim, side=side):
                outside(dim, side)
                ref = (xg, yg)[dim]
                ref[1 - side] = jnp.zeros(ref.shape[1:], jnp.float32)
        @pl.when(jnp.logical_not((upper if side else lower)[2]))
        def _(side=side):
            zi[1 if side else 0] = jnp.zeros(zi.shape[1:], jnp.float32)
            for k in range(STEPS):
                zr[k, 0 if side else 1] = jnp.zeros(zr.shape[2:], jnp.float32)

    ux[:, TOP - 1:TOP, :] = jnp.zeros((X + 2, 1, LANES), jnp.float32)
    ux[:, TOP + Y:TOP + Y + 1, :] = jnp.zeros((X + 2, 1, LANES), jnp.float32)
    ux[0, TOP:TOP + Y, :] = jnp.zeros((Y, LANES), jnp.float32)
    ux[X + 1, TOP:TOP + Y, :] = jnp.zeros((Y, LANES), jnp.float32)
    wref[...] = jnp.zeros_like(wref)
    wide[...] = jnp.zeros_like(wide)

    def mask(rows, z, depth_z):
        y = iota((rows + 2 * DEPTH, LANES), 0) - DEPTH
        part = jnp.where(y < 0, inlow[1], jnp.where(y >= rows, inup[1], 1.0))
        return part * jnp.where(z < 0, inlow[2], jnp.where(z >= depth_z, inup[2], 1.0)) * (1.0 / 9.0)

    for l in range(HALOED):
        lane = iota((dims[l][1] + 2 * DEPTH, LANES), 1)
        masks[l][...] = mask(dims[l][1], lane if l == 0 else wrapped(lane), dims[l][2])
    CA, CB, CC = dims[HALOED]
    CD = dims[HALOED + 1][2]
    cells = CA * CB
    row, column = iota(pmat.shape, 0), iota(pmat.shape, 1)
    cell, device = column // n, column % n
    plane, line = row // ROWS, row % ROWS
    dx, dy = device // (ny * nz), device // nz % ny
    fits = (cell < cells) & (plane == dx * CA + cell // CB) & (line == dy * CB + cell % CB)
    fits = fits | ((cell == cells) & (plane == nx * CA + dx) & (line == dy))
    pmat[...] = jnp.where(fits, 1.0, 0.0)
    lane = iota((Y + 2 * DEPTH, LANES), 1) % SPAN
    ms[...] = mask(Y, jnp.where(lane < SPAN // 2, lane + Z - SPAN // 4, lane - 3 * SPAN // 4), Z)

    def face_copies():
        out = []
        for i, (d, s) in enumerate(FACES):
            target = list(at)
            target[d] = at[d] + s
            into = 1 if s > 0 else 0
            if d == 0:
                src, dst = ux.at[X if s > 0 else 1, TOP:TOP + Y], xg.at[into]
            elif d == 1:
                a = TOP + Y - 1 if s > 0 else TOP
                src, dst = ux.at[1:X + 1, a:a + 1], yg.at[into]
            else:
                src, dst = ze, zi.at[0 if s > 0 else 1]
            copy = pltpu.make_async_remote_copy(
                src_ref=src, dst_ref=dst, send_sem=xsend.at[i], recv_sem=xrecv.at[i],
                device_id=tuple(target), device_id_type=MESH,
            )
            out.append((copy, upper[d] if s > 0 else lower[d], lower[d] if s > 0 else upper[d]))
        return out

    def z_copies(k):
        out = []
        for side in (0, 1):
            copy = pltpu.make_async_remote_copy(
                src_ref=zs.at[k, side], dst_ref=zr.at[k, side], send_sem=zsend.at[side], recv_sem=zrecv.at[k, side],
                device_id=(at[0], at[1], at[2] + (1 if side else -1)), device_id_type=MESH,
            )
            out.append((copy, upper[2] if side else lower[2], lower[2] if side else upper[2]))
        return out

    def span(step, depth, start, own, other):
        if step > 0:
            return (start + own - depth, depth), (start - depth, depth)
        if step < 0:
            return (start, depth), (start + own, depth)
        return (start, own), (start, own)

    def around_copies(ref, k, depth, planes, rows, rsem):
        out = []
        for i, (dx, dy) in enumerate(AROUND):
            (sx, lx), (tx, _) = span(dx, depth, depth, planes, None)
            (sy, ly), (ty, _) = span(dy, DEPTH, TOP, rows, None)
            copy = pltpu.make_async_remote_copy(
                src_ref=ref.at[k, sx:sx + lx, sy:sy + ly], dst_ref=ref.at[k, tx:tx + lx, ty:ty + ly],
                send_sem=send.at[i], recv_sem=rsem.at[k, i],
                device_id=(at[0] + dx, at[1] + dy, at[2]), device_id_type=MESH,
            )
            to, fro = None, None
            for d, s in ((0, dx), (1, dy)):
                if s:
                    a, b = (upper[d], lower[d]) if s > 0 else (lower[d], upper[d])
                    to = a if to is None else jnp.logical_and(to, a)
                    fro = b if fro is None else jnp.logical_and(fro, b)
            out.append((copy, to, fro, lx * ly))
        return out

    def main_copies(k):
        return around_copies(g0, k, DEPTH, X, Y, mrecv)

    def more_copies(k):
        out = [around_copies(gs, k, 1, groups, Y, frecv)]
        for l in range(1, HALOED):
            out.append(around_copies(fields[l], k, DEPTH, dims[l][0], dims[l][1], frecv))
        return [[kind[i] for kind in out] for i in range(len(AROUND))]

    def lines(copies):
        return sum(entry[3] for entry in copies)

    def bytes_done(count, sem):
        part = blank.at[pl.ds(0, count)]
        pltpu.make_async_copy(part, part, sem).wait()

    def start_all(copies):
        for copy, cond, *_ in copies:
            pl.when(cond)(copy.start)

    def wait_all(copies):
        for copy, _, cond, *_ in copies:
            pl.when(cond)(copy.wait_recv)

    def sent_all(copies):
        for copy, cond, *_ in copies:
            pl.when(cond)(copy.wait_send)

    def start_more(k):
        for same in more_copies(k):
            @pl.when(same[0][1])
            def _(same=same):
                for copy, *_ in same:
                    copy.start()

    def wait_more(k):
        for i, same in enumerate(more_copies(k)):
            pl.when(same[0][2])(lambda i=i, same=same: bytes_done(lines(same), frecv.at[k, i]))

    def sent_around():
        for i, same in enumerate(more_copies(0)):
            count = STEPS * (lines(same) + lines([main_copies(0)[i]]))
            pl.when(same[0][1])(lambda i=i, count=count: bytes_done(count, send.at[i]))
        for side in (0, 1):
            part = zs.at[:, side]
            cond = upper[2] if side else lower[2]
            pl.when(cond)(pltpu.make_async_copy(part, part, zsend.at[side]).wait)

    def to_all(src, dst, s_sem, r_sem):
        for target in others():
            pltpu.make_async_remote_copy(
                src_ref=src, dst_ref=dst.at[me], send_sem=s_sem, recv_sem=r_sem,
                device_id=target, device_id_type=MESH,
            ).start()

    def all_done(dst, sem):
        part = dst.at[pl.ds(0, n - 1)]
        pltpu.make_async_copy(part, part, sem).wait()

    def fold_xy(field):
        A, B, _ = field.shape
        pairs = field.reshape(A // 2, 2, B, LANES)
        fold[0:A // 2, 0:B, :] = pairs[:, 0] + pairs[:, 1]
        return fold[0:A // 2, pl.ds(0, B // 2, 2), :] + fold[0:A // 2, pl.ds(1, B // 2, 2), :]

    def spread_y(field, into, first=0):
        A, B, _ = field.shape
        into[0:A, pl.ds(first, B, 2), :] = field
        into[0:A, pl.ds(first + 1, B, 2), :] = field

    def twice(field):
        A, B, _ = field.shape
        return jnp.broadcast_to(field[:, None], (A, 2, B, LANES)).reshape(2 * A, B, LANES)

    def own(ref, l, k=None):
        A, B, _ = dims[l]
        return ref[(k,) * (k is not None) + (slice(DEPTH, DEPTH + A), slice(TOP, TOP + B))]

    def update(src, rhs, dst, a, c, low, rows, scale):
        at_rows = slice(low, low + rows)
        mid = src[a:a + c, at_rows, :]
        total = src[a - 1:a - 1 + c, at_rows, :] + src[a + 1:a + 1 + c, at_rows, :]
        total = total + src[a:a + c, low - 1:low - 1 + rows, :] + src[a:a + c, low + 1:low + 1 + rows, :]
        total = total + turn(mid, 1) + turn(mid, -1)
        dst[a:a + c, at_rows, :] = rhs[a:a + c, at_rows, :] + (3.0 * mid + total) * scale

    def pieces(a, b):
        return [(p, min(4, b - p)) for p in range(a, b, 4)]

    def sweep(l, src, rhs, dst, k):
        A, B, _ = dims[l]
        low, rows = TOP - DEPTH, B + 2 * DEPTH
        m = masks[l][...]
        update(src, rhs, dst, k, DEPTH - k, low, rows, m * inlow[0])
        for a, c in pieces(DEPTH, DEPTH + A):
            update(src, rhs, dst, a, c, low, rows, m)
        update(src, rhs, dst, DEPTH + A, DEPTH - k, low, rows, m * inup[0])

    def sweep_inside(src, rhs, dst, k):
        for a, c in pieces(DEPTH + k, DEPTH + X - k):
            update(src, rhs, dst, a, c, TOP + k, Y - 2 * k, 1.0 / 9.0)

    def sweep_rim(src, rhs, dst, k):
        low, rows = TOP - DEPTH, Y + 2 * DEPTH
        m = m0[...]
        update(src, rhs, dst, k, DEPTH - k, low, rows, m * inlow[0])
        update(src, rhs, dst, DEPTH, k, low, rows, m)
        update(src, rhs, dst, DEPTH + X - k, k, low, rows, m)
        update(src, rhs, dst, DEPTH + X, DEPTH - k, low, rows, m * inup[0])
        for start in (0, Y):
            edge = m0[start:start + 2 * DEPTH, :]
            for a, c in pieces(DEPTH + k, DEPTH + X - k):
                update(src, rhs, dst, a, c, low + start, 2 * DEPTH, edge)

    def sweep_slab(src, rhs, dst):
        low, rows = TOP - DEPTH, Y + 2 * DEPTH
        lane = iota((rows, LANES), 1)
        m = ms[...]
        for g in range(groups + 2):
            mid = src[g, low:low + rows, :]
            total = src[g, low - 1:low - 1 + rows, :] + src[g, low + 1:low + 1 + rows, :]
            total = total + turn(mid, 1) + turn(mid, -1)
            before = mid if g == 0 else jnp.where(lane >= LANES - SPAN, src[g - 1, low:low + rows, :], mid)
            behind = mid if g == groups + 1 else jnp.where(lane < SPAN, src[g + 1, low:low + rows, :], mid)
            total = total + turn(before, SPAN) + turn(behind, -SPAN)
            scale = m * inlow[0] if g == 0 else m * inup[0] if g == groups + 1 else m
            dst[g, low:low + rows, :] = rhs[g, low:low + rows, :] + (3.0 * mid + total) * scale

    def smooth_whole(rhs, depth_y, depth_z, l):
        A, B, _ = rhs.shape
        lane, row = iota(rhs.shape, 2), iota(rhs.shape, 1)
        e = rhs
        for _ in range(SWEEPS - 1):
            px, py = jnp.zeros((1, B, LANES), jnp.float32), jnp.zeros((A, 1, LANES), jnp.float32)
            total = jnp.concatenate([px, e[:-1]], axis=0) + jnp.concatenate([e[1:], px], axis=0)
            total = total + jnp.concatenate([py, e[:, :-1]], axis=1) + jnp.concatenate([e[:, 1:], py], axis=1)
            total = total + jnp.where(lane == 0, 0.0, turn(e, 1))
            total = total + jnp.where(lane == depth_z - 1, 0.0, turn(e, -1))
            e = rhs + jnp.where(row < depth_y, (3.0 * e + total) * (1.0 / 9.0), 0.0)
        return e * (4.0 ** l / 9.0)

    half, quarter = SPAN // 2, SPAN // 4

    def pack_slab(k):
        lane = iota((Y, LANES), 1)
        line, spot = lane // SPAN, lane % SPAN
        low = high = jnp.zeros((Y, LANES), jnp.float32)
        for g in range(groups):
            both = jnp.zeros((Y, LANES), jnp.float32)
            for i in range(PER):
                field = g0[k, DEPTH + g * PER + i, TOP:TOP + Y, :]
                both = jnp.where((line == i) & (spot < half), turn(field, SPAN * i + quarter), both)
            gs[k, g + 1, TOP:TOP + Y, :] = jnp.where(
                spot < quarter, both, jnp.where(spot >= 3 * quarter, turn(both, half), 0.0))
            here = spot // DEPTH == g
            low = jnp.where(here, turn(both, DEPTH * g - quarter), low)
            high = jnp.where(here, turn(both, DEPTH * g - quarter + DEPTH), high)
        zs[k, 0, 0:Y, :] = low
        zs[k, 1, 0:Y, :] = high

    def pack_level(k, l, first):
        A, B, C = dims[l]
        lane = iota((B, LANES), 1)
        out = jnp.zeros((B, LANES), jnp.float32)
        for i in range(A):
            field = fields[l][k, DEPTH + i, TOP:TOP + B, :]
            out = jnp.where(lane // DEPTH == i, turn(field, DEPTH * i), out)
            out = jnp.where(lane // DEPTH == A + i, turn(field, DEPTH * (A + i) - C + DEPTH), out)
        for side in (0, 1):
            zs[k, side, first:first + B, :] = out

    def unpack_slab(k):
        spot = iota((Y, LANES), 1) % SPAN
        above, below = zr[k, 0, 0:Y, :], zr[k, 1, 0:Y, :]
        for g in range(groups):
            held = gs[k, g + 1, TOP:TOP + Y, :]
            held = jnp.where(spot // DEPTH == 2, turn(above, 2 * DEPTH - DEPTH * g), held)
            gs[k, g + 1, TOP:TOP + Y, :] = jnp.where(spot // DEPTH == 5, turn(below, 5 * DEPTH - DEPTH * g), held)

    def unpack_level(k, l, first):
        A, B, C = dims[l]
        lane = iota((B, LANES), 1)
        above, below = zr[k, 0, first:first + B, :], zr[k, 1, first:first + B, :]
        for i in range(A):
            held = fields[l][k, DEPTH + i, TOP:TOP + B, :]
            held = jnp.where(lane // DEPTH == C // DEPTH, turn(above, C - DEPTH * i), held)
            fields[l][k, DEPTH + i, TOP:TOP + B, :] = jnp.where(
                lane >= LANES - DEPTH, turn(below, -DEPTH - DEPTH * (A + i)), held)

    half_row = LANES // 2
    starts = [sum(dims[i][1] for i in range(l)) for l in range(HALOED)]

    def own_row(k):
        lane = iota((1, LANES), 1)
        out, total = jnp.zeros((1, LANES), jnp.float32), None
        for i in range(CA):
            for j in range(CB):
                part = None
                for a in (0, 1):
                    for b in (0, 1):
                        y = TOP + 2 * j + b
                        one = fields[HALOED - 1][k, DEPTH + 2 * i + a, y:y + 1, :]
                        part = one if part is None else part + one
                part = halve(part, CC)
                out = jnp.where(lane // CC == i * CB + j, part, out)
                total = part if total is None else total + part
        return jnp.where((lane >= cells * CC) & (lane < cells * CC + CD), halve(total, CD), out)

    def coarse(k):
        rows = cr[k, :, 0, :]
        lane, row = iota((n, LANES), 1), iota((n, LANES), 0)
        parts = [jnp.where(lane // CC == row % nz, take(rows, cell * CC + lane % CC), 0.0) for cell in range(cells)]
        parts.append(jnp.where(lane // CD == row % nz, take(rows, cells * CC + lane % CD), 0.0))
        out = jnp.dot(pmat[...], jnp.concatenate(parts, axis=0), precision=HIGH, preferred_element_type=jnp.float32)
        out = out.reshape(-1, ROWS, LANES)
        last = smooth_whole(out[nx * CA:], ny, nz * CD, HALOED + 1)
        spread_y(last, spread)
        grown = take(spread[0:nx, 0:ROWS, :], iota((8, LANES), 1) // 2)
        whole = twice(grown) + smooth_whole(out[:nx * CA], ny * CB, nz * CC, HALOED)
        wref[DEPTH // 2:DEPTH // 2 + nx * CA, :, :] = whole

    def precondition(k, z, extra):
        start_all(main_copies(k))
        lane = iota((8, LANES), 1)
        for l in range(HALOED - 1):
            A, B, C = dims[l + 1]
            coarser = jnp.where(iota((1, 1, LANES), 2) < C, halve(fold_xy(own(fields[l], l, k)), LANES // 2), 0.0)
            fields[l + 1][k, DEPTH:DEPTH + A, TOP:TOP + B, :] = coarser
            pack_level(k, l + 1, starts[l + 1])
        pack_slab(k)
        start_all(z_copies(k))
        mine = own_row(k) if extra is None else jnp.where(iota((1, LANES), 1) < half_row, own_row(k), extra)
        cs[k] = mine
        cr[k, me] = mine
        to_all(cs.at[k], cr.at[k], csend.at[k], crecv.at[k])
        for s in range(1, SWEEPS):
            sweep_inside(after[0][s - 2] if s > 1 else g0.at[k], g0.at[k], after[0][s - 1], s)
        wait_all(z_copies(k))
        unpack_slab(k)
        for l in range(1, HALOED):
            unpack_level(k, l, starts[l])
        start_more(k)
        wait_all(main_copies(k))
        for s in range(1, SWEEPS):
            sweep_rim(after[0][s - 2] if s > 1 else g0.at[k], g0.at[k], after[0][s - 1], s)
        all_done(cr.at[k], crecv.at[k])
        coarse(k)
        A, B, C = dims[HALOED - 1]
        spread_y(wref[pl.ds(at[0] * CA, CA + DEPTH)], wide, DEPTH)
        part = wide[:, 0:2 * ROWS, :]
        for j in range(1, ny):
            part = jnp.where(at[1] == j, wide[:, j * B:j * B + 2 * ROWS, :], part)
        source = (wrapped(lane) >> 1) + at[2] * CC
        inside = (source >= 0) & (source < CC * nz)
        part = take(part, jnp.where(inside, source, 0))
        part = jnp.where(inside[0:1][None], part, 0.0)
        part = twice(part)[DEPTH - 1:DEPTH + A + 1, 0:B + 2 * DEPTH]
        wait_more(k)
        for s in range(1, SWEEPS):
            sweep_slab(after[HALOED][s - 2] if s > 1 else gs.at[k], gs.at[k], after[HALOED][s - 1])
            for l in range(1, HALOED):
                sweep(l, after[l][s - 2] if s > 1 else fields[l].at[k], fields[l].at[k], after[l][s - 1], s)
        for l in range(HALOED - 1, 0, -1):
            A, B, C = dims[l]
            end = after[l][SWEEPS - 2][DEPTH - 1:DEPTH + A + 1, TOP - DEPTH:TOP + B + DEPTH, :]
            full = end * (4.0 ** l / 9.0) + part
            if l > 1:
                spread_y(take(full, (wrapped(lane) >> 1) & (LANES - 1)), spread)
                part = twice(spread[0:A + 2, DEPTH:DEPTH + 2 * B + 2 * DEPTH, :])[1:2 * A + 3]
            else:
                spread_y(take(full, lane // 2), pd)
                spread_y(take(full, jnp.where(lane == 0, LANES - 1, C)), pe)
        low, rows = TOP - DEPTH, Y + 2 * DEPTH
        slab = after[HALOED][SWEEPS - 2]
        spot = iota((rows, LANES), 1) % SPAN
        for g in range(groups + 2):
            s = slab[g, low:low + rows, :]
            sc[g] = jnp.where(spot < quarter, s, turn(s, -half))
            sd[g] = jnp.where(spot <= quarter, s, turn(s, quarter + 1 - (3 * quarter - 1)))
        lane = iota((rows, LANES), 1)
        near = (lane < DEPTH - 1) | (lane > LANES - DEPTH)
        end = after[0][SWEEPS - 2]
        for p in range(DEPTH - 1, DEPTH + X + 1):
            g, i = p // PER, p % PER
            f = jnp.where(near, turn(sc[g], -quarter - SPAN * i), end[p, low:low + rows, :])
            z[p, low:low + rows, :] = f * (1.0 / 9.0) + pd[(p - DEPTH + 2) // 2, low:low + rows, :]

    def around(ref, p):
        mid = ref[p, TOP:TOP + Y, :]
        total = ref[p - 1, TOP:TOP + Y, :] + ref[p + 1, TOP:TOP + Y, :]
        return mid, total + ref[p, TOP - 1:TOP - 1 + Y, :] + ref[p, TOP + 1:TOP + 1 + Y, :]

    lane = iota((Y, LANES), 1)
    first, last = lane == 0, lane == LANES - 1

    def operator(z, p):
        mid, total = around(z, p)
        g, i = p // PER, p % PER
        ghost = turn(sd[g, DEPTH:DEPTH + Y, :], LANES - 1 - quarter - SPAN * i) * (1.0 / 9.0)
        ghost = ghost + pe[(p - DEPTH + 2) // 2, TOP:TOP + Y, :]
        total = total + jnp.where(first, ghost, turn(mid, 1))
        total = total + jnp.where(last, ghost, turn(mid, -1))
        return mid, 6.0 * mid - total

    load_x.wait()
    out = jnp.zeros((Y, LANES), jnp.float32)
    for i in range(X):
        out = jnp.where(lane // 2 == i, turn(ux[1 + i, TOP:TOP + Y, :], 2 * i + 1), out)
    ze[...] = out
    pl.semaphore_wait(barrier, n - 1)
    start_all(face_copies())
    load_b.wait()
    for i in range(X):
        mid, total = around(ux, 1 + i)
        total = total + jnp.where(first, 0.0, turn(mid, 1))
        total = total + jnp.where(last, 0.0, turn(mid, -1))
        g0[0, DEPTH + i, TOP:TOP + Y, :] = bb[i] - (6.0 * mid - total)
    wait_all(face_copies())
    for i, side in ((0, 1), (X - 1, 0)):
        here = (0, DEPTH + i, slice(TOP, TOP + Y))
        g0[here] = g0[here] + xg[side]
    for j, side in ((0, 1), (Y - 1, 0)):
        here = (0, slice(DEPTH, DEPTH + X), slice(TOP + j, TOP + j + 1))
        g0[here] = g0[here] + yg[side]
    ghosts = jnp.where(lane % 2 == 0, turn(zi[1], -1), turn(zi[0], 1))
    for i in range(X):
        here = (0, DEPTH + i, slice(TOP, TOP + Y))
        g0[here] = g0[here] + jnp.where(first | last, turn(ghosts, -2 * i - 1), 0.0)

    def sums_of(a, b):
        lane = iota((1, LANES), 1)
        pair = jnp.concatenate([jnp.sum(a, axis=0, keepdims=True), jnp.sum(b, axis=0, keepdims=True)], axis=0)
        pair = pair + turn(pair, LANES // 2)
        pair = pair + turn(pair, LANES // 4)
        return jnp.where(lane < 3 * LANES // 4, pair[0:1], pair[1:2])

    def ratio(rows):
        lane = iota((1, LANES), 1)
        row = jnp.sum(rows, axis=0, keepdims=True)
        upper_half = jnp.where(lane >= 3 * LANES // 4, row, 0.0)
        lower_half = jnp.where((lane >= half_row) & (lane < 3 * LANES // 4), row, 0.0)
        return jnp.sum(lower_half, axis=1, keepdims=True) / jnp.sum(upper_half, axis=1, keepdims=True)

    nothing = jnp.zeros((Y, LANES), jnp.float32)
    precondition(0, z0, None)
    rz, zw = nothing, nothing
    for i in range(X):
        mid, image = operator(z0, DEPTH + i)
        g0[1, DEPTH + i, TOP:TOP + Y, :] = image
        rz = rz + g0[0, DEPTH + i, TOP:TOP + Y, :] * mid
        zw = zw + mid * image
    precondition(1, z1, sums_of(rz, zw))
    alpha = ratio(cr[1, :, 0, :])
    rz, zw = nothing, nothing
    for i in range(X):
        mid, image = operator(z1, DEPTH + i)
        here = (DEPTH + i, slice(TOP, TOP + Y))
        before, w = z0[here], g0[(1,) + here]
        r = g0[(0,) + here] - alpha * w
        z = before - alpha * mid
        w = w - alpha * image
        rz = rz + r * z
        zw = zw + z * w
        sol_ref[i] = ux[1 + i, TOP:TOP + Y, :] + alpha * before
        z_ref[i] = z
        res_ref[i] = r
        w_ref[i] = w
    sums = sums_of(rz, zw)
    ds[...] = sums
    dr[me] = sums
    to_all(ds, dr, dsend.at[0], drecv.at[0])
    sent_all(face_copies())
    sent_around()
    for k in range(STEPS):
        all_done(cr.at[k], csend.at[k])
    all_done(dr, dsend.at[0])
    all_done(dr, drecv.at[0])
    alpha_ref[...] = jnp.broadcast_to(ratio(dr[:, 0, :]), alpha_ref.shape)


def finish(base, z, r, w, alpha, sol, res, sol_out, res_out, sem):
    X = base.shape[0]
    size = X // PARTS
    a = alpha[0:1, 0:1][None]
    copies = []
    for part in range(PARTS):
        here = slice(part * size, (part + 1) * size)
        sol_out[here] = base[here] + a * z[here]
        res_out[here] = r[here] - a * w[here]
        for i, (src, dst) in enumerate(((sol_out, sol), (res_out, res))):
            copies.append(pltpu.make_async_copy(src.at[here], dst.at[here], sem.at[i, part]))
            copies[-1].start()
    for copy in copies:
        copy.wait()


def solution(mesh):
    sizes = tuple(mesh.shape[a] for a in AXES)
    n = sizes[0] * sizes[1] * sizes[2]

    def run(right_side, guess):
        X, Y, Z = block = guess.shape
        assert Z == LANES and PER == DEPTH and X % PER == 0 and X * DEPTH <= LANES
        dims = [tuple(d >> l for d in block) for l in range(LEVELS)]
        f32 = jnp.float32
        vm = lambda *s: pltpu.VMEM(s, f32)
        ext = [(dims[l][0] + 2 * DEPTH, dims[l][1] + 2 * TOP, LANES) for l in range(HALOED)]
        slab = (X // PER + 2, Y + 2 * TOP, LANES)
        tall = [(dims[l][1] + 2 * DEPTH, LANES) for l in range(HALOED)]
        CA, CB, CC = dims[HALOED]
        assert dims[HALOED + 1][:2] == (1, 1) and sizes[1] * CB <= ROWS and CA * CB * CC + CC // 2 <= LANES // 2
        zrows = sum(dims[l][1] for l in range(HALOED))
        dma = lambda *s: pltpu.SemaphoreType.DMA(s)
        scratch = [
            vm(X + 2, Y + 2 * TOP, LANES), vm(*block),
            *(vm(STEPS, *e) for e in ext), vm(STEPS, *slab),
            *(vm(*e) for e in ext + [slab] for _ in range(SWEEPS - 1)),
            vm(*ext[0]), vm(*ext[0]),
            vm(slab[0], *tall[0]), vm(slab[0], *tall[0]),
            vm(dims[1][0] + 2, 2 * tall[1][0], LANES), vm(dims[1][0] + 2, 2 * tall[1][0], LANES),
            *(vm(*t) for t in tall), vm(*tall[0]),
            vm((CA + 1) * sizes[0] * ROWS, (CA * CB + 1) * n),
            vm(CA * sizes[0] + DEPTH, ROWS, LANES),
            vm(CA + DEPTH, 4 * ROWS, LANES),
            vm(X // 2, Y, LANES), vm(X // 2, 2 * Y, LANES),
            vm(2, Y, LANES), vm(2, X, 1, LANES), vm(Y, LANES), vm(2, Y, LANES),
            vm(STEPS, 2, zrows, LANES), vm(STEPS, 2, zrows, LANES),
            vm(STEPS, 1, LANES), vm(STEPS, n, 1, LANES),
            vm(1, LANES), vm(n, 1, LANES), vm(3 * STEPS * DEPTH * max(X, Y), LANES),
            dma(2), dma(6), dma(6), dma(2), dma(STEPS, 2),
            dma(8), dma(STEPS, 8), dma(STEPS, 8),
            dma(STEPS), dma(STEPS), dma(1), dma(1),
        ]
        whole = pltpu.VMEM(block, f32)
        base, z, r, w, alpha = pl.pallas_call(
            functools.partial(kernel, sizes, block),
            out_shape=(whole, whole, whole, whole, pltpu.VMEM((8, LANES), f32)),
            in_specs=[pl.BlockSpec(memory_space=pl.ANY)] * 2,
            out_specs=[pl.BlockSpec(memory_space=pltpu.VMEM)] * 5,
            scratch_shapes=scratch,
            compiler_params=pltpu.CompilerParams(collective_id=0, has_side_effects=True),
        )(right_side, guess)
        inner = [pltpu.with_memory_space_constraint(v, pltpu.VMEM) for v in (base, z, r, w, alpha)]
        out = jax.ShapeDtypeStruct(block, f32)
        return tuple(pl.pallas_call(
            finish,
            out_shape=(out, out),
            in_specs=[pl.BlockSpec(memory_space=pltpu.VMEM)] * 5,
            out_specs=[pl.BlockSpec(memory_space=pl.ANY)] * 2,
            scratch_shapes=[vm(*block), vm(*block), dma(2, PARTS)],
        )(*inner))

    spec = P(*AXES)
    return jax.shard_map(run, mesh=mesh, in_specs=(spec, spec), out_specs=(spec, spec), check_vma=False)
```

```python
import functools

import jax
import jax.numpy as jnp
from jax import lax
from jax.experimental import pallas as pl
from jax.experimental.pallas import tpu as pltpu
from jax.sharding import PartitionSpec as P

LEVELS = 6
SWEEPS = 4
STEPS = 2
HALOED = 4
AXES = ("gx", "gy", "gz")
LANES = 128
TOP = 8
DEPTH = SWEEPS
SPAN = 8 * DEPTH
PER = LANES // SPAN
PARTS = 4
MESH = pl.DeviceIdType.MESH
HIGH = lax.Precision.HIGHEST
ROWS = 8
ALL = [(a, b, c) for c in (-1, 1, 0) for a in (0, -1, 1) for b in (0, -1, 1) if (a, b, c) != (0, 0, 0)]
AROUND = [(a, b) for a in (-1, 0, 1) for b in (-1, 0, 1) if (a, b) != (0, 0)]
FACES = [(d, s) for d in range(3) for s in (-1, 1)]


def iota(shape, dim):
    return lax.broadcasted_iota(jnp.int32, shape, dim)


def take(x, index):
    if x.ndim == 3:
        return jnp.stack([take(x[i], index) for i in range(x.shape[0])])
    rows = x.shape[0]
    more = -rows % 8
    if rows == 1:
        x = jnp.broadcast_to(x, (8, LANES))
    elif more:
        x = jnp.concatenate([x, jnp.zeros((more, LANES), x.dtype)], axis=0)
    index = jnp.broadcast_to(index[:1], x.shape)
    out = jnp.take_along_axis(x, index, axis=1, mode="promise_in_bounds")
    return out[:rows] if more else out


def wrapped(lane):
    return jnp.where(lane >= LANES - DEPTH, lane - LANES, lane)


def halve(x, width):
    lane = iota((8, LANES), 1)
    return take(x + turn(x, -1), 2 * (lane % width)) * 0.125


def turn(x, shift):
    shift = shift % LANES
    return pltpu.roll(x, shift, x.ndim - 1) if shift else x


def kernel(sizes, block, b_hbm, x_hbm, sol_ref, z_ref, res_ref, w_ref, alpha_ref, *rest):
    (ux, bb, g0, g1, g2, g3, gs, h1, h2, h3, hs, f0a, f0b, f0c, f1a, f1b, f1c, f2a, f2b, f2c, f3a, f3b, f3c, fsa, fsb, fsc,
     z0, z1, sc, sd, pd, pe, m0, m1, m2, m3, ms, pmat, wref, wide, fold, spread, xg, yg, ze, zi, zq0, zq1, zq2, zr0, zr1, zr2, es, zx, xs, xf, cs, cr, ds, dr, blank,
     isem, xsend, xrecv, fsend, frecv, send, mrecv, csend, crecv, dsend, drecv) = rest
    nx, ny, nz = sizes
    n = nx * ny * nz
    at = tuple(lax.axis_index(a) for a in AXES)
    me = (at[0] * ny + at[1]) * nz + at[2]
    dims = [tuple(d >> l for d in block) for l in range(LEVELS)]
    X, Y, Z = block
    fields = (g0, g1, g2, g3)
    after = ((f0a, f0b, f0c), (f1a, f1b, f1c), (f2a, f2b, f2c), (f3a, f3b, f3c), (fsa, fsb, fsc))
    masks = (m0, m1, m2, m3)
    whole = (None, h1, h2, h3, hs)
    groups = X // PER
    lower = [at[d] > 0 for d in range(3)]
    upper = [at[d] < sizes[d] - 1 for d in range(3)]
    inlow = [jnp.where(c, 1.0, 0.0) for c in lower]
    inup = [jnp.where(c, 1.0, 0.0) for c in upper]

    load_x = pltpu.make_async_copy(x_hbm, ux.at[1:X + 1, TOP:TOP + Y], isem.at[0])
    load_b = pltpu.make_async_copy(b_hbm, bb, isem.at[1])
    load_x.start()
    load_b.start()

    def others():
        out = []
        for b in range(ny - 1, -1, -1):
            for c in range(nz - 1, -1, -1):
                for a in range(nx):
                    if b or c:
                        first = jnp.where(at[0] < nx // 2, nx - 1 - a, a)
                    elif a:
                        first = lax.rem(at[0] + a, nx)
                    else:
                        continue
                    out.append((first, lax.rem(at[1] + b, ny), lax.rem(at[2] + c, nz)))
        return out

    barrier = pltpu.get_barrier_semaphore()
    for target in others():
        pl.semaphore_signal(barrier, inc=1, device_id=target, device_id_type=MESH)

    def outside(dim, side):
        for l in range(HALOED + 1):
            A, B = (groups if l == HALOED else dims[l][0]), (Y if l == HALOED else dims[l][1])
            d, ref = (1, gs) if l == HALOED else (DEPTH, fields[l])
            for k in range(STEPS):
                if dim == 0:
                    a = A + d if side else 0
                    ref[k, a:a + d, TOP - DEPTH:TOP + B + DEPTH, :] = jnp.zeros((d, B + 2 * DEPTH, LANES), jnp.float32)
                else:
                    a = TOP + B if side else TOP - DEPTH
                    ref[k, :, a:a + DEPTH, :] = jnp.zeros((A + 2 * d, DEPTH, LANES), jnp.float32)

    far = (zr0, zr1, zr2, zx, xf)

    def nothing_in(ref):
        ref[...] = jnp.zeros(ref.shape, jnp.float32)

    for side in (0, 1):
        for dim in range(2):
            @pl.when(jnp.logical_not((upper if side else lower)[dim]))
            def _(dim=dim, side=side):
                outside(dim, side)
                nothing_in((xg, yg)[dim].at[1 - side])
                for ref in far if dim else ():
                    head = (slice(None),) * (len(ref.shape) - 2)
                    a = ref.shape[-2] - DEPTH if side else 0
                    nothing_in(ref.at[head + (slice(a, a + DEPTH),)])
                if dim == 0:
                    nothing_in(zx.at[:, :, side])
                    nothing_in(xf.at[:, side])
        @pl.when(jnp.logical_not((upper if side else lower)[2]))
        def _(side=side):
            nothing_in(zi.at[side])
            for ref in far[:4]:
                nothing_in(ref.at[:, 1 - side])

    ux[:, TOP - 1:TOP, :] = jnp.zeros((X + 2, 1, LANES), jnp.float32)
    ux[:, TOP + Y:TOP + Y + 1, :] = jnp.zeros((X + 2, 1, LANES), jnp.float32)
    ux[0, TOP:TOP + Y, :] = jnp.zeros((Y, LANES), jnp.float32)
    ux[X + 1, TOP:TOP + Y, :] = jnp.zeros((Y, LANES), jnp.float32)
    wref[...] = jnp.zeros_like(wref)
    wide[...] = jnp.zeros_like(wide)

    def mask(rows, z, depth_z):
        y = iota((rows + 2 * DEPTH, LANES), 0) - DEPTH
        part = jnp.where(y < 0, inlow[1], jnp.where(y >= rows, inup[1], 1.0))
        return part * jnp.where(z < 0, inlow[2], jnp.where(z >= depth_z, inup[2], 1.0)) * (1.0 / 9.0)

    for l in range(HALOED):
        lane = iota((dims[l][1] + 2 * DEPTH, LANES), 1)
        masks[l][...] = mask(dims[l][1], lane if l == 0 else wrapped(lane), dims[l][2])
    CA, CB, CC = dims[HALOED]
    CD = dims[HALOED + 1][2]
    cells = CA * CB
    row, column = iota(pmat.shape, 0), iota(pmat.shape, 1)
    cell, device = column // n, column % n
    plane, line = row // ROWS, row % ROWS
    dx, dy = device // (ny * nz), device // nz % ny
    fits = (cell < cells) & (plane == dx * CA + cell // CB) & (line == dy * CB + cell % CB)
    fits = fits | ((cell == cells) & (plane == nx * CA + dx) & (line == dy))
    pmat[...] = jnp.where(fits, 1.0, 0.0)
    lane = iota((Y + 2 * DEPTH, LANES), 1) % SPAN
    ms[...] = mask(Y, jnp.where(lane < SPAN // 2, lane + Z - SPAN // 4, lane - 3 * SPAN // 4), Z)

    def face_copies():
        out = []
        for i, (d, s) in enumerate(FACES):
            target = list(at)
            target[d] = at[d] + s
            into = 1 if s > 0 else 0
            if d == 0:
                src, dst = ux.at[X if s > 0 else 1, TOP:TOP + Y], xg.at[into]
            elif d == 1:
                a = TOP + Y - 1 if s > 0 else TOP
                src, dst = ux.at[1:X + 1, a:a + 1], yg.at[into]
            else:
                src, dst = ze, zi.at[0 if s > 0 else 1]
            copy = pltpu.make_async_remote_copy(
                src_ref=src, dst_ref=dst, send_sem=xsend.at[i], recv_sem=xrecv.at[i],
                device_id=tuple(target), device_id_type=MESH,
            )
            out.append((copy, upper[d] if s > 0 else lower[d], lower[d] if s > 0 else upper[d]))
        return out

    def span(step, depth, start, own, other):
        if step > 0:
            return (start + own - depth, depth), (start - depth, depth)
        if step < 0:
            return (start, depth), (start + own, depth)
        return (start, own), (start, own)

    def around_copies(ref, k, depth, planes, rows, rsem):
        out = []
        for i, (dx, dy) in enumerate(AROUND):
            (sx, lx), (tx, _) = span(dx, depth, depth, planes, None)
            (sy, ly), (ty, _) = span(dy, DEPTH, TOP, rows, None)
            copy = pltpu.make_async_remote_copy(
                src_ref=ref.at[k, sx:sx + lx, sy:sy + ly], dst_ref=ref.at[k, tx:tx + lx, ty:ty + ly],
                send_sem=send.at[i], recv_sem=rsem.at[k, i],
                device_id=(at[0] + dx, at[1] + dy, at[2]), device_id_type=MESH,
            )
            to, fro = None, None
            for d, s in ((0, dx), (1, dy)):
                if s:
                    a, b = (upper[d], lower[d]) if s > 0 else (lower[d], upper[d])
                    to = a if to is None else jnp.logical_and(to, a)
                    fro = b if fro is None else jnp.logical_and(fro, b)
            out.append((copy, to, fro, lx * ly))
        return out

    def main_copies(k):
        return around_copies(g0, k, DEPTH, X, Y, mrecv)

    def rows_of(dy, rows):
        if dy > 0:
            return pl.ds(rows - DEPTH, DEPTH), pl.ds(0, DEPTH), DEPTH
        if dy < 0:
            return pl.ds(0, DEPTH), pl.ds(rows + DEPTH, DEPTH), DEPTH
        return pl.ds(0, rows), pl.ds(DEPTH, rows), rows

    def every(conds):
        out = None
        for cond in conds:
            out = cond if out is None else jnp.logical_and(out, cond)
        return out

    def far_copies(k):
        out = []
        for i, (dx, dy, dz) in enumerate(ALL):
            step = (dx, dy, dz)
            to = every([(upper if t > 0 else lower)[d] for d, t in enumerate(step) if t])
            fro = every([(lower if t > 0 else upper)[d] for d, t in enumerate(step) if t])
            from_x, into_x = (1, 0) if dx > 0 else (0, 1)
            side = 1 if dz > 0 else 0
            pairs = []
            if dz and dx:
                a, b, c = rows_of(dy, Y)
                pairs.append((es.at[k, from_x, a], zx.at[k, side, into_x, b], c))
            elif dz:
                for src, dst in ((zq0.at[k, side], zr0), (zq1.at[k], zr1), (zq2.at[k], zr2)):
                    a, b, c = rows_of(dy, src.shape[0])
                    pairs.append((src.at[a], dst.at[k, side, b], c))
            else:
                arrays = [(gs, 1, groups, Y)]
                if dx:
                    a, b, c = rows_of(dy, dims[1][1])
                    pairs.append((xs.at[k, from_x, :, a], xf.at[k, into_x, :, b], DEPTH * c))
                else:
                    arrays += [(fields[l], DEPTH, dims[l][0], dims[l][1]) for l in range(1, HALOED)]
                for ref, depth, planes, rows in arrays:
                    (sx, lx), (tx, _) = span(dx, depth, depth, planes, None)
                    (sy, ly), (ty, _) = span(dy, DEPTH, TOP, rows, None)
                    pairs.append((ref.at[k, sx:sx + lx, sy:sy + ly], ref.at[k, tx:tx + lx, ty:ty + ly], lx * ly))
            copies = [pltpu.make_async_remote_copy(
                src_ref=src, dst_ref=dst, send_sem=fsend.at[i], recv_sem=frecv.at[k, i],
                device_id=(at[0] + dx, at[1] + dy, at[2] + dz), device_id_type=MESH,
            ) for src, dst, _ in pairs]
            out.append((copies, to, fro, sum(c for _, _, c in pairs)))
        return out

    def lines(copies):
        return sum(entry[3] for entry in copies)

    def bytes_done(count, sem):
        part = blank.at[pl.ds(0, count)]
        pltpu.make_async_copy(part, part, sem).wait()

    def start_all(copies):
        for copy, cond, *_ in copies:
            pl.when(cond)(copy.start)

    def wait_all(copies):
        for copy, _, cond, *_ in copies:
            pl.when(cond)(copy.wait_recv)

    def sent_all(copies):
        for copy, cond, *_ in copies:
            pl.when(cond)(copy.wait_send)

    def start_far(k):
        for copies, to, _, _ in far_copies(k):
            @pl.when(to)
            def _(copies=copies):
                for copy in copies:
                    copy.start()

    def wait_far(k):
        for i, (_, _, fro, count) in enumerate(far_copies(k)):
            pl.when(fro)(lambda i=i, count=count: bytes_done(count, frecv.at[k, i]))

    def sent_around():
        for i, (_, to, _, count) in enumerate(far_copies(0)):
            pl.when(to)(lambda i=i, count=count: bytes_done(STEPS * count, fsend.at[i]))
        for i, entry in enumerate(main_copies(0)):
            pl.when(entry[1])(lambda i=i, entry=entry: bytes_done(STEPS * entry[3], send.at[i]))

    def to_all(src, dst, s_sem, r_sem):
        for target in others():
            pltpu.make_async_remote_copy(
                src_ref=src, dst_ref=dst.at[me], send_sem=s_sem, recv_sem=r_sem,
                device_id=target, device_id_type=MESH,
            ).start()

    def all_done(dst, sem):
        part = dst.at[pl.ds(0, n - 1)]
        pltpu.make_async_copy(part, part, sem).wait()

    def fold_xy(field):
        A, B, _ = field.shape
        pairs = field.reshape(A // 2, 2, B, LANES)
        fold[0:A // 2, 0:B, :] = pairs[:, 0] + pairs[:, 1]
        return fold[0:A // 2, pl.ds(0, B // 2, 2), :] + fold[0:A // 2, pl.ds(1, B // 2, 2), :]

    def spread_y(field, into, first=0):
        A, B, _ = field.shape
        into[0:A, pl.ds(first, B, 2), :] = field
        into[0:A, pl.ds(first + 1, B, 2), :] = field

    def twice(field):
        A, B, _ = field.shape
        return jnp.broadcast_to(field[:, None], (A, 2, B, LANES)).reshape(2 * A, B, LANES)

    def own(ref, l, k=None):
        A, B, _ = dims[l]
        return ref[(k,) * (k is not None) + (slice(DEPTH, DEPTH + A), slice(TOP, TOP + B))]

    def update(src, rhs, dst, a, c, low, rows, scale):
        at_rows = slice(low, low + rows)
        mid = src[a:a + c, at_rows, :]
        total = src[a - 1:a - 1 + c, at_rows, :] + src[a + 1:a + 1 + c, at_rows, :]
        total = total + src[a:a + c, low - 1:low - 1 + rows, :] + src[a:a + c, low + 1:low + 1 + rows, :]
        total = total + turn(mid, 1) + turn(mid, -1)
        dst[a:a + c, at_rows, :] = rhs[a:a + c, at_rows, :] + (3.0 * mid + total) * scale

    def pieces(a, b):
        return [(p, min(4, b - p)) for p in range(a, b, 4)]

    def sweep(l, src, rhs, dst, k):
        A, B, _ = dims[l]
        low, rows = TOP - DEPTH, B + 2 * DEPTH
        m = masks[l][...]
        update(src, rhs, dst, k, DEPTH - k, low, rows, m * inlow[0])
        for a, c in pieces(DEPTH, DEPTH + A):
            update(src, rhs, dst, a, c, low, rows, m)
        update(src, rhs, dst, DEPTH + A, DEPTH - k, low, rows, m * inup[0])

    def sweep_inside(src, rhs, dst, k):
        for a, c in pieces(DEPTH + k, DEPTH + X - k):
            update(src, rhs, dst, a, c, TOP + k, Y - 2 * k, 1.0 / 9.0)

    def sweep_rim(src, rhs, dst, k):
        low, rows = TOP - DEPTH, Y + 2 * DEPTH
        m = m0[...]
        update(src, rhs, dst, k, DEPTH - k, low, rows, m * inlow[0])
        update(src, rhs, dst, DEPTH, k, low, rows, m)
        update(src, rhs, dst, DEPTH + X - k, k, low, rows, m)
        update(src, rhs, dst, DEPTH + X, DEPTH - k, low, rows, m * inup[0])
        for start in (0, Y):
            edge = m0[start:start + 2 * DEPTH, :]
            for a, c in pieces(DEPTH + k, DEPTH + X - k):
                update(src, rhs, dst, a, c, low + start, 2 * DEPTH, edge)

    def sweep_slab(src, rhs, dst):
        low, rows = TOP - DEPTH, Y + 2 * DEPTH
        lane = iota((rows, LANES), 1)
        m = ms[...]
        for g in range(groups + 2):
            mid = src[g, low:low + rows, :]
            total = src[g, low - 1:low - 1 + rows, :] + src[g, low + 1:low + 1 + rows, :]
            total = total + turn(mid, 1) + turn(mid, -1)
            before = mid if g == 0 else jnp.where(lane >= LANES - SPAN, src[g - 1, low:low + rows, :], mid)
            behind = mid if g == groups + 1 else jnp.where(lane < SPAN, src[g + 1, low:low + rows, :], mid)
            total = total + turn(before, SPAN) + turn(behind, -SPAN)
            scale = m * inlow[0] if g == 0 else m * inup[0] if g == groups + 1 else m
            dst[g, low:low + rows, :] = rhs[g, low:low + rows, :] + (3.0 * mid + total) * scale

    def smooth_whole(rhs, depth_y, depth_z, l):
        A, B, _ = rhs.shape
        lane, row = iota(rhs.shape, 2), iota(rhs.shape, 1)
        e = rhs
        for _ in range(SWEEPS - 1):
            px, py = jnp.zeros((1, B, LANES), jnp.float32), jnp.zeros((A, 1, LANES), jnp.float32)
            total = jnp.concatenate([px, e[:-1]], axis=0) + jnp.concatenate([e[1:], px], axis=0)
            total = total + jnp.concatenate([py, e[:, :-1]], axis=1) + jnp.concatenate([e[:, 1:], py], axis=1)
            total = total + jnp.where(lane == 0, 0.0, turn(e, 1))
            total = total + jnp.where(lane == depth_z - 1, 0.0, turn(e, -1))
            e = rhs + jnp.where(row < depth_y, (3.0 * e + total) * (1.0 / 9.0), 0.0)
        return e * (4.0 ** l / 9.0)

    half, quarter = SPAN // 2, SPAN // 4

    def pack_slab(k):
        lane = iota((Y, LANES), 1)
        line, spot = lane // SPAN, lane % SPAN
        low = high = jnp.zeros((Y, LANES), jnp.float32)
        for g in range(groups):
            both = jnp.zeros((Y, LANES), jnp.float32)
            for i in range(PER):
                field = g0[k, DEPTH + g * PER + i, TOP:TOP + Y, :]
                both = jnp.where((line == i) & (spot < half), turn(field, SPAN * i + quarter), both)
            gs[k, g + 1, TOP:TOP + Y, :] = jnp.where(
                spot < quarter, both, jnp.where(spot >= 3 * quarter, turn(both, half), 0.0))
            here = spot // DEPTH == g
            low = jnp.where(here, turn(both, DEPTH * g - quarter), low)
            high = jnp.where(here, turn(both, DEPTH * g - quarter + DEPTH), high)
        zq0[k, 0] = low
        zq0[k, 1] = high
        for side, j in ((0, 0), (1, groups - 1)):
            es[k, side] = put(0, low, j, 0) + put(0, high, j, 1)

    def slots(l):
        return (0, 0, 0, dims[2][0] // DEPTH * 2)[l], dims[l][0] // DEPTH

    def put(l, x, source, target):
        lane = iota(x.shape, 1)
        return jnp.where(lane % SPAN // DEPTH == target, turn(x, DEPTH * (target - source)), 0.0)

    def pack_level(k, l):
        A, B, C = dims[l]
        base, many = slots(l)
        lane = iota((B, LANES), 1)
        line, slot = lane // SPAN, lane % SPAN // DEPTH
        out = jnp.zeros((B, LANES), jnp.float32)
        for i in range(A):
            field = fields[l][k, DEPTH + i, TOP:TOP + B, :]
            x, j = i % DEPTH, i // DEPTH
            lo, hi = base + j, base + many + j
            out = jnp.where((line == x) & (slot == lo), turn(field, SPAN * x + DEPTH * lo), out)
            out = jnp.where((line == x) & (slot == hi), turn(field, SPAN * x + DEPTH * hi - C + DEPTH), out)
        return out

    def pack_rest(k):
        one, two, three = [pack_level(k, l) for l in range(1, HALOED)]
        zq1[k] = one
        B1, B2, B3 = [dims[l][1] for l in range(1, HALOED)]
        zq2[k, 0:B2] = two
        for a in (0, B2 - B3):
            zq2[k, a:a + B3] = zq2[k, a:a + B3] + three
        for side in (0, 1):
            def edge(l, x):
                base, many = slots(l)
                j = many - 1 if side else 0
                return put(l, x, base + j, 2 * l) + put(l, x, base + many + j, 2 * l + 1)
            first, second, third = edge(1, one), edge(2, two), edge(3, three)
            for src, dst, size, part in (
                    (0, 0, B1 - DEPTH, first), (B1 - DEPTH, Y - DEPTH, DEPTH, first),
                    (0, 0, DEPTH, second), (B2 - DEPTH, Y - DEPTH, DEPTH, second),
                    (0, 0, DEPTH, third), (0, Y - DEPTH, DEPTH, third)):
                es[k, side, dst:dst + size] = es[k, side, dst:dst + size] + part[src:src + size]
            for x in range(DEPTH):
                p1, p2, p3 = [DEPTH + x + (dims[l][0] - DEPTH if side else 0) for l in range(1, HALOED)]
                xs[k, side, x] = g1[k, p1, TOP:TOP + B1, :]
                second = turn(g2[k, p2, TOP:TOP + B2, :], dims[1][2])
                third = turn(g3[k, p3, TOP:TOP + B3, :], dims[1][2] + dims[2][2])
                xs[k, side, x, 0:DEPTH] = xs[k, side, x, 0:DEPTH] + second[0:DEPTH] + third
                xs[k, side, x, B1 - DEPTH:B1] = xs[k, side, x, B1 - DEPTH:B1] + second[B2 - DEPTH:B2] + third

    def unpack_slab(k):
        low, rows = TOP - DEPTH, Y + 2 * DEPTH
        spot = iota((rows, LANES), 1) % SPAN
        for g in range(groups + 2):
            edge = 0 if g == 0 else 1 if g == groups + 1 else None
            if edge is None:
                above, below, up, down = zr0[k, 0], zr0[k, 1], g - 1, g - 1
            else:
                above, below, up, down = zx[k, 0, edge], zx[k, 1, edge], 0, 1
            held = gs[k, g, low:low + rows, :]
            held = jnp.where(spot // DEPTH == 2, turn(above, DEPTH * (2 - up)), held)
            hs[g, low:low + rows, :] = jnp.where(spot // DEPTH == 5, turn(below, DEPTH * (5 - down)), held)

    def unpack_level(k, l):
        A, B, C = dims[l]
        low, rows = TOP - DEPTH, B + 2 * DEPTH
        base, many = slots(l)
        lane = iota((rows, LANES), 1)

        def cut(ref, head):
            end = ref.shape[-2]
            tail = 0 if end == rows else (2 * DEPTH if B > DEPTH else DEPTH)
            a = ref[head + (slice(0, rows - tail),)]
            return jnp.concatenate([a, ref[head + (slice(end - tail, end),)]], axis=0) if tail else a

        ref = (None, zr1, zr2, zr2)[l]
        sides = [cut(ref, (k, 0)), cut(ref, (k, 1))]
        edges = [[cut(zx, (k, side, e)) for side in (0, 1)] for e in (0, 1)]
        start = sum(dims[i][2] for i in range(1, l))
        for p in range(A + 2 * DEPTH):
            edge = 0 if p < DEPTH else 1 if p >= DEPTH + A else None
            x, j = p % DEPTH, p // DEPTH - 1
            if edge is None:
                held = fields[l][k, p, low:low + rows, :]
                (above, below), up, down = sides, base + j, base + many + j
            else:
                held = jnp.where(lane < C, turn(cut(xf, (k, edge, x)), -start), 0.0)
                (above, below), up, down = edges[edge], 2 * l, 2 * l + 1
            held = jnp.where(lane // DEPTH == C // DEPTH, turn(above, C - SPAN * x - DEPTH * up), held)
            whole[l][p, low:low + rows, :] = jnp.where(
                lane >= LANES - DEPTH, turn(below, -DEPTH - SPAN * x - DEPTH * down), held)

    half_row = LANES // 2
    def own_row(k):
        lane = iota((1, LANES), 1)
        out, total = jnp.zeros((1, LANES), jnp.float32), None
        for i in range(CA):
            for j in range(CB):
                part = None
                for a in (0, 1):
                    for b in (0, 1):
                        y = TOP + 2 * j + b
                        one = fields[HALOED - 1][k, DEPTH + 2 * i + a, y:y + 1, :]
                        part = one if part is None else part + one
                part = halve(part, CC)
                out = jnp.where(lane // CC == i * CB + j, part, out)
                total = part if total is None else total + part
        return jnp.where((lane >= cells * CC) & (lane < cells * CC + CD), halve(total, CD), out)

    def coarse(k):
        rows = cr[k, :, 0, :]
        lane, row = iota((n, LANES), 1), iota((n, LANES), 0)
        parts = [jnp.where(lane // CC == row % nz, take(rows, cell * CC + lane % CC), 0.0) for cell in range(cells)]
        parts.append(jnp.where(lane // CD == row % nz, take(rows, cells * CC + lane % CD), 0.0))
        out = jnp.dot(pmat[...], jnp.concatenate(parts, axis=0), precision=HIGH, preferred_element_type=jnp.float32)
        out = out.reshape(-1, ROWS, LANES)
        last = smooth_whole(out[nx * CA:], ny, nz * CD, HALOED + 1)
        spread_y(last, spread)
        grown = take(spread[0:nx, 0:ROWS, :], iota((8, LANES), 1) // 2)
        wref[DEPTH // 2:DEPTH // 2 + nx * CA, :, :] = (
            twice(grown) + smooth_whole(out[:nx * CA], ny * CB, nz * CC, HALOED))

    def precondition(k, z, extra):
        start_all(main_copies(k))
        lane = iota((8, LANES), 1)
        for l in range(HALOED - 1):
            A, B, C = dims[l + 1]
            coarser = jnp.where(iota((1, 1, LANES), 2) < C, halve(fold_xy(own(fields[l], l, k)), LANES // 2), 0.0)
            fields[l + 1][k, DEPTH:DEPTH + A, TOP:TOP + B, :] = coarser
        pack_slab(k)
        pack_rest(k)
        start_far(k)
        mine = own_row(k) if extra is None else jnp.where(iota((1, LANES), 1) < half_row, own_row(k), extra)
        cs[k] = mine
        cr[k, me] = mine
        to_all(cs.at[k], cr.at[k], csend.at[k], crecv.at[k])
        for s in range(1, SWEEPS):
            sweep_inside(after[0][s - 2] if s > 1 else g0.at[k], g0.at[k], after[0][s - 1], s)
        wait_all(main_copies(k))
        for s in range(1, SWEEPS):
            sweep_rim(after[0][s - 2] if s > 1 else g0.at[k], g0.at[k], after[0][s - 1], s)
        wait_far(k)
        unpack_slab(k)
        for l in range(1, HALOED):
            unpack_level(k, l)
        for s in range(1, SWEEPS):
            sweep_slab(after[HALOED][s - 2] if s > 1 else hs, hs, after[HALOED][s - 1])
            for l in range(1, HALOED):
                sweep(l, after[l][s - 2] if s > 1 else whole[l], whole[l], after[l][s - 1], s)
        all_done(cr.at[k], crecv.at[k])
        coarse(k)
        A, B, C = dims[HALOED - 1]
        spread_y(wref[pl.ds(at[0] * CA, CA + DEPTH)], wide, DEPTH)
        part = wide[:, 0:2 * ROWS, :]
        for j in range(1, ny):
            part = jnp.where(at[1] == j, wide[:, j * B:j * B + 2 * ROWS, :], part)
        source = (wrapped(lane) >> 1) + at[2] * CC
        inside = (source >= 0) & (source < CC * nz)
        part = take(part, jnp.where(inside, source, 0))
        part = jnp.where(inside[0:1][None], part, 0.0)
        part = twice(part)[DEPTH - 1:DEPTH + A + 1, 0:B + 2 * DEPTH]
        for l in range(HALOED - 1, 0, -1):
            A, B, C = dims[l]
            end = after[l][SWEEPS - 2][DEPTH - 1:DEPTH + A + 1, TOP - DEPTH:TOP + B + DEPTH, :]
            full = end * (4.0 ** l / 9.0) + part
            if l > 1:
                spread_y(take(full, (wrapped(lane) >> 1) & (LANES - 1)), spread)
                part = twice(spread[0:A + 2, DEPTH:DEPTH + 2 * B + 2 * DEPTH, :])[1:2 * A + 3]
            else:
                spread_y(take(full, lane // 2), pd)
                spread_y(take(full, jnp.where(lane == 0, LANES - 1, C)), pe)
        low, rows = TOP - DEPTH, Y + 2 * DEPTH
        slab = after[HALOED][SWEEPS - 2]
        spot = iota((rows, LANES), 1) % SPAN
        for g in range(groups + 2):
            s = slab[g, low:low + rows, :]
            sc[g] = jnp.where(spot < quarter, s, turn(s, -half))
            sd[g] = jnp.where(spot <= quarter, s, turn(s, quarter + 1 - (3 * quarter - 1)))
        lane = iota((rows, LANES), 1)
        near = (lane < DEPTH - 1) | (lane > LANES - DEPTH)
        end = after[0][SWEEPS - 2]
        for p in range(DEPTH - 1, DEPTH + X + 1):
            g, i = p // PER, p % PER
            f = jnp.where(near, turn(sc[g], -quarter - SPAN * i), end[p, low:low + rows, :])
            z[p, low:low + rows, :] = f * (1.0 / 9.0) + pd[(p - DEPTH + 2) // 2, low:low + rows, :]

    def around(ref, p):
        mid = ref[p, TOP:TOP + Y, :]
        total = ref[p - 1, TOP:TOP + Y, :] + ref[p + 1, TOP:TOP + Y, :]
        return mid, total + ref[p, TOP - 1:TOP - 1 + Y, :] + ref[p, TOP + 1:TOP + 1 + Y, :]

    lane = iota((Y, LANES), 1)
    first, last = lane == 0, lane == LANES - 1

    def operator(z, p):
        mid, total = around(z, p)
        g, i = p // PER, p % PER
        ghost = turn(sd[g, DEPTH:DEPTH + Y, :], LANES - 1 - quarter - SPAN * i) * (1.0 / 9.0)
        ghost = ghost + pe[(p - DEPTH + 2) // 2, TOP:TOP + Y, :]
        total = total + jnp.where(first, ghost, turn(mid, 1))
        total = total + jnp.where(last, ghost, turn(mid, -1))
        return mid, 6.0 * mid - total

    load_x.wait()
    out = jnp.zeros((Y, LANES), jnp.float32)
    for i in range(X):
        out = jnp.where(lane // 2 == i, turn(ux[1 + i, TOP:TOP + Y, :], 2 * i + 1), out)
    ze[...] = out
    pl.semaphore_wait(barrier, n - 1)
    start_all(face_copies())
    load_b.wait()
    for i in range(X):
        mid, total = around(ux, 1 + i)
        total = total + jnp.where(first, 0.0, turn(mid, 1))
        total = total + jnp.where(last, 0.0, turn(mid, -1))
        g0[0, DEPTH + i, TOP:TOP + Y, :] = bb[i] - (6.0 * mid - total)
    wait_all(face_copies())
    for i, side in ((0, 1), (X - 1, 0)):
        here = (0, DEPTH + i, slice(TOP, TOP + Y))
        g0[here] = g0[here] + xg[side]
    for j, side in ((0, 1), (Y - 1, 0)):
        here = (0, slice(DEPTH, DEPTH + X), slice(TOP + j, TOP + j + 1))
        g0[here] = g0[here] + yg[side]
    ghosts = jnp.where(lane % 2 == 0, turn(zi[1], -1), turn(zi[0], 1))
    for i in range(X):
        here = (0, DEPTH + i, slice(TOP, TOP + Y))
        g0[here] = g0[here] + jnp.where(first | last, turn(ghosts, -2 * i - 1), 0.0)

    def sums_of(a, b):
        lane = iota((1, LANES), 1)
        pair = jnp.concatenate([jnp.sum(a, axis=0, keepdims=True), jnp.sum(b, axis=0, keepdims=True)], axis=0)
        pair = pair + turn(pair, LANES // 2)
        pair = pair + turn(pair, LANES // 4)
        return jnp.where(lane < 3 * LANES // 4, pair[0:1], pair[1:2])

    def ratio(rows):
        lane = iota((1, LANES), 1)
        row = jnp.sum(rows, axis=0, keepdims=True)
        upper_half = jnp.where(lane >= 3 * LANES // 4, row, 0.0)
        lower_half = jnp.where((lane >= half_row) & (lane < 3 * LANES // 4), row, 0.0)
        return jnp.sum(lower_half, axis=1, keepdims=True) / jnp.sum(upper_half, axis=1, keepdims=True)

    nothing = jnp.zeros((Y, LANES), jnp.float32)
    precondition(0, z0, None)
    rz, zw = nothing, nothing
    for i in range(X):
        mid, image = operator(z0, DEPTH + i)
        g0[1, DEPTH + i, TOP:TOP + Y, :] = image
        rz = rz + g0[0, DEPTH + i, TOP:TOP + Y, :] * mid
        zw = zw + mid * image
    precondition(1, z1, sums_of(rz, zw))
    alpha = ratio(cr[1, :, 0, :])
    rz, zw = nothing, nothing
    for i in range(X):
        mid, image = operator(z1, DEPTH + i)
        here = (DEPTH + i, slice(TOP, TOP + Y))
        before, w = z0[here], g0[(1,) + here]
        r = g0[(0,) + here] - alpha * w
        z = before - alpha * mid
        w = w - alpha * image
        rz = rz + r * z
        zw = zw + z * w
        sol_ref[i] = ux[1 + i, TOP:TOP + Y, :] + alpha * before
        z_ref[i] = z
        res_ref[i] = r
        w_ref[i] = w
    sums = sums_of(rz, zw)
    ds[...] = sums
    dr[me] = sums
    to_all(ds, dr, dsend.at[0], drecv.at[0])
    sent_all(face_copies())
    sent_around()
    for k in range(STEPS):
        all_done(cr.at[k], csend.at[k])
    all_done(dr, dsend.at[0])
    all_done(dr, drecv.at[0])
    alpha_ref[...] = jnp.broadcast_to(ratio(dr[:, 0, :]), alpha_ref.shape)


def finish(base, z, r, w, alpha, sol, res, sol_out, res_out, sem):
    X = base.shape[0]
    size = X // PARTS
    a = alpha[0:1, 0:1][None]
    copies = []
    for part in range(PARTS):
        here = slice(part * size, (part + 1) * size)
        sol_out[here] = base[here] + a * z[here]
        res_out[here] = r[here] - a * w[here]
        for i, (src, dst) in enumerate(((sol_out, sol), (res_out, res))):
            copies.append(pltpu.make_async_copy(src.at[here], dst.at[here], sem.at[i, part]))
            copies[-1].start()
    for copy in copies:
        copy.wait()


def solution(mesh):
    sizes = tuple(mesh.shape[a] for a in AXES)
    n = sizes[0] * sizes[1] * sizes[2]

    def run(right_side, guess):
        X, Y, Z = block = guess.shape
        assert Z == LANES and PER == DEPTH and X % PER == 0 and X * DEPTH <= LANES
        dims = [tuple(d >> l for d in block) for l in range(LEVELS)]
        f32 = jnp.float32
        vm = lambda *s: pltpu.VMEM(s, f32)
        ext = [(dims[l][0] + 2 * DEPTH, dims[l][1] + 2 * TOP, LANES) for l in range(HALOED)]
        slab = (X // PER + 2, Y + 2 * TOP, LANES)
        tall = [(dims[l][1] + 2 * DEPTH, LANES) for l in range(HALOED)]
        CA, CB, CC = dims[HALOED]
        assert dims[HALOED + 1][:2] == (1, 1) and sizes[1] * CB <= ROWS and CA * CB * CC + CC // 2 <= LANES // 2
        dma = lambda *s: pltpu.SemaphoreType.DMA(s)
        scratch = [
            vm(X + 2, Y + 2 * TOP, LANES), vm(*block),
            *(vm(STEPS, *e) for e in ext), vm(STEPS, *slab),
            *(vm(*e) for e in ext[1:]), vm(*slab),
            *(vm(*e) for e in ext + [slab] for _ in range(SWEEPS - 1)),
            vm(*ext[0]), vm(*ext[0]),
            vm(slab[0], *tall[0]), vm(slab[0], *tall[0]),
            vm(dims[1][0] + 2, 2 * tall[1][0], LANES), vm(dims[1][0] + 2, 2 * tall[1][0], LANES),
            *(vm(*t) for t in tall), vm(*tall[0]),
            vm((CA + 1) * sizes[0] * ROWS, (CA * CB + 1) * n),
            vm(CA * sizes[0] + DEPTH, ROWS, LANES),
            vm(CA + DEPTH, 4 * ROWS, LANES),
            vm(X // 2, Y, LANES), vm(X // 2, 2 * Y, LANES),
            vm(2, Y, LANES), vm(2, X, 1, LANES), vm(Y, LANES), vm(2, Y, LANES),
            vm(STEPS, 2, Y, LANES), vm(STEPS, dims[1][1], LANES), vm(STEPS, dims[2][1], LANES),
            *(vm(STEPS, 2, dims[l][1] + 2 * DEPTH, LANES) for l in range(HALOED - 1)),
            vm(STEPS, 2, Y, LANES), vm(STEPS, 2, 2, Y + 2 * DEPTH, LANES),
            vm(STEPS, 2, DEPTH, dims[1][1], LANES), vm(STEPS, 2, DEPTH, dims[1][1] + 2 * DEPTH, LANES),
            vm(STEPS, 1, LANES), vm(STEPS, n, 1, LANES),
            vm(1, LANES), vm(n, 1, LANES), vm(3 * STEPS * DEPTH * max(X, Y), LANES),
            dma(2), dma(6), dma(6), dma(len(ALL)), dma(STEPS, len(ALL)),
            dma(8), dma(STEPS, 8),
            dma(STEPS), dma(STEPS), dma(1), dma(1),
        ]
        whole = pltpu.VMEM(block, f32)
        base, z, r, w, alpha = pl.pallas_call(
            functools.partial(kernel, sizes, block),
            out_shape=(whole, whole, whole, whole, pltpu.VMEM((8, LANES), f32)),
            in_specs=[pl.BlockSpec(memory_space=pl.ANY)] * 2,
            out_specs=[pl.BlockSpec(memory_space=pltpu.VMEM)] * 5,
            scratch_shapes=scratch,
            compiler_params=pltpu.CompilerParams(collective_id=0, has_side_effects=True),
        )(right_side, guess)
        inner = [pltpu.with_memory_space_constraint(v, pltpu.VMEM) for v in (base, z, r, w, alpha)]
        out = jax.ShapeDtypeStruct(block, f32)
        return tuple(pl.pallas_call(
            finish,
            out_shape=(out, out),
            in_specs=[pl.BlockSpec(memory_space=pltpu.VMEM)] * 5,
            out_specs=[pl.BlockSpec(memory_space=pl.ANY)] * 2,
            scratch_shapes=[vm(*block), vm(*block), dma(2, PARTS)],
        )(*inner))

    spec = P(*AXES)
    return jax.shard_map(run, mesh=mesh, in_specs=(spec, spec), out_specs=(spec, spec), check_vma=False)
```

```python
import functools

import jax
import jax.numpy as jnp
from jax import lax
from jax.experimental import pallas as pl
from jax.experimental.pallas import tpu as pltpu
from jax.sharding import PartitionSpec as P

LEVELS = 6
SWEEPS = 4
STEPS = 2
HALOED = 4
AXES = ("gx", "gy", "gz")
LANES = 128
TOP = 8
DEPTH = SWEEPS
SPAN = 8 * DEPTH
PER = LANES // SPAN
PARTS = 4
MESH = pl.DeviceIdType.MESH
HIGH = lax.Precision.HIGHEST
ROWS = 8
ALL = [(a, b, c) for c in (-1, 1, 0) for a in (0, -1, 1) for b in (0, -1, 1) if (a, b, c) != (0, 0, 0)]
AROUND = [(a, b) for a in (-1, 0, 1) for b in (-1, 0, 1) if (a, b) != (0, 0)]
FACES = [(d, s) for d in range(3) for s in (-1, 1)]


def iota(shape, dim):
    return lax.broadcasted_iota(jnp.int32, shape, dim)


def take(x, index):
    if x.ndim == 3:
        return jnp.stack([take(x[i], index) for i in range(x.shape[0])])
    rows = x.shape[0]
    more = -rows % 8
    if rows == 1:
        x = jnp.broadcast_to(x, (8, LANES))
    elif more:
        x = jnp.concatenate([x, jnp.zeros((more, LANES), x.dtype)], axis=0)
    index = jnp.broadcast_to(index[:1], x.shape)
    out = jnp.take_along_axis(x, index, axis=1, mode="promise_in_bounds")
    return out[:rows] if more else out


def wrapped(lane):
    return jnp.where(lane >= LANES - DEPTH, lane - LANES, lane)


def halve(x, width):
    lane = iota((8, LANES), 1)
    return take(x + turn(x, -1), 2 * (lane % width)) * 0.125


def turn(x, shift):
    shift = shift % LANES
    return pltpu.roll(x, shift, x.ndim - 1) if shift else x


def kernel(sizes, block, b_hbm, x_hbm, sol_ref, z_ref, res_ref, w_ref, alpha_ref, *rest):
    (ux, bb, g0, g1, g2, g3, gs, h1, h2, h3, hs, f0a, f0b, f0c, f1a, f1b, f1c, f2a, f2b, f2c, f3a, f3b, f3c, fsa, fsb, fsc,
     z0, z1, sc, sd, pd, pe, m0, m1, m2, m3, ms, pmat, wref, wide, fold, spread, xg, yg, ze, zi, zq0, zq1, zq2, zr0, zr1, zr2, es, zx, xs, xf, cs, cr, ds, dr, blank,
     isem, xsend, xrecv, frecv, send, mrecv, csend, crecv, dsend, drecv) = rest
    nx, ny, nz = sizes
    n = nx * ny * nz
    at = tuple(lax.axis_index(a) for a in AXES)
    me = (at[0] * ny + at[1]) * nz + at[2]
    dims = [tuple(d >> l for d in block) for l in range(LEVELS)]
    X, Y, Z = block
    fields = (g0, g1, g2, g3)
    after = ((f0a, f0b, f0c), (f1a, f1b, f1c), (f2a, f2b, f2c), (f3a, f3b, f3c), (fsa, fsb, fsc))
    masks = (m0, m1, m2, m3)
    whole = (None, h1, h2, h3, hs)
    groups = X // PER
    lower = [at[d] > 0 for d in range(3)]
    upper = [at[d] < sizes[d] - 1 for d in range(3)]
    inlow = [jnp.where(c, 1.0, 0.0) for c in lower]
    inup = [jnp.where(c, 1.0, 0.0) for c in upper]

    load_x = pltpu.make_async_copy(x_hbm, ux.at[1:X + 1, TOP:TOP + Y], isem.at[0])
    load_b = pltpu.make_async_copy(b_hbm, bb, isem.at[1])
    load_x.start()
    load_b.start()

    def others():
        out = []
        for b in range(ny - 1, -1, -1):
            for c in range(nz - 1, -1, -1):
                for a in range(nx):
                    if b or c:
                        first = jnp.where(at[0] < nx // 2, nx - 1 - a, a)
                    elif a:
                        first = lax.rem(at[0] + a, nx)
                    else:
                        continue
                    out.append((first, lax.rem(at[1] + b, ny), lax.rem(at[2] + c, nz)))
        return out

    barrier = pltpu.get_barrier_semaphore()
    for target in others():
        pl.semaphore_signal(barrier, inc=1, device_id=target, device_id_type=MESH)

    def outside(dim, side):
        for l in range(HALOED + 1):
            A, B = (groups if l == HALOED else dims[l][0]), (Y if l == HALOED else dims[l][1])
            d, ref = (1, gs) if l == HALOED else (DEPTH, fields[l])
            for k in range(STEPS):
                if dim == 0:
                    a = A + d if side else 0
                    ref[k, a:a + d, TOP - DEPTH:TOP + B + DEPTH, :] = jnp.zeros((d, B + 2 * DEPTH, LANES), jnp.float32)
                else:
                    a = TOP + B if side else TOP - DEPTH
                    ref[k, :, a:a + DEPTH, :] = jnp.zeros((A + 2 * d, DEPTH, LANES), jnp.float32)

    far = (zr0, zr1, zr2, zx, xf)

    def nothing_in(ref):
        ref[...] = jnp.zeros(ref.shape, jnp.float32)

    for side in (0, 1):
        for dim in range(2):
            @pl.when(jnp.logical_not((upper if side else lower)[dim]))
            def _(dim=dim, side=side):
                outside(dim, side)
                nothing_in((xg, yg)[dim].at[1 - side])
                for ref in far if dim else ():
                    head = (slice(None),) * (len(ref.shape) - 2)
                    a = ref.shape[-2] - DEPTH if side else 0
                    nothing_in(ref.at[head + (slice(a, a + DEPTH),)])
                if dim == 0:
                    nothing_in(zx.at[:, :, side])
                    nothing_in(xf.at[:, side])
        @pl.when(jnp.logical_not((upper if side else lower)[2]))
        def _(side=side):
            nothing_in(zi.at[side])
            for ref in far[:4]:
                nothing_in(ref.at[:, 1 - side])

    ux[:, TOP - 1:TOP, :] = jnp.zeros((X + 2, 1, LANES), jnp.float32)
    ux[:, TOP + Y:TOP + Y + 1, :] = jnp.zeros((X + 2, 1, LANES), jnp.float32)
    ux[0, TOP:TOP + Y, :] = jnp.zeros((Y, LANES), jnp.float32)
    ux[X + 1, TOP:TOP + Y, :] = jnp.zeros((Y, LANES), jnp.float32)
    wref[...] = jnp.zeros_like(wref)
    wide[...] = jnp.zeros_like(wide)

    def mask(rows, z, depth_z):
        y = iota((rows + 2 * DEPTH, LANES), 0) - DEPTH
        part = jnp.where(y < 0, inlow[1], jnp.where(y >= rows, inup[1], 1.0))
        return part * jnp.where(z < 0, inlow[2], jnp.where(z >= depth_z, inup[2], 1.0)) * (1.0 / 9.0)

    for l in range(HALOED):
        lane = iota((dims[l][1] + 2 * DEPTH, LANES), 1)
        masks[l][...] = mask(dims[l][1], lane if l == 0 else wrapped(lane), dims[l][2])
    CA, CB, CC = dims[HALOED]
    CD = dims[HALOED + 1][2]
    cells = CA * CB
    row, column = iota(pmat.shape, 0), iota(pmat.shape, 1)
    cell, device = column // n, column % n
    plane, line = row // ROWS, row % ROWS
    dx, dy = device // (ny * nz), device // nz % ny
    fits = (cell < cells) & (plane == dx * CA + cell // CB) & (line == dy * CB + cell % CB)
    fits = fits | ((cell == cells) & (plane == nx * CA + dx) & (line == dy))
    pmat[...] = jnp.where(fits, 1.0, 0.0)
    lane = iota((Y + 2 * DEPTH, LANES), 1) % SPAN
    ms[...] = mask(Y, jnp.where(lane < SPAN // 2, lane + Z - SPAN // 4, lane - 3 * SPAN // 4), Z)

    def face_copies():
        out = []
        for i, (d, s) in enumerate(FACES):
            target = list(at)
            target[d] = at[d] + s
            into = 1 if s > 0 else 0
            if d == 0:
                src, dst = ux.at[X if s > 0 else 1, TOP:TOP + Y], xg.at[into]
            elif d == 1:
                a = TOP + Y - 1 if s > 0 else TOP
                src, dst = ux.at[1:X + 1, a:a + 1], yg.at[into]
            else:
                src, dst = ze, zi.at[0 if s > 0 else 1]
            copy = pltpu.make_async_remote_copy(
                src_ref=src, dst_ref=dst, send_sem=xsend.at[0], recv_sem=xrecv.at[0],
                device_id=tuple(target), device_id_type=MESH,
            )
            out.append((copy, upper[d] if s > 0 else lower[d], lower[d] if s > 0 else upper[d]))
        return out

    def span(step, depth, start, own, other):
        if step > 0:
            return (start + own - depth, depth), (start - depth, depth)
        if step < 0:
            return (start, depth), (start + own, depth)
        return (start, own), (start, own)

    def around_copies(ref, k, depth, planes, rows, rsem):
        out = []
        for i, (dx, dy) in enumerate(AROUND):
            (sx, lx), (tx, _) = span(dx, depth, depth, planes, None)
            (sy, ly), (ty, _) = span(dy, DEPTH, TOP, rows, None)
            copy = pltpu.make_async_remote_copy(
                src_ref=ref.at[k, sx:sx + lx, sy:sy + ly], dst_ref=ref.at[k, tx:tx + lx, ty:ty + ly],
                send_sem=send.at[0], recv_sem=rsem.at[k],
                device_id=(at[0] + dx, at[1] + dy, at[2]), device_id_type=MESH,
            )
            to, fro = None, None
            for d, s in ((0, dx), (1, dy)):
                if s:
                    a, b = (upper[d], lower[d]) if s > 0 else (lower[d], upper[d])
                    to = a if to is None else jnp.logical_and(to, a)
                    fro = b if fro is None else jnp.logical_and(fro, b)
            out.append((copy, to, fro, lx * ly))
        return out

    def main_copies(k):
        return around_copies(g0, k, DEPTH, X, Y, mrecv)

    def rows_of(dy, rows):
        if dy > 0:
            return pl.ds(rows - DEPTH, DEPTH), pl.ds(0, DEPTH), DEPTH
        if dy < 0:
            return pl.ds(0, DEPTH), pl.ds(rows + DEPTH, DEPTH), DEPTH
        return pl.ds(0, rows), pl.ds(DEPTH, rows), rows

    def every(conds):
        out = None
        for cond in conds:
            out = cond if out is None else jnp.logical_and(out, cond)
        return out

    def far_copies(k):
        out = []
        for i, (dx, dy, dz) in enumerate(ALL):
            step = (dx, dy, dz)
            to = every([(upper if t > 0 else lower)[d] for d, t in enumerate(step) if t])
            fro = every([(lower if t > 0 else upper)[d] for d, t in enumerate(step) if t])
            from_x, into_x = (1, 0) if dx > 0 else (0, 1)
            side = 1 if dz > 0 else 0
            pairs = []
            if dz and dx:
                a, b, c = rows_of(dy, Y)
                pairs.append((es.at[k, from_x, a], zx.at[k, side, into_x, b], c))
            elif dz:
                for src, dst in ((zq0.at[k, side], zr0), (zq1.at[k], zr1), (zq2.at[k], zr2)):
                    a, b, c = rows_of(dy, src.shape[0])
                    pairs.append((src.at[a], dst.at[k, side, b], c))
            else:
                arrays = [(gs, 1, groups, Y)]
                if dx:
                    a, b, c = rows_of(dy, dims[1][1])
                    pairs.append((xs.at[k, from_x, :, a], xf.at[k, into_x, :, b], DEPTH * c))
                else:
                    arrays += [(fields[l], DEPTH, dims[l][0], dims[l][1]) for l in range(1, HALOED)]
                for ref, depth, planes, rows in arrays:
                    (sx, lx), (tx, _) = span(dx, depth, depth, planes, None)
                    (sy, ly), (ty, _) = span(dy, DEPTH, TOP, rows, None)
                    pairs.append((ref.at[k, sx:sx + lx, sy:sy + ly], ref.at[k, tx:tx + lx, ty:ty + ly], lx * ly))
            copies = [pltpu.make_async_remote_copy(
                src_ref=src, dst_ref=dst, send_sem=send.at[0], recv_sem=frecv.at[k],
                device_id=(at[0] + dx, at[1] + dy, at[2] + dz), device_id_type=MESH,
            ) for src, dst, _ in pairs]
            out.append((copies, to, fro, sum(c for _, _, c in pairs)))
        return out

    def bytes_done(count, sem):
        assert count <= blank.shape[0]
        part = blank.at[pl.ds(0, count)]
        pltpu.make_async_copy(part, part, sem).wait()

    def all_of(entries, sem, sign):
        def nest(d, have):
            if d == len(sizes):
                total = sum(c for step, c in entries if all(t == 0 or sign * t in have[i] for i, t in enumerate(step)))
                if total:
                    bytes_done(total, sem)
            elif sizes[d] == 1 or not any(step[d] for step, _ in entries):
                nest(d + 1, have + [()])
            else:
                pl.when(jnp.logical_not(lower[d]))(lambda: nest(d + 1, have + [(1,)]))
                pl.when(jnp.logical_not(upper[d]))(lambda: nest(d + 1, have + [(-1,)]))
                if sizes[d] > 2:
                    pl.when(jnp.logical_and(lower[d], upper[d]))(lambda: nest(d + 1, have + [(-1, 1)]))

        nest(0, [])

    def main_entries():
        return [((dx, dy, 0), entry[3]) for (dx, dy), entry in zip(AROUND, main_copies(0))]

    def far_entries():
        return [(step, entry[3]) for step, entry in zip(ALL, far_copies(0))]

    def face_entries():
        return [(tuple(s if i == d else 0 for i in range(3)), X if d == 1 else Y) for d, s in FACES]

    def start_all(copies):
        for copy, cond, *_ in copies:
            pl.when(cond)(copy.start)

    def start_far(k):
        for copies, to, _, _ in far_copies(k):
            @pl.when(to)
            def _(copies=copies):
                for copy in copies:
                    copy.start()

    def to_all(src, dst, s_sem, r_sem):
        for target in others():
            pltpu.make_async_remote_copy(
                src_ref=src, dst_ref=dst.at[me], send_sem=s_sem, recv_sem=r_sem,
                device_id=target, device_id_type=MESH,
            ).start()

    def all_done(dst, sem):
        part = dst.at[pl.ds(0, n - 1)]
        pltpu.make_async_copy(part, part, sem).wait()

    def fold_xy(field):
        A, B, _ = field.shape
        pairs = field.reshape(A // 2, 2, B, LANES)
        fold[0:A // 2, 0:B, :] = pairs[:, 0] + pairs[:, 1]
        return fold[0:A // 2, pl.ds(0, B // 2, 2), :] + fold[0:A // 2, pl.ds(1, B // 2, 2), :]

    def spread_y(field, into, first=0):
        A, B, _ = field.shape
        into[0:A, pl.ds(first, B, 2), :] = field
        into[0:A, pl.ds(first + 1, B, 2), :] = field

    def twice(field):
        A, B, _ = field.shape
        return jnp.broadcast_to(field[:, None], (A, 2, B, LANES)).reshape(2 * A, B, LANES)

    def own(ref, l, k=None):
        A, B, _ = dims[l]
        return ref[(k,) * (k is not None) + (slice(DEPTH, DEPTH + A), slice(TOP, TOP + B))]

    def update(src, rhs, dst, a, c, low, rows, scale):
        at_rows = slice(low, low + rows)
        mid = src[a:a + c, at_rows, :]
        total = src[a - 1:a - 1 + c, at_rows, :] + src[a + 1:a + 1 + c, at_rows, :]
        total = total + src[a:a + c, low - 1:low - 1 + rows, :] + src[a:a + c, low + 1:low + 1 + rows, :]
        total = total + turn(mid, 1) + turn(mid, -1)
        dst[a:a + c, at_rows, :] = rhs[a:a + c, at_rows, :] + (3.0 * mid + total) * scale

    def pieces(a, b):
        return [(p, min(4, b - p)) for p in range(a, b, 4)]

    def sweep(l, src, rhs, dst, k):
        A, B, _ = dims[l]
        low, rows = TOP - DEPTH, B + 2 * DEPTH
        m = masks[l][...]
        update(src, rhs, dst, k, DEPTH - k, low, rows, m * inlow[0])
        for a, c in pieces(DEPTH, DEPTH + A):
            update(src, rhs, dst, a, c, low, rows, m)
        update(src, rhs, dst, DEPTH + A, DEPTH - k, low, rows, m * inup[0])

    def sweep_inside(src, rhs, dst, k):
        for a, c in pieces(DEPTH + k, DEPTH + X - k):
            update(src, rhs, dst, a, c, TOP + k, Y - 2 * k, 1.0 / 9.0)

    def sweep_rim(src, rhs, dst, k):
        low, rows = TOP - DEPTH, Y + 2 * DEPTH
        m = m0[...]
        update(src, rhs, dst, k, DEPTH - k, low, rows, m * inlow[0])
        update(src, rhs, dst, DEPTH, k, low, rows, m)
        update(src, rhs, dst, DEPTH + X - k, k, low, rows, m)
        update(src, rhs, dst, DEPTH + X, DEPTH - k, low, rows, m * inup[0])
        for start in (0, Y):
            edge = m0[start:start + 2 * DEPTH, :]
            for a, c in pieces(DEPTH + k, DEPTH + X - k):
                update(src, rhs, dst, a, c, low + start, 2 * DEPTH, edge)

    def sweep_slab(src, rhs, dst):
        low, rows = TOP - DEPTH, Y + 2 * DEPTH
        lane = iota((rows, LANES), 1)
        m = ms[...]
        for g in range(groups + 2):
            mid = src[g, low:low + rows, :]
            total = src[g, low - 1:low - 1 + rows, :] + src[g, low + 1:low + 1 + rows, :]
            total = total + turn(mid, 1) + turn(mid, -1)
            before = mid if g == 0 else jnp.where(lane >= LANES - SPAN, src[g - 1, low:low + rows, :], mid)
            behind = mid if g == groups + 1 else jnp.where(lane < SPAN, src[g + 1, low:low + rows, :], mid)
            total = total + turn(before, SPAN) + turn(behind, -SPAN)
            scale = m * inlow[0] if g == 0 else m * inup[0] if g == groups + 1 else m
            dst[g, low:low + rows, :] = rhs[g, low:low + rows, :] + (3.0 * mid + total) * scale

    def smooth_whole(rhs, depth_y, depth_z, l):
        A, B, _ = rhs.shape
        lane, row = iota(rhs.shape, 2), iota(rhs.shape, 1)
        e = rhs
        for _ in range(SWEEPS - 1):
            px, py = jnp.zeros((1, B, LANES), jnp.float32), jnp.zeros((A, 1, LANES), jnp.float32)
            total = jnp.concatenate([px, e[:-1]], axis=0) + jnp.concatenate([e[1:], px], axis=0)
            total = total + jnp.concatenate([py, e[:, :-1]], axis=1) + jnp.concatenate([e[:, 1:], py], axis=1)
            total = total + jnp.where(lane == 0, 0.0, turn(e, 1))
            total = total + jnp.where(lane == depth_z - 1, 0.0, turn(e, -1))
            e = rhs + jnp.where(row < depth_y, (3.0 * e + total) * (1.0 / 9.0), 0.0)
        return e * (4.0 ** l / 9.0)

    half, quarter = SPAN // 2, SPAN // 4

    def pack_slab(k):
        lane = iota((Y, LANES), 1)
        line, spot = lane // SPAN, lane % SPAN
        low = high = jnp.zeros((Y, LANES), jnp.float32)
        for g in range(groups):
            both = jnp.zeros((Y, LANES), jnp.float32)
            for i in range(PER):
                field = g0[k, DEPTH + g * PER + i, TOP:TOP + Y, :]
                both = jnp.where((line == i) & (spot < half), turn(field, SPAN * i + quarter), both)
            gs[k, g + 1, TOP:TOP + Y, :] = jnp.where(
                spot < quarter, both, jnp.where(spot >= 3 * quarter, turn(both, half), 0.0))
            here = spot // DEPTH == g
            low = jnp.where(here, turn(both, DEPTH * g - quarter), low)
            high = jnp.where(here, turn(both, DEPTH * g - quarter + DEPTH), high)
        zq0[k, 0] = low
        zq0[k, 1] = high
        for side, j in ((0, 0), (1, groups - 1)):
            es[k, side] = put(0, low, j, 0) + put(0, high, j, 1)

    def slots(l):
        return (0, 0, 0, dims[2][0] // DEPTH * 2)[l], dims[l][0] // DEPTH

    def put(l, x, source, target):
        lane = iota(x.shape, 1)
        return jnp.where(lane % SPAN // DEPTH == target, turn(x, DEPTH * (target - source)), 0.0)

    def pack_level(k, l):
        A, B, C = dims[l]
        base, many = slots(l)
        lane = iota((B, LANES), 1)
        line, slot = lane // SPAN, lane % SPAN // DEPTH
        out = jnp.zeros((B, LANES), jnp.float32)
        for i in range(A):
            field = fields[l][k, DEPTH + i, TOP:TOP + B, :]
            x, j = i % DEPTH, i // DEPTH
            lo, hi = base + j, base + many + j
            out = jnp.where((line == x) & (slot == lo), turn(field, SPAN * x + DEPTH * lo), out)
            out = jnp.where((line == x) & (slot == hi), turn(field, SPAN * x + DEPTH * hi - C + DEPTH), out)
        return out

    def pack_rest(k):
        one, two, three = [pack_level(k, l) for l in range(1, HALOED)]
        zq1[k] = one
        B1, B2, B3 = [dims[l][1] for l in range(1, HALOED)]
        zq2[k, 0:B2] = two
        for a in (0, B2 - B3):
            zq2[k, a:a + B3] = zq2[k, a:a + B3] + three
        for side in (0, 1):
            def edge(l, x):
                base, many = slots(l)
                j = many - 1 if side else 0
                return put(l, x, base + j, 2 * l) + put(l, x, base + many + j, 2 * l + 1)
            first, second, third = edge(1, one), edge(2, two), edge(3, three)
            for src, dst, size, part in (
                    (0, 0, B1 - DEPTH, first), (B1 - DEPTH, Y - DEPTH, DEPTH, first),
                    (0, 0, DEPTH, second), (B2 - DEPTH, Y - DEPTH, DEPTH, second),
                    (0, 0, DEPTH, third), (0, Y - DEPTH, DEPTH, third)):
                es[k, side, dst:dst + size] = es[k, side, dst:dst + size] + part[src:src + size]
            for x in range(DEPTH):
                p1, p2, p3 = [DEPTH + x + (dims[l][0] - DEPTH if side else 0) for l in range(1, HALOED)]
                xs[k, side, x] = g1[k, p1, TOP:TOP + B1, :]
                second = turn(g2[k, p2, TOP:TOP + B2, :], dims[1][2])
                third = turn(g3[k, p3, TOP:TOP + B3, :], dims[1][2] + dims[2][2])
                xs[k, side, x, 0:DEPTH] = xs[k, side, x, 0:DEPTH] + second[0:DEPTH] + third
                xs[k, side, x, B1 - DEPTH:B1] = xs[k, side, x, B1 - DEPTH:B1] + second[B2 - DEPTH:B2] + third

    def unpack_slab(k):
        low, rows = TOP - DEPTH, Y + 2 * DEPTH
        spot = iota((rows, LANES), 1) % SPAN
        for g in range(groups + 2):
            edge = 0 if g == 0 else 1 if g == groups + 1 else None
            if edge is None:
                above, below, up, down = zr0[k, 0], zr0[k, 1], g - 1, g - 1
            else:
                above, below, up, down = zx[k, 0, edge], zx[k, 1, edge], 0, 1
            held = gs[k, g, low:low + rows, :]
            held = jnp.where(spot // DEPTH == 2, turn(above, DEPTH * (2 - up)), held)
            hs[g, low:low + rows, :] = jnp.where(spot // DEPTH == 5, turn(below, DEPTH * (5 - down)), held)

    def unpack_level(k, l):
        A, B, C = dims[l]
        low, rows = TOP - DEPTH, B + 2 * DEPTH
        base, many = slots(l)
        lane = iota((rows, LANES), 1)

        def cut(ref, head):
            end = ref.shape[-2]
            tail = 0 if end == rows else (2 * DEPTH if B > DEPTH else DEPTH)
            a = ref[head + (slice(0, rows - tail),)]
            return jnp.concatenate([a, ref[head + (slice(end - tail, end),)]], axis=0) if tail else a

        ref = (None, zr1, zr2, zr2)[l]
        sides = [cut(ref, (k, 0)), cut(ref, (k, 1))]
        edges = [[cut(zx, (k, side, e)) for side in (0, 1)] for e in (0, 1)]
        start = sum(dims[i][2] for i in range(1, l))
        for p in range(A + 2 * DEPTH):
            edge = 0 if p < DEPTH else 1 if p >= DEPTH + A else None
            x, j = p % DEPTH, p // DEPTH - 1
            if edge is None:
                held = fields[l][k, p, low:low + rows, :]
                (above, below), up, down = sides, base + j, base + many + j
            else:
                held = jnp.where(lane < C, turn(cut(xf, (k, edge, x)), -start), 0.0)
                (above, below), up, down = edges[edge], 2 * l, 2 * l + 1
            held = jnp.where(lane // DEPTH == C // DEPTH, turn(above, C - SPAN * x - DEPTH * up), held)
            whole[l][p, low:low + rows, :] = jnp.where(
                lane >= LANES - DEPTH, turn(below, -DEPTH - SPAN * x - DEPTH * down), held)

    half_row = LANES // 2
    def own_row(k):
        lane = iota((1, LANES), 1)
        out, total = jnp.zeros((1, LANES), jnp.float32), None
        for i in range(CA):
            for j in range(CB):
                part = None
                for a in (0, 1):
                    for b in (0, 1):
                        y = TOP + 2 * j + b
                        one = fields[HALOED - 1][k, DEPTH + 2 * i + a, y:y + 1, :]
                        part = one if part is None else part + one
                part = halve(part, CC)
                out = jnp.where(lane // CC == i * CB + j, part, out)
                total = part if total is None else total + part
        return jnp.where((lane >= cells * CC) & (lane < cells * CC + CD), halve(total, CD), out)

    def coarse(k):
        rows = cr[k, :, 0, :]
        lane, row = iota((n, LANES), 1), iota((n, LANES), 0)
        parts = [jnp.where(lane // CC == row % nz, take(rows, cell * CC + lane % CC), 0.0) for cell in range(cells)]
        parts.append(jnp.where(lane // CD == row % nz, take(rows, cells * CC + lane % CD), 0.0))
        out = jnp.dot(pmat[...], jnp.concatenate(parts, axis=0), precision=HIGH, preferred_element_type=jnp.float32)
        out = out.reshape(-1, ROWS, LANES)
        last = smooth_whole(out[nx * CA:], ny, nz * CD, HALOED + 1)
        spread_y(last, spread)
        grown = take(spread[0:nx, 0:ROWS, :], iota((8, LANES), 1) // 2)
        wref[DEPTH // 2:DEPTH // 2 + nx * CA, :, :] = (
            twice(grown) + smooth_whole(out[:nx * CA], ny * CB, nz * CC, HALOED))

    def precondition(k, z, extra):
        start_all(main_copies(k))
        lane = iota((8, LANES), 1)
        sums = own(g0, 0, k)
        for l in range(1, HALOED):
            A, B, C = dims[l]
            sums = fold_xy(sums)
            sums = sums + turn(sums, -(1 << (l - 1)))
            coarser = jnp.where(lane[0:1][None] < C, take(sums, (1 << l) * (lane % C)) * 0.125 ** l, 0.0)
            fields[l][k, DEPTH:DEPTH + A, TOP:TOP + B, :] = coarser
        pack_slab(k)
        pack_rest(k)
        mine = own_row(k) if extra is None else jnp.where(iota((1, LANES), 1) < half_row, own_row(k), extra)
        cs[k] = mine
        cr[k, me] = mine
        start_far(k)
        to_all(cs.at[k], cr.at[k], csend.at[0], crecv.at[k])
        for s in range(1, SWEEPS):
            sweep_inside(after[0][s - 2] if s > 1 else g0.at[k], g0.at[k], after[0][s - 1], s)
        all_of(main_entries(), mrecv.at[k], -1)
        for s in range(1, SWEEPS):
            sweep_rim(after[0][s - 2] if s > 1 else g0.at[k], g0.at[k], after[0][s - 1], s)
        all_of(far_entries(), frecv.at[k], -1)
        unpack_slab(k)
        for l in range(1, HALOED):
            unpack_level(k, l)
        for s in range(1, SWEEPS):
            sweep_slab(after[HALOED][s - 2] if s > 1 else hs, hs, after[HALOED][s - 1])
            for l in range(1, HALOED):
                sweep(l, after[l][s - 2] if s > 1 else whole[l], whole[l], after[l][s - 1], s)
        all_done(cr.at[k], crecv.at[k])
        coarse(k)
        A, B, C = dims[HALOED - 1]
        spread_y(wref[pl.ds(at[0] * CA, CA + DEPTH)], wide, DEPTH)
        part = wide[:, 0:2 * ROWS, :]
        for j in range(1, ny):
            part = jnp.where(at[1] == j, wide[:, j * B:j * B + 2 * ROWS, :], part)
        source = (wrapped(lane) >> 1) + at[2] * CC
        inside = (source >= 0) & (source < CC * nz)
        part = take(part, jnp.where(inside, source, 0))
        part = jnp.where(inside[0:1][None], part, 0.0)
        part = twice(part)[DEPTH - 1:DEPTH + A + 1, 0:B + 2 * DEPTH]
        for l in range(HALOED - 1, 0, -1):
            A, B, C = dims[l]
            end = after[l][SWEEPS - 2][DEPTH - 1:DEPTH + A + 1, TOP - DEPTH:TOP + B + DEPTH, :]
            full = end * (4.0 ** l / 9.0) + part
            if l > 1:
                spread_y(take(full, (wrapped(lane) >> 1) & (LANES - 1)), spread)
                part = twice(spread[0:A + 2, DEPTH:DEPTH + 2 * B + 2 * DEPTH, :])[1:2 * A + 3]
            else:
                spread_y(take(full, lane // 2), pd)
                spread_y(take(full, jnp.where(lane == 0, LANES - 1, C)), pe)
        low, rows = TOP - DEPTH, Y + 2 * DEPTH
        slab = after[HALOED][SWEEPS - 2]
        spot = iota((rows, LANES), 1) % SPAN
        for g in range(groups + 2):
            s = slab[g, low:low + rows, :]
            sc[g] = jnp.where(spot < quarter, s, turn(s, -half))
            sd[g] = jnp.where(spot <= quarter, s, turn(s, quarter + 1 - (3 * quarter - 1)))
        lane = iota((rows, LANES), 1)
        near = (lane < DEPTH - 1) | (lane > LANES - DEPTH)
        end = after[0][SWEEPS - 2]
        for p in range(DEPTH - 1, DEPTH + X + 1):
            g, i = p // PER, p % PER
            f = jnp.where(near, turn(sc[g], -quarter - SPAN * i), end[p, low:low + rows, :])
            z[p, low:low + rows, :] = f * (1.0 / 9.0) + pd[(p - DEPTH + 2) // 2, low:low + rows, :]

    def around(ref, p):
        mid = ref[p, TOP:TOP + Y, :]
        total = ref[p - 1, TOP:TOP + Y, :] + ref[p + 1, TOP:TOP + Y, :]
        return mid, total + ref[p, TOP - 1:TOP - 1 + Y, :] + ref[p, TOP + 1:TOP + 1 + Y, :]

    lane = iota((Y, LANES), 1)
    first, last = lane == 0, lane == LANES - 1

    def operator(z, p):
        mid, total = around(z, p)
        g, i = p // PER, p % PER
        ghost = turn(sd[g, DEPTH:DEPTH + Y, :], LANES - 1 - quarter - SPAN * i) * (1.0 / 9.0)
        ghost = ghost + pe[(p - DEPTH + 2) // 2, TOP:TOP + Y, :]
        total = total + jnp.where(first, ghost, turn(mid, 1))
        total = total + jnp.where(last, ghost, turn(mid, -1))
        return mid, 6.0 * mid - total

    load_x.wait()
    out = jnp.zeros((Y, LANES), jnp.float32)
    for i in range(X):
        out = jnp.where(lane // 2 == i, turn(ux[1 + i, TOP:TOP + Y, :], 2 * i + 1), out)
    ze[...] = out
    pl.semaphore_wait(barrier, n - 1)
    start_all(face_copies())
    load_b.wait()
    for i in range(X):
        mid, total = around(ux, 1 + i)
        total = total + jnp.where(first, 0.0, turn(mid, 1))
        total = total + jnp.where(last, 0.0, turn(mid, -1))
        g0[0, DEPTH + i, TOP:TOP + Y, :] = bb[i] - (6.0 * mid - total)
    all_of(face_entries(), xrecv.at[0], -1)
    for i, side in ((0, 1), (X - 1, 0)):
        here = (0, DEPTH + i, slice(TOP, TOP + Y))
        g0[here] = g0[here] + xg[side]
    for j, side in ((0, 1), (Y - 1, 0)):
        here = (0, slice(DEPTH, DEPTH + X), slice(TOP + j, TOP + j + 1))
        g0[here] = g0[here] + yg[side]
    ghosts = jnp.where(lane % 2 == 0, turn(zi[1], -1), turn(zi[0], 1))
    for i in range(X):
        here = (0, DEPTH + i, slice(TOP, TOP + Y))
        g0[here] = g0[here] + jnp.where(first | last, turn(ghosts, -2 * i - 1), 0.0)

    def sums_of(a, b):
        lane = iota((1, LANES), 1)
        pair = jnp.concatenate([jnp.sum(a, axis=0, keepdims=True), jnp.sum(b, axis=0, keepdims=True)], axis=0)
        pair = pair + turn(pair, LANES // 2)
        pair = pair + turn(pair, LANES // 4)
        return jnp.where(lane < 3 * LANES // 4, pair[0:1], pair[1:2])

    def ratio(rows):
        lane = iota((1, LANES), 1)
        row = jnp.sum(rows, axis=0, keepdims=True)
        upper_half = jnp.where(lane >= 3 * LANES // 4, row, 0.0)
        lower_half = jnp.where((lane >= half_row) & (lane < 3 * LANES // 4), row, 0.0)
        return jnp.sum(lower_half, axis=1, keepdims=True) / jnp.sum(upper_half, axis=1, keepdims=True)

    nothing = jnp.zeros((Y, LANES), jnp.float32)
    precondition(0, z0, None)
    rz, zw = nothing, nothing
    for i in range(X):
        mid, image = operator(z0, DEPTH + i)
        g0[1, DEPTH + i, TOP:TOP + Y, :] = image
        rz = rz + g0[0, DEPTH + i, TOP:TOP + Y, :] * mid
        zw = zw + mid * image
    precondition(1, z1, sums_of(rz, zw))
    alpha = ratio(cr[1, :, 0, :])
    rz, zw = nothing, nothing
    for i in range(X):
        mid, image = operator(z1, DEPTH + i)
        here = (DEPTH + i, slice(TOP, TOP + Y))
        before, w = z0[here], g0[(1,) + here]
        r = g0[(0,) + here] - alpha * w
        z = before - alpha * mid
        w = w - alpha * image
        rz = rz + r * z
        zw = zw + z * w
        sol_ref[i] = ux[1 + i, TOP:TOP + Y, :] + alpha * before
        z_ref[i] = z
        res_ref[i] = r
        w_ref[i] = w
    sums = sums_of(rz, zw)
    ds[...] = sums
    dr[me] = sums
    to_all(ds, dr, dsend.at[0], drecv.at[0])
    all_of(face_entries(), xsend.at[0], 1)
    all_of([(step, STEPS * c) for step, c in main_entries() + far_entries()], send.at[0], 1)
    part = cr.at[:, pl.ds(0, n - 1)]
    pltpu.make_async_copy(part, part, csend.at[0]).wait()
    all_done(dr, dsend.at[0])
    all_done(dr, drecv.at[0])
    alpha_ref[...] = jnp.broadcast_to(ratio(dr[:, 0, :]), alpha_ref.shape)


def finish(base, z, r, w, alpha, sol, res, sol_out, res_out, sem):
    X = base.shape[0]
    size = X // PARTS
    a = alpha[0:1, 0:1][None]
    copies = []
    for part in range(PARTS):
        here = slice(part * size, (part + 1) * size)
        sol_out[here] = base[here] + a * z[here]
        res_out[here] = r[here] - a * w[here]
        for i, (src, dst) in enumerate(((sol_out, sol), (res_out, res))):
            copies.append(pltpu.make_async_copy(src.at[here], dst.at[here], sem.at[i, part]))
            copies[-1].start()
    for copy in copies:
        copy.wait()


def solution(mesh):
    sizes = tuple(mesh.shape[a] for a in AXES)
    n = sizes[0] * sizes[1] * sizes[2]

    def run(right_side, guess):
        X, Y, Z = block = guess.shape
        assert Z == LANES and PER == DEPTH and X % PER == 0 and X * DEPTH <= LANES
        dims = [tuple(d >> l for d in block) for l in range(LEVELS)]
        f32 = jnp.float32
        vm = lambda *s: pltpu.VMEM(s, f32)
        ext = [(dims[l][0] + 2 * DEPTH, dims[l][1] + 2 * TOP, LANES) for l in range(HALOED)]
        slab = (X // PER + 2, Y + 2 * TOP, LANES)
        tall = [(dims[l][1] + 2 * DEPTH, LANES) for l in range(HALOED)]
        CA, CB, CC = dims[HALOED]
        assert dims[HALOED + 1][:2] == (1, 1) and sizes[1] * CB <= ROWS and CA * CB * CC + CC // 2 <= LANES // 2
        dma = lambda *s: pltpu.SemaphoreType.DMA(s)
        scratch = [
            vm(X + 2, Y + 2 * TOP, LANES), vm(*block),
            *(vm(STEPS, *e) for e in ext), vm(STEPS, *slab),
            *(vm(*e) for e in ext[1:]), vm(*slab),
            *(vm(*e) for e in ext + [slab] for _ in range(SWEEPS - 1)),
            vm(*ext[0]), vm(*ext[0]),
            vm(slab[0], *tall[0]), vm(slab[0], *tall[0]),
            vm(dims[1][0] + 2, 2 * tall[1][0], LANES), vm(dims[1][0] + 2, 2 * tall[1][0], LANES),
            *(vm(*t) for t in tall), vm(*tall[0]),
            vm((CA + 1) * sizes[0] * ROWS, (CA * CB + 1) * n),
            vm(CA * sizes[0] + DEPTH, ROWS, LANES),
            vm(CA + DEPTH, 4 * ROWS, LANES),
            vm(X // 2, Y, LANES), vm(X // 2, 2 * Y, LANES),
            vm(2, Y, LANES), vm(2, X, 1, LANES), vm(Y, LANES), vm(2, Y, LANES),
            vm(STEPS, 2, Y, LANES), vm(STEPS, dims[1][1], LANES), vm(STEPS, dims[2][1], LANES),
            *(vm(STEPS, 2, dims[l][1] + 2 * DEPTH, LANES) for l in range(HALOED - 1)),
            vm(STEPS, 2, Y, LANES), vm(STEPS, 2, 2, Y + 2 * DEPTH, LANES),
            vm(STEPS, 2, DEPTH, dims[1][1], LANES), vm(STEPS, 2, DEPTH, dims[1][1] + 2 * DEPTH, LANES),
            vm(STEPS, 1, LANES), vm(STEPS, n, 1, LANES),
            vm(1, LANES), vm(n, 1, LANES), vm(16 * STEPS * DEPTH * max(X, Y), LANES),
            dma(2), dma(1), dma(1), dma(STEPS), dma(1), dma(STEPS),
            dma(1), dma(STEPS), dma(1), dma(1),
        ]
        whole = pltpu.VMEM(block, f32)
        base, z, r, w, alpha = pl.pallas_call(
            functools.partial(kernel, sizes, block),
            out_shape=(whole, whole, whole, whole, pltpu.VMEM((8, LANES), f32)),
            in_specs=[pl.BlockSpec(memory_space=pl.ANY)] * 2,
            out_specs=[pl.BlockSpec(memory_space=pltpu.VMEM)] * 5,
            scratch_shapes=scratch,
            compiler_params=pltpu.CompilerParams(collective_id=0, has_side_effects=True),
        )(right_side, guess)
        inner = [pltpu.with_memory_space_constraint(v, pltpu.VMEM) for v in (base, z, r, w, alpha)]
        out = jax.ShapeDtypeStruct(block, f32)
        return tuple(pl.pallas_call(
            finish,
            out_shape=(out, out),
            in_specs=[pl.BlockSpec(memory_space=pltpu.VMEM)] * 5,
            out_specs=[pl.BlockSpec(memory_space=pl.ANY)] * 2,
            scratch_shapes=[vm(*block), vm(*block), dma(2, PARTS)],
        )(*inner))

    spec = P(*AXES)
    return jax.shard_map(run, mesh=mesh, in_specs=(spec, spec), out_specs=(spec, spec), check_vma=False)
```

```python
import functools

import jax
import jax.numpy as jnp
from jax import lax
from jax.experimental import pallas as pl
from jax.experimental.pallas import tpu as pltpu
from jax.sharding import PartitionSpec as P

LEVELS = 6
SWEEPS = 4
STEPS = 2
HALOED = 4
AXES = ("gx", "gy", "gz")
LANES = 128
TOP = 8
DEPTH = SWEEPS
SPAN = 8 * DEPTH
PER = LANES // SPAN
PARTS = 4
MESH = pl.DeviceIdType.MESH
HIGH = lax.Precision.HIGHEST
ROWS = 8
ALL = [(a, b, c) for c in (-1, 1, 0) for a in (0, -1, 1) for b in (0, -1, 1) if (a, b, c) != (0, 0, 0)]
AROUND = [(a, b) for a in (-1, 0, 1) for b in (-1, 0, 1) if (a, b) != (0, 0)]
FACES = [(d, s) for d in range(3) for s in (-1, 1)]


def iota(shape, dim):
    return lax.broadcasted_iota(jnp.int32, shape, dim)


def take(x, index):
    if x.ndim == 3:
        return jnp.stack([take(x[i], index) for i in range(x.shape[0])])
    rows = x.shape[0]
    more = -rows % 8
    if rows == 1:
        x = jnp.broadcast_to(x, (8, LANES))
    elif more:
        x = jnp.concatenate([x, jnp.zeros((more, LANES), x.dtype)], axis=0)
    index = jnp.broadcast_to(index[:1], x.shape)
    out = jnp.take_along_axis(x, index, axis=1, mode="promise_in_bounds")
    return out[:rows] if more else out


def wrapped(lane):
    return jnp.where(lane >= LANES - DEPTH, lane - LANES, lane)


def halve(x, width):
    lane = iota((8, LANES), 1)
    return take(x + turn(x, -1), 2 * (lane % width)) * 0.125


def turn(x, shift):
    shift = shift % LANES
    return pltpu.roll(x, shift, x.ndim - 1) if shift else x


def kernel(sizes, block, b_hbm, x_hbm, sol_ref, z_ref, res_ref, w_ref, alpha_ref, *rest):
    (ux, bb, g0, g1, g2, g3, gs, h1, h2, h3, hs, f0a, f0b, f0c, f1a, f1b, f1c, f2a, f2b, f2c, f3a, f3b, f3c, fsa, fsb, fsc,
     z0, z1, sc, sd, pd, pe, m0, m1, m2, m3, ms, pmat, wref, wide, fold, spread, xg, yg, ze, zi, zq0, zq1, zq2, zr0, zr1, zr2, es, zx, xs, xf, cs, cr, ds, dr, blank,
     isem, xsend, xrecv, frecv, send, mrecv, csend, crecv, dsend, drecv) = rest
    nx, ny, nz = sizes
    n = nx * ny * nz
    at = tuple(lax.axis_index(a) for a in AXES)
    me = (at[0] * ny + at[1]) * nz + at[2]
    dims = [tuple(d >> l for d in block) for l in range(LEVELS)]
    X, Y, Z = block
    fields = (g0, g1, g2, g3)
    after = ((f0a, f0b, f0c), (f1a, f1b, f1c), (f2a, f2b, f2c), (f3a, f3b, f3c), (fsa, fsb, fsc))
    masks = (m0, m1, m2, m3)
    whole = (None, h1, h2, h3, hs)
    groups = X // PER
    lower = [at[d] > 0 for d in range(3)]
    upper = [at[d] < sizes[d] - 1 for d in range(3)]
    inlow = [jnp.where(c, 1.0, 0.0) for c in lower]
    inup = [jnp.where(c, 1.0, 0.0) for c in upper]

    load_x = pltpu.make_async_copy(x_hbm, ux.at[1:X + 1, TOP:TOP + Y], isem.at[0])
    load_b = pltpu.make_async_copy(b_hbm, bb, isem.at[1])
    load_x.start()
    load_b.start()

    def others():
        out = []
        for b in range(ny - 1, -1, -1):
            for c in range(nz - 1, -1, -1):
                for a in range(nx):
                    if b or c:
                        first = jnp.where(at[0] < nx // 2, nx - 1 - a, a)
                    elif a:
                        first = lax.rem(at[0] + a, nx)
                    else:
                        continue
                    out.append((first, lax.rem(at[1] + b, ny), lax.rem(at[2] + c, nz)))
        return out

    barrier = pltpu.get_barrier_semaphore()
    for target in others():
        pl.semaphore_signal(barrier, inc=1, device_id=target, device_id_type=MESH)

    def outside(dim, side):
        for l in range(HALOED + 1):
            A, B = (groups if l == HALOED else dims[l][0]), (Y if l == HALOED else dims[l][1])
            d, ref = (1, gs) if l == HALOED else (DEPTH, fields[l])
            for k in range(STEPS):
                if dim == 0:
                    a = A + d if side else 0
                    ref[k, a:a + d, TOP - DEPTH:TOP + B + DEPTH, :] = jnp.zeros((d, B + 2 * DEPTH, LANES), jnp.float32)
                else:
                    a = TOP + B if side else TOP - DEPTH
                    ref[k, :, a:a + DEPTH, :] = jnp.zeros((A + 2 * d, DEPTH, LANES), jnp.float32)

    far = (zr0, zr1, zr2, zx, xf)

    def nothing_in(ref):
        ref[...] = jnp.zeros(ref.shape, jnp.float32)

    for side in (0, 1):
        for dim in range(2):
            @pl.when(jnp.logical_not((upper if side else lower)[dim]))
            def _(dim=dim, side=side):
                outside(dim, side)
                nothing_in((xg, yg)[dim].at[1 - side])
                for ref in far if dim else ():
                    head = (slice(None),) * (len(ref.shape) - 2)
                    a = ref.shape[-2] - DEPTH if side else 0
                    nothing_in(ref.at[head + (slice(a, a + DEPTH),)])
                if dim == 0:
                    nothing_in(zx.at[:, :, side])
                    nothing_in(xf.at[:, side])
        @pl.when(jnp.logical_not((upper if side else lower)[2]))
        def _(side=side):
            nothing_in(zi.at[side])
            for ref in far[:4]:
                nothing_in(ref.at[:, 1 - side])

    ux[:, TOP - 1:TOP, :] = jnp.zeros((X + 2, 1, LANES), jnp.float32)
    ux[:, TOP + Y:TOP + Y + 1, :] = jnp.zeros((X + 2, 1, LANES), jnp.float32)
    ux[0, TOP:TOP + Y, :] = jnp.zeros((Y, LANES), jnp.float32)
    ux[X + 1, TOP:TOP + Y, :] = jnp.zeros((Y, LANES), jnp.float32)
    wref[...] = jnp.zeros_like(wref)
    wide[...] = jnp.zeros_like(wide)

    def mask(rows, z, depth_z):
        y = iota((rows + 2 * DEPTH, LANES), 0) - DEPTH
        part = jnp.where(y < 0, inlow[1], jnp.where(y >= rows, inup[1], 1.0))
        return part * jnp.where(z < 0, inlow[2], jnp.where(z >= depth_z, inup[2], 1.0)) * (1.0 / 9.0)

    for l in range(HALOED):
        lane = iota((dims[l][1] + 2 * DEPTH, LANES), 1)
        masks[l][...] = mask(dims[l][1], lane if l == 0 else wrapped(lane), dims[l][2])
    CA, CB, CC = dims[HALOED]
    CD = dims[HALOED + 1][2]
    cells = CA * CB
    row, column = iota(pmat.shape, 0), iota(pmat.shape, 1)
    cell, device = column // n, column % n
    plane, line = row // ROWS, row % ROWS
    dx, dy = device // (ny * nz), device // nz % ny
    fits = (cell < cells) & (plane == dx * CA + cell // CB) & (line == dy * CB + cell % CB)
    fits = fits | ((cell == cells) & (plane == nx * CA + dx) & (line == dy))
    pmat[...] = jnp.where(fits, 1.0, 0.0)
    lane = iota((Y + 2 * DEPTH, LANES), 1) % SPAN
    ms[...] = mask(Y, jnp.where(lane < SPAN // 2, lane + Z - SPAN // 4, lane - 3 * SPAN // 4), Z)

    def face_copies():
        out = []
        for i, (d, s) in enumerate(FACES):
            target = list(at)
            target[d] = at[d] + s
            into = 1 if s > 0 else 0
            if d == 0:
                src, dst = ux.at[X if s > 0 else 1, TOP:TOP + Y], xg.at[into]
            elif d == 1:
                a = TOP + Y - 1 if s > 0 else TOP
                src, dst = ux.at[1:X + 1, a:a + 1], yg.at[into]
            else:
                src, dst = ze, zi.at[0 if s > 0 else 1]
            copy = pltpu.make_async_remote_copy(
                src_ref=src, dst_ref=dst, send_sem=xsend.at[0], recv_sem=xrecv.at[0],
                device_id=tuple(target), device_id_type=MESH,
            )
            out.append((copy, upper[d] if s > 0 else lower[d], lower[d] if s > 0 else upper[d]))
        return out

    def span(step, depth, start, own, other):
        if step > 0:
            return (start + own - depth, depth), (start - depth, depth)
        if step < 0:
            return (start, depth), (start + own, depth)
        return (start, own), (start, own)

    def around_copies(ref, k, depth, planes, rows, rsem):
        out = []
        for i, (dx, dy) in enumerate(AROUND):
            (sx, lx), (tx, _) = span(dx, depth, depth, planes, None)
            (sy, ly), (ty, _) = span(dy, DEPTH, TOP, rows, None)
            copy = pltpu.make_async_remote_copy(
                src_ref=ref.at[k, sx:sx + lx, sy:sy + ly], dst_ref=ref.at[k, tx:tx + lx, ty:ty + ly],
                send_sem=send.at[0], recv_sem=rsem.at[k],
                device_id=(at[0] + dx, at[1] + dy, at[2]), device_id_type=MESH,
            )
            to, fro = None, None
            for d, s in ((0, dx), (1, dy)):
                if s:
                    a, b = (upper[d], lower[d]) if s > 0 else (lower[d], upper[d])
                    to = a if to is None else jnp.logical_and(to, a)
                    fro = b if fro is None else jnp.logical_and(fro, b)
            out.append((copy, to, fro, lx * ly))
        return out

    def main_copies(k):
        return around_copies(g0, k, DEPTH, X, Y, mrecv)

    def rows_of(dy, rows):
        if dy > 0:
            return pl.ds(rows - DEPTH, DEPTH), pl.ds(0, DEPTH), DEPTH
        if dy < 0:
            return pl.ds(0, DEPTH), pl.ds(rows + DEPTH, DEPTH), DEPTH
        return pl.ds(0, rows), pl.ds(DEPTH, rows), rows

    def every(conds):
        out = None
        for cond in conds:
            out = cond if out is None else jnp.logical_and(out, cond)
        return out

    def far_copies(k):
        out = []
        for i, (dx, dy, dz) in enumerate(ALL):
            step = (dx, dy, dz)
            to = every([(upper if t > 0 else lower)[d] for d, t in enumerate(step) if t])
            fro = every([(lower if t > 0 else upper)[d] for d, t in enumerate(step) if t])
            from_x, into_x = (1, 0) if dx > 0 else (0, 1)
            side = 1 if dz > 0 else 0
            pairs = []
            if dz and dx:
                a, b, c = rows_of(dy, Y)
                pairs.append((es.at[k, from_x, a], zx.at[k, side, into_x, b], c))
            elif dz:
                for src, dst in ((zq0.at[k, side], zr0), (zq1.at[k], zr1), (zq2.at[k], zr2)):
                    a, b, c = rows_of(dy, src.shape[0])
                    pairs.append((src.at[a], dst.at[k, side, b], c))
            else:
                arrays = []
                if dx:
                    a, b, c = rows_of(dy, dims[1][1])
                    pairs.append((xs.at[k, from_x, :, a], xf.at[k, into_x, :, b], DEPTH * c))
                else:
                    arrays = [(gs, 1, groups, Y)]
                    arrays += [(fields[l], DEPTH, dims[l][0], dims[l][1]) for l in range(1, HALOED)]
                for ref, depth, planes, rows in arrays:
                    (sx, lx), (tx, _) = span(dx, depth, depth, planes, None)
                    (sy, ly), (ty, _) = span(dy, DEPTH, TOP, rows, None)
                    pairs.append((ref.at[k, sx:sx + lx, sy:sy + ly], ref.at[k, tx:tx + lx, ty:ty + ly], lx * ly))
            copies = [pltpu.make_async_remote_copy(
                src_ref=src, dst_ref=dst, send_sem=send.at[0], recv_sem=frecv.at[k],
                device_id=(at[0] + dx, at[1] + dy, at[2] + dz), device_id_type=MESH,
            ) for src, dst, _ in pairs]
            out.append((copies, to, fro, sum(c for _, _, c in pairs)))
        return out

    def bytes_done(count, sem):
        assert count <= blank.shape[0]
        part = blank.at[pl.ds(0, count)]
        pltpu.make_async_copy(part, part, sem).wait()

    def all_of(entries, sem, sign):
        def nest(d, have):
            if d == len(sizes):
                total = sum(c for step, c in entries if all(t == 0 or sign * t in have[i] for i, t in enumerate(step)))
                if total:
                    bytes_done(total, sem)
            elif sizes[d] == 1 or not any(step[d] for step, _ in entries):
                nest(d + 1, have + [()])
            else:
                pl.when(jnp.logical_not(lower[d]))(lambda: nest(d + 1, have + [(1,)]))
                pl.when(jnp.logical_not(upper[d]))(lambda: nest(d + 1, have + [(-1,)]))
                if sizes[d] > 2:
                    pl.when(jnp.logical_and(lower[d], upper[d]))(lambda: nest(d + 1, have + [(-1, 1)]))

        nest(0, [])

    def main_entries():
        return [((dx, dy, 0), entry[3]) for (dx, dy), entry in zip(AROUND, main_copies(0))]

    def far_entries():
        return [(step, entry[3]) for step, entry in zip(ALL, far_copies(0))]

    def face_entries():
        return [(tuple(s if i == d else 0 for i in range(3)), X if d == 1 else Y) for d, s in FACES]

    def start_all(copies):
        for copy, cond, *_ in copies:
            pl.when(cond)(copy.start)

    def start_far(k):
        for copies, to, _, _ in far_copies(k):
            @pl.when(to)
            def _(copies=copies):
                for copy in copies:
                    copy.start()

    def to_all(src, dst, s_sem, r_sem):
        for target in others():
            pltpu.make_async_remote_copy(
                src_ref=src, dst_ref=dst.at[me], send_sem=s_sem, recv_sem=r_sem,
                device_id=target, device_id_type=MESH,
            ).start()

    def all_done(dst, sem):
        part = dst.at[pl.ds(0, n - 1)]
        pltpu.make_async_copy(part, part, sem).wait()

    def fold_xy(field):
        A, B, _ = field.shape
        pairs = field.reshape(A // 2, 2, B, LANES)
        fold[0:A // 2, 0:B, :] = pairs[:, 0] + pairs[:, 1]
        return fold[0:A // 2, pl.ds(0, B // 2, 2), :] + fold[0:A // 2, pl.ds(1, B // 2, 2), :]

    def spread_y(field, into, first=0):
        A, B, _ = field.shape
        into[0:A, pl.ds(first, B, 2), :] = field
        into[0:A, pl.ds(first + 1, B, 2), :] = field

    def twice(field):
        A, B, _ = field.shape
        return jnp.broadcast_to(field[:, None], (A, 2, B, LANES)).reshape(2 * A, B, LANES)

    def own(ref, l, k=None):
        A, B, _ = dims[l]
        return ref[(k,) * (k is not None) + (slice(DEPTH, DEPTH + A), slice(TOP, TOP + B))]

    def update(src, rhs, dst, a, c, low, rows, scale):
        at_rows = slice(low, low + rows)
        mid = src[a:a + c, at_rows, :]
        total = src[a - 1:a - 1 + c, at_rows, :] + src[a + 1:a + 1 + c, at_rows, :]
        total = total + src[a:a + c, low - 1:low - 1 + rows, :] + src[a:a + c, low + 1:low + 1 + rows, :]
        total = total + turn(mid, 1) + turn(mid, -1)
        dst[a:a + c, at_rows, :] = rhs[a:a + c, at_rows, :] + (3.0 * mid + total) * scale

    def pieces(a, b):
        return [(p, min(4, b - p)) for p in range(a, b, 4)]

    def sweep(l, src, rhs, dst, k):
        A, B, _ = dims[l]
        low, rows = TOP - DEPTH, B + 2 * DEPTH
        m = masks[l][...]
        update(src, rhs, dst, k, DEPTH - k, low, rows, m * inlow[0])
        for a, c in pieces(DEPTH, DEPTH + A):
            update(src, rhs, dst, a, c, low, rows, m)
        update(src, rhs, dst, DEPTH + A, DEPTH - k, low, rows, m * inup[0])

    def sweep_inside(src, rhs, dst, k):
        for a, c in pieces(DEPTH + k, DEPTH + X - k):
            update(src, rhs, dst, a, c, TOP + k, Y - 2 * k, 1.0 / 9.0)

    def sweep_rim(src, rhs, dst, k):
        low, rows = TOP - DEPTH, Y + 2 * DEPTH
        m = m0[...]
        update(src, rhs, dst, k, DEPTH - k, low, rows, m * inlow[0])
        update(src, rhs, dst, DEPTH, k, low, rows, m)
        update(src, rhs, dst, DEPTH + X - k, k, low, rows, m)
        update(src, rhs, dst, DEPTH + X, DEPTH - k, low, rows, m * inup[0])
        for start in (0, Y):
            edge = m0[start:start + 2 * DEPTH, :]
            for a, c in pieces(DEPTH + k, DEPTH + X - k):
                update(src, rhs, dst, a, c, low + start, 2 * DEPTH, edge)

    def sweep_slab(src, rhs, dst):
        low, rows = TOP - DEPTH, Y + 2 * DEPTH
        lane = iota((rows, LANES), 1)
        m = ms[...]
        for g in range(groups + 2):
            mid = src[g, low:low + rows, :]
            total = src[g, low - 1:low - 1 + rows, :] + src[g, low + 1:low + 1 + rows, :]
            total = total + turn(mid, 1) + turn(mid, -1)
            before = mid if g == 0 else jnp.where(lane >= LANES - SPAN, src[g - 1, low:low + rows, :], mid)
            behind = mid if g == groups + 1 else jnp.where(lane < SPAN, src[g + 1, low:low + rows, :], mid)
            total = total + turn(before, SPAN) + turn(behind, -SPAN)
            scale = m * inlow[0] if g == 0 else m * inup[0] if g == groups + 1 else m
            dst[g, low:low + rows, :] = rhs[g, low:low + rows, :] + (3.0 * mid + total) * scale

    def smooth_whole(rhs, depth_y, depth_z, l):
        A, B, _ = rhs.shape
        lane, row = iota(rhs.shape, 2), iota(rhs.shape, 1)
        e = rhs
        for _ in range(SWEEPS - 1):
            px, py = jnp.zeros((1, B, LANES), jnp.float32), jnp.zeros((A, 1, LANES), jnp.float32)
            total = jnp.concatenate([px, e[:-1]], axis=0) + jnp.concatenate([e[1:], px], axis=0)
            total = total + jnp.concatenate([py, e[:, :-1]], axis=1) + jnp.concatenate([e[:, 1:], py], axis=1)
            total = total + jnp.where(lane == 0, 0.0, turn(e, 1))
            total = total + jnp.where(lane == depth_z - 1, 0.0, turn(e, -1))
            e = rhs + jnp.where(row < depth_y, (3.0 * e + total) * (1.0 / 9.0), 0.0)
        return e * (4.0 ** l / 9.0)

    half, quarter = SPAN // 2, SPAN // 4

    def pack_slab(k):
        lane = iota((Y, LANES), 1)
        line, spot = lane // SPAN, lane % SPAN
        low = high = jnp.zeros((Y, LANES), jnp.float32)
        for g in range(groups):
            both = jnp.zeros((Y, LANES), jnp.float32)
            for i in range(PER):
                field = g0[k, DEPTH + g * PER + i, TOP:TOP + Y, :]
                both = jnp.where((line == i) & (spot < half), turn(field, SPAN * i + quarter), both)
            gs[k, g + 1, TOP:TOP + Y, :] = jnp.where(
                spot < quarter, both, jnp.where(spot >= 3 * quarter, turn(both, half), 0.0))
            here = spot // DEPTH == g
            low = jnp.where(here, turn(both, DEPTH * g - quarter), low)
            high = jnp.where(here, turn(both, DEPTH * g - quarter + DEPTH), high)
        zq0[k, 0] = low
        zq0[k, 1] = high
        for side, j in ((0, 0), (1, groups - 1)):
            es[k, side] = put(0, low, j, 0) + put(0, high, j, 1)

    def pack_ends(k):
        low, rows = TOP - DEPTH, Y + 2 * DEPTH
        lane = iota((rows, LANES), 1)
        line, spot = lane // SPAN, lane % SPAN
        for g, p in ((0, 0), (groups + 1, DEPTH + X)):
            both = jnp.zeros((rows, LANES), jnp.float32)
            for i in range(PER):
                field = g0[k, p + i, low:low + rows, :]
                both = jnp.where((line == i) & (spot < half), turn(field, SPAN * i + quarter), both)
            gs[k, g, low:low + rows, :] = jnp.where(
                spot < quarter, both, jnp.where(spot >= 3 * quarter, turn(both, half), 0.0))

    def slots(l):
        return (0, 0, 0, dims[2][0] // DEPTH * 2)[l], dims[l][0] // DEPTH

    def put(l, x, source, target):
        lane = iota(x.shape, 1)
        return jnp.where(lane % SPAN // DEPTH == target, turn(x, DEPTH * (target - source)), 0.0)

    def pack_level(k, l):
        A, B, C = dims[l]
        base, many = slots(l)
        lane = iota((B, LANES), 1)
        line, slot = lane // SPAN, lane % SPAN // DEPTH
        out = jnp.zeros((B, LANES), jnp.float32)
        for i in range(A):
            field = fields[l][k, DEPTH + i, TOP:TOP + B, :]
            x, j = i % DEPTH, i // DEPTH
            lo, hi = base + j, base + many + j
            out = jnp.where((line == x) & (slot == lo), turn(field, SPAN * x + DEPTH * lo), out)
            out = jnp.where((line == x) & (slot == hi), turn(field, SPAN * x + DEPTH * hi - C + DEPTH), out)
        return out

    def pack_rest(k):
        one, two, three = [pack_level(k, l) for l in range(1, HALOED)]
        zq1[k] = one
        B1, B2, B3 = [dims[l][1] for l in range(1, HALOED)]
        zq2[k, 0:B2] = two
        for a in (0, B2 - B3):
            zq2[k, a:a + B3] = zq2[k, a:a + B3] + three
        for side in (0, 1):
            def edge(l, x):
                base, many = slots(l)
                j = many - 1 if side else 0
                return put(l, x, base + j, 2 * l) + put(l, x, base + many + j, 2 * l + 1)
            first, second, third = edge(1, one), edge(2, two), edge(3, three)
            for src, dst, size, part in (
                    (0, 0, B1 - DEPTH, first), (B1 - DEPTH, Y - DEPTH, DEPTH, first),
                    (0, 0, DEPTH, second), (B2 - DEPTH, Y - DEPTH, DEPTH, second),
                    (0, 0, DEPTH, third), (0, Y - DEPTH, DEPTH, third)):
                es[k, side, dst:dst + size] = es[k, side, dst:dst + size] + part[src:src + size]
            for x in range(DEPTH):
                p1, p2, p3 = [DEPTH + x + (dims[l][0] - DEPTH if side else 0) for l in range(1, HALOED)]
                xs[k, side, x] = g1[k, p1, TOP:TOP + B1, :]
                second = turn(g2[k, p2, TOP:TOP + B2, :], dims[1][2])
                third = turn(g3[k, p3, TOP:TOP + B3, :], dims[1][2] + dims[2][2])
                xs[k, side, x, 0:DEPTH] = xs[k, side, x, 0:DEPTH] + second[0:DEPTH] + third
                xs[k, side, x, B1 - DEPTH:B1] = xs[k, side, x, B1 - DEPTH:B1] + second[B2 - DEPTH:B2] + third

    def unpack_slab(k):
        low, rows = TOP - DEPTH, Y + 2 * DEPTH
        spot = iota((rows, LANES), 1) % SPAN
        for g in range(groups + 2):
            edge = 0 if g == 0 else 1 if g == groups + 1 else None
            if edge is None:
                above, below, up, down = zr0[k, 0], zr0[k, 1], g - 1, g - 1
            else:
                above, below, up, down = zx[k, 0, edge], zx[k, 1, edge], 0, 1
            held = gs[k, g, low:low + rows, :]
            held = jnp.where(spot // DEPTH == 2, turn(above, DEPTH * (2 - up)), held)
            hs[g, low:low + rows, :] = jnp.where(spot // DEPTH == 5, turn(below, DEPTH * (5 - down)), held)

    def unpack_level(k, l):
        A, B, C = dims[l]
        low, rows = TOP - DEPTH, B + 2 * DEPTH
        base, many = slots(l)
        lane = iota((rows, LANES), 1)

        def cut(ref, head):
            end = ref.shape[-2]
            tail = 0 if end == rows else (2 * DEPTH if B > DEPTH else DEPTH)
            a = ref[head + (slice(0, rows - tail),)]
            return jnp.concatenate([a, ref[head + (slice(end - tail, end),)]], axis=0) if tail else a

        ref = (None, zr1, zr2, zr2)[l]
        sides = [cut(ref, (k, 0)), cut(ref, (k, 1))]
        edges = [[cut(zx, (k, side, e)) for side in (0, 1)] for e in (0, 1)]
        start = sum(dims[i][2] for i in range(1, l))
        for p in range(A + 2 * DEPTH):
            edge = 0 if p < DEPTH else 1 if p >= DEPTH + A else None
            x, j = p % DEPTH, p // DEPTH - 1
            if edge is None:
                held = fields[l][k, p, low:low + rows, :]
                (above, below), up, down = sides, base + j, base + many + j
            else:
                held = jnp.where(lane < C, turn(cut(xf, (k, edge, x)), -start), 0.0)
                (above, below), up, down = edges[edge], 2 * l, 2 * l + 1
            held = jnp.where(lane // DEPTH == C // DEPTH, turn(above, C - SPAN * x - DEPTH * up), held)
            whole[l][p, low:low + rows, :] = jnp.where(
                lane >= LANES - DEPTH, turn(below, -DEPTH - SPAN * x - DEPTH * down), held)

    half_row = LANES // 2
    def own_row(k):
        lane = iota((1, LANES), 1)
        out, total = jnp.zeros((1, LANES), jnp.float32), None
        for i in range(CA):
            for j in range(CB):
                part = None
                for a in (0, 1):
                    for b in (0, 1):
                        y = TOP + 2 * j + b
                        one = fields[HALOED - 1][k, DEPTH + 2 * i + a, y:y + 1, :]
                        part = one if part is None else part + one
                part = halve(part, CC)
                out = jnp.where(lane // CC == i * CB + j, part, out)
                total = part if total is None else total + part
        return jnp.where((lane >= cells * CC) & (lane < cells * CC + CD), halve(total, CD), out)

    def coarse(k):
        rows = cr[k, :, 0, :]
        lane, row = iota((n, LANES), 1), iota((n, LANES), 0)
        parts = [jnp.where(lane // CC == row % nz, take(rows, cell * CC + lane % CC), 0.0) for cell in range(cells)]
        parts.append(jnp.where(lane // CD == row % nz, take(rows, cells * CC + lane % CD), 0.0))
        out = jnp.dot(pmat[...], jnp.concatenate(parts, axis=0), precision=HIGH, preferred_element_type=jnp.float32)
        out = out.reshape(-1, ROWS, LANES)
        last = smooth_whole(out[nx * CA:], ny, nz * CD, HALOED + 1)
        spread_y(last, spread)
        grown = take(spread[0:nx, 0:ROWS, :], iota((8, LANES), 1) // 2)
        wref[DEPTH // 2:DEPTH // 2 + nx * CA, :, :] = (
            twice(grown) + smooth_whole(out[:nx * CA], ny * CB, nz * CC, HALOED))

    def precondition(k, z, extra):
        start_all([main_copies(k)[i] for i, (dx, _) in enumerate(AROUND) if not dx])
        lane = iota((8, LANES), 1)
        sums = own(g0, 0, k)
        for l in range(1, HALOED):
            A, B, C = dims[l]
            sums = fold_xy(sums)
            sums = sums + turn(sums, -(1 << (l - 1)))
            coarser = jnp.where(lane[0:1][None] < C, take(sums, (1 << l) * (lane % C)) * 0.125 ** l, 0.0)
            fields[l][k, DEPTH:DEPTH + A, TOP:TOP + B, :] = coarser
        pack_slab(k)
        pack_rest(k)
        mine = own_row(k) if extra is None else jnp.where(iota((1, LANES), 1) < half_row, own_row(k), extra)
        cs[k] = mine
        cr[k, me] = mine
        start_far(k)
        to_all(cs.at[k], cr.at[k], csend.at[0], crecv.at[k])
        for s in range(1, SWEEPS):
            sweep_inside(after[0][s - 2] if s > 1 else g0.at[k], g0.at[k], after[0][s - 1], s)
        all_of(main_entries(), mrecv.at[k], -1)
        pack_ends(k)
        for s in range(1, SWEEPS):
            sweep_rim(after[0][s - 2] if s > 1 else g0.at[k], g0.at[k], after[0][s - 1], s)
        all_of(far_entries(), frecv.at[k], -1)
        unpack_slab(k)
        for l in range(1, HALOED):
            unpack_level(k, l)
        for s in range(1, SWEEPS):
            sweep_slab(after[HALOED][s - 2] if s > 1 else hs, hs, after[HALOED][s - 1])
            for l in range(1, HALOED):
                sweep(l, after[l][s - 2] if s > 1 else whole[l], whole[l], after[l][s - 1], s)
        all_done(cr.at[k], crecv.at[k])
        coarse(k)
        A, B, C = dims[HALOED - 1]
        spread_y(wref[pl.ds(at[0] * CA, CA + DEPTH)], wide, DEPTH)
        part = wide[:, 0:2 * ROWS, :]
        for j in range(1, ny):
            part = jnp.where(at[1] == j, wide[:, j * B:j * B + 2 * ROWS, :], part)
        source = (wrapped(lane) >> 1) + at[2] * CC
        inside = (source >= 0) & (source < CC * nz)
        part = take(part, jnp.where(inside, source, 0))
        part = jnp.where(inside[0:1][None], part, 0.0)
        part = twice(part)[DEPTH - 1:DEPTH + A + 1, 0:B + 2 * DEPTH]
        for l in range(HALOED - 1, 0, -1):
            A, B, C = dims[l]
            end = after[l][SWEEPS - 2][DEPTH - 1:DEPTH + A + 1, TOP - DEPTH:TOP + B + DEPTH, :]
            full = end * (4.0 ** l / 9.0) + part
            if l > 1:
                spread_y(take(full, (wrapped(lane) >> 1) & (LANES - 1)), spread)
                part = twice(spread[0:A + 2, DEPTH:DEPTH + 2 * B + 2 * DEPTH, :])[1:2 * A + 3]
            else:
                spread_y(take(full, lane // 2), pd)
                spread_y(take(full, jnp.where(lane == 0, LANES - 1, C)), pe)
        low, rows = TOP - DEPTH, Y + 2 * DEPTH
        slab = after[HALOED][SWEEPS - 2]
        spot = iota((rows, LANES), 1) % SPAN
        for g in range(groups + 2):
            s = slab[g, low:low + rows, :]
            sc[g] = jnp.where(spot < quarter, s, turn(s, -half))
            sd[g] = jnp.where(spot <= quarter, s, turn(s, quarter + 1 - (3 * quarter - 1)))
        lane = iota((rows, LANES), 1)
        near = (lane < DEPTH - 1) | (lane > LANES - DEPTH)
        end = after[0][SWEEPS - 2]
        for p in range(DEPTH - 1, DEPTH + X + 1):
            g, i = p // PER, p % PER
            f = jnp.where(near, turn(sc[g], -quarter - SPAN * i), end[p, low:low + rows, :])
            z[p, low:low + rows, :] = f * (1.0 / 9.0) + pd[(p - DEPTH + 2) // 2, low:low + rows, :]

    def around(ref, p):
        mid = ref[p, TOP:TOP + Y, :]
        total = ref[p - 1, TOP:TOP + Y, :] + ref[p + 1, TOP:TOP + Y, :]
        return mid, total + ref[p, TOP - 1:TOP - 1 + Y, :] + ref[p, TOP + 1:TOP + 1 + Y, :]

    lane = iota((Y, LANES), 1)
    first, last = lane == 0, lane == LANES - 1

    def operator(z, p):
        mid, total = around(z, p)
        g, i = p // PER, p % PER
        ghost = turn(sd[g, DEPTH:DEPTH + Y, :], LANES - 1 - quarter - SPAN * i) * (1.0 / 9.0)
        ghost = ghost + pe[(p - DEPTH + 2) // 2, TOP:TOP + Y, :]
        total = total + jnp.where(first, ghost, turn(mid, 1))
        total = total + jnp.where(last, ghost, turn(mid, -1))
        return mid, 6.0 * mid - total

    load_x.wait()
    out = jnp.zeros((Y, LANES), jnp.float32)
    for i in range(X):
        out = jnp.where(lane // 2 == i, turn(ux[1 + i, TOP:TOP + Y, :], 2 * i + 1), out)
    ze[...] = out
    pl.semaphore_wait(barrier, n - 1)
    start_all(face_copies())
    load_b.wait()
    for i in range(X):
        mid, total = around(ux, 1 + i)
        total = total + jnp.where(first, 0.0, turn(mid, 1))
        total = total + jnp.where(last, 0.0, turn(mid, -1))
        g0[0, DEPTH + i, TOP:TOP + Y, :] = bb[i] - (6.0 * mid - total)
    all_of(face_entries(), xrecv.at[0], -1)
    for i, side in ((0, 1), (X - 1, 0)):
        here = (0, DEPTH + i, slice(TOP, TOP + Y))
        g0[here] = g0[here] + xg[side]
    ghosts = jnp.where(lane % 2 == 0, turn(zi[1], -1), turn(zi[0], 1))

    def complete(a, b):
        for j, side in ((0, 1), (Y - 1, 0)):
            here = (0, slice(DEPTH + a, DEPTH + b), slice(TOP + j, TOP + j + 1))
            g0[here] = g0[here] + yg[side, a:b]
        for i in range(a, b):
            here = (0, DEPTH + i, slice(TOP, TOP + Y))
            g0[here] = g0[here] + jnp.where(first | last, turn(ghosts, -2 * i - 1), 0.0)

    def start_edges(k):
        start_all([main_copies(k)[i] for i, (dx, _) in enumerate(AROUND) if dx])

    complete(0, DEPTH)
    complete(X - DEPTH, X)
    start_edges(0)
    complete(DEPTH, X - DEPTH)

    def sums_of(a, b):
        lane = iota((1, LANES), 1)
        pair = jnp.concatenate([jnp.sum(a, axis=0, keepdims=True), jnp.sum(b, axis=0, keepdims=True)], axis=0)
        pair = pair + turn(pair, LANES // 2)
        pair = pair + turn(pair, LANES // 4)
        return jnp.where(lane < 3 * LANES // 4, pair[0:1], pair[1:2])

    def ratio(rows):
        lane = iota((1, LANES), 1)
        row = jnp.sum(rows, axis=0, keepdims=True)
        upper_half = jnp.where(lane >= 3 * LANES // 4, row, 0.0)
        lower_half = jnp.where((lane >= half_row) & (lane < 3 * LANES // 4), row, 0.0)
        return jnp.sum(lower_half, axis=1, keepdims=True) / jnp.sum(upper_half, axis=1, keepdims=True)

    nothing = jnp.zeros((Y, LANES), jnp.float32)
    precondition(0, z0, None)
    rz, zw = nothing, nothing
    inner = list(range(DEPTH, X - DEPTH))
    for i in [i for i in range(X) if i not in inner] + inner:
        if i == DEPTH:
            start_edges(1)
        mid, image = operator(z0, DEPTH + i)
        g0[1, DEPTH + i, TOP:TOP + Y, :] = image
        rz = rz + g0[0, DEPTH + i, TOP:TOP + Y, :] * mid
        zw = zw + mid * image
    precondition(1, z1, sums_of(rz, zw))
    alpha = ratio(cr[1, :, 0, :])
    rz, zw = nothing, nothing
    for i in range(X):
        mid, image = operator(z1, DEPTH + i)
        here = (DEPTH + i, slice(TOP, TOP + Y))
        before, w = z0[here], g0[(1,) + here]
        r = g0[(0,) + here] - alpha * w
        z = before - alpha * mid
        w = w - alpha * image
        rz = rz + r * z
        zw = zw + z * w
        sol_ref[i] = ux[1 + i, TOP:TOP + Y, :] + alpha * before
        z_ref[i] = z
        res_ref[i] = r
        w_ref[i] = w
    sums = sums_of(rz, zw)
    ds[...] = sums
    dr[me] = sums
    to_all(ds, dr, dsend.at[0], drecv.at[0])
    all_of(face_entries(), xsend.at[0], 1)
    all_of([(step, STEPS * c) for step, c in main_entries() + far_entries()], send.at[0], 1)
    part = cr.at[:, pl.ds(0, n - 1)]
    pltpu.make_async_copy(part, part, csend.at[0]).wait()
    all_done(dr, dsend.at[0])
    all_done(dr, drecv.at[0])
    alpha_ref[...] = jnp.broadcast_to(ratio(dr[:, 0, :]), alpha_ref.shape)


def finish(base, z, r, w, alpha, sol, res, sol_out, res_out, sem):
    X = base.shape[0]
    size = X // PARTS
    a = alpha[0:1, 0:1][None]
    copies = []
    for part in range(PARTS):
        here = slice(part * size, (part + 1) * size)
        sol_out[here] = base[here] + a * z[here]
        res_out[here] = r[here] - a * w[here]
        for i, (src, dst) in enumerate(((sol_out, sol), (res_out, res))):
            copies.append(pltpu.make_async_copy(src.at[here], dst.at[here], sem.at[i, part]))
            copies[-1].start()
    for copy in copies:
        copy.wait()


def solution(mesh):
    sizes = tuple(mesh.shape[a] for a in AXES)
    n = sizes[0] * sizes[1] * sizes[2]

    def run(right_side, guess):
        X, Y, Z = block = guess.shape
        assert Z == LANES and PER == DEPTH and X % PER == 0 and X * DEPTH <= LANES
        dims = [tuple(d >> l for d in block) for l in range(LEVELS)]
        f32 = jnp.float32
        vm = lambda *s: pltpu.VMEM(s, f32)
        ext = [(dims[l][0] + 2 * DEPTH, dims[l][1] + 2 * TOP, LANES) for l in range(HALOED)]
        slab = (X // PER + 2, Y + 2 * TOP, LANES)
        tall = [(dims[l][1] + 2 * DEPTH, LANES) for l in range(HALOED)]
        CA, CB, CC = dims[HALOED]
        assert dims[HALOED + 1][:2] == (1, 1) and sizes[1] * CB <= ROWS and CA * CB * CC + CC // 2 <= LANES // 2
        dma = lambda *s: pltpu.SemaphoreType.DMA(s)
        scratch = [
            vm(X + 2, Y + 2 * TOP, LANES), vm(*block),
            *(vm(STEPS, *e) for e in ext), vm(STEPS, *slab),
            *(vm(*e) for e in ext[1:]), vm(*slab),
            *(vm(*e) for e in ext + [slab] for _ in range(SWEEPS - 1)),
            vm(*ext[0]), vm(*ext[0]),
            vm(slab[0], *tall[0]), vm(slab[0], *tall[0]),
            vm(dims[1][0] + 2, 2 * tall[1][0], LANES), vm(dims[1][0] + 2, 2 * tall[1][0], LANES),
            *(vm(*t) for t in tall), vm(*tall[0]),
            vm((CA + 1) * sizes[0] * ROWS, (CA * CB + 1) * n),
            vm(CA * sizes[0] + DEPTH, ROWS, LANES),
            vm(CA + DEPTH, 4 * ROWS, LANES),
            vm(X // 2, Y, LANES), vm(X // 2, 2 * Y, LANES),
            vm(2, Y, LANES), vm(2, X, 1, LANES), vm(Y, LANES), vm(2, Y, LANES),
            vm(STEPS, 2, Y, LANES), vm(STEPS, dims[1][1], LANES), vm(STEPS, dims[2][1], LANES),
            *(vm(STEPS, 2, dims[l][1] + 2 * DEPTH, LANES) for l in range(HALOED - 1)),
            vm(STEPS, 2, Y, LANES), vm(STEPS, 2, 2, Y + 2 * DEPTH, LANES),
            vm(STEPS, 2, DEPTH, dims[1][1], LANES), vm(STEPS, 2, DEPTH, dims[1][1] + 2 * DEPTH, LANES),
            vm(STEPS, 1, LANES), vm(STEPS, n, 1, LANES),
            vm(1, LANES), vm(n, 1, LANES), vm(16 * STEPS * DEPTH * max(X, Y), LANES),
            dma(2), dma(1), dma(1), dma(STEPS), dma(1), dma(STEPS),
            dma(1), dma(STEPS), dma(1), dma(1),
        ]
        whole = pltpu.VMEM(block, f32)
        base, z, r, w, alpha = pl.pallas_call(
            functools.partial(kernel, sizes, block),
            out_shape=(whole, whole, whole, whole, pltpu.VMEM((8, LANES), f32)),
            in_specs=[pl.BlockSpec(memory_space=pl.ANY)] * 2,
            out_specs=[pl.BlockSpec(memory_space=pltpu.VMEM)] * 5,
            scratch_shapes=scratch,
            compiler_params=pltpu.CompilerParams(collective_id=0, has_side_effects=True),
        )(right_side, guess)
        inner = [pltpu.with_memory_space_constraint(v, pltpu.VMEM) for v in (base, z, r, w, alpha)]
        out = jax.ShapeDtypeStruct(block, f32)
        return tuple(pl.pallas_call(
            finish,
            out_shape=(out, out),
            in_specs=[pl.BlockSpec(memory_space=pltpu.VMEM)] * 5,
            out_specs=[pl.BlockSpec(memory_space=pl.ANY)] * 2,
            scratch_shapes=[vm(*block), vm(*block), dma(2, PARTS)],
        )(*inner))

    spec = P(*AXES)
    return jax.shard_map(run, mesh=mesh, in_specs=(spec, spec), out_specs=(spec, spec), check_vma=False)
```

```python
import functools

import jax
import jax.numpy as jnp
from jax import lax
from jax.experimental import pallas as pl
from jax.experimental.pallas import tpu as pltpu
from jax.sharding import PartitionSpec as P

LEVELS = 6
SWEEPS = 4
STEPS = 2
HALOED = 4
AXES = ("gx", "gy", "gz")
LANES = 128
TOP = 8
DEPTH = SWEEPS
SPAN = 8 * DEPTH
PER = LANES // SPAN
PARTS = 4
MESH = pl.DeviceIdType.MESH
HIGH = lax.Precision.HIGHEST
ROWS = 8
ALL = [(a, b, c) for c in (-1, 1, 0) for a in (0, -1, 1) for b in (0, -1, 1) if (a, b, c) != (0, 0, 0)]
AROUND = [(a, b) for a in (-1, 0, 1) for b in (-1, 0, 1) if (a, b) != (0, 0)]
FACES = [(d, s) for d in range(3) for s in (-1, 1)]


def iota(shape, dim):
    return lax.broadcasted_iota(jnp.int32, shape, dim)


def take(x, index):
    if x.ndim == 3:
        return jnp.stack([take(x[i], index) for i in range(x.shape[0])])
    rows = x.shape[0]
    more = -rows % 8
    if rows == 1:
        x = jnp.broadcast_to(x, (8, LANES))
    elif more:
        x = jnp.concatenate([x, jnp.zeros((more, LANES), x.dtype)], axis=0)
    index = jnp.broadcast_to(index[:1], x.shape)
    out = jnp.take_along_axis(x, index, axis=1, mode="promise_in_bounds")
    return out[:rows] if more else out


def wrapped(lane):
    return jnp.where(lane >= LANES - DEPTH, lane - LANES, lane)


def halve(x, width):
    lane = iota((8, LANES), 1)
    return take(x + turn(x, -1), 2 * (lane % width)) * 0.125


def turn(x, shift):
    shift = shift % LANES
    return pltpu.roll(x, shift, x.ndim - 1) if shift else x


def kernel(sizes, block, b_hbm, x_hbm, sol_ref, z_ref, res_ref, w_ref, alpha_ref, *rest):
    (ux, bb, g0, g1, g2, g3, gs, h1, h2, h3, hs, f0a, f0b, f0c, f1a, f1b, f1c, f2a, f2b, f2c, f3a, f3b, f3c, fsa, fsb, fsc,
     z0, z1, sc, sd, pd, pe, m0, m1, m2, m3, ms, pmat, wref, wide, fold, spread, xg, yg, ze, zi, zq0, zq1, zq2, zr0, zr1, zr2, es, zx, xs, xf, cs, cr, ds, dr, blank,
     isem, xsend, xrecv, frecv, send, mrecv, csend, crecv, dsend, drecv) = rest
    nx, ny, nz = sizes
    n = nx * ny * nz
    at = tuple(lax.axis_index(a) for a in AXES)
    me = (at[0] * ny + at[1]) * nz + at[2]
    dims = [tuple(d >> l for d in block) for l in range(LEVELS)]
    X, Y, Z = block
    fields = (g0, g1, g2, g3)
    after = ((f0a, f0b, f0c), (f1a, f1b, f1c), (f2a, f2b, f2c), (f3a, f3b, f3c), (fsa, fsb, fsc))
    masks = (m0, m1, m2, m3)
    whole = (None, h1, h2, h3, hs)
    groups = X // PER
    lower = [at[d] > 0 for d in range(3)]
    upper = [at[d] < sizes[d] - 1 for d in range(3)]
    inlow = [jnp.where(c, 1.0, 0.0) for c in lower]
    inup = [jnp.where(c, 1.0, 0.0) for c in upper]

    load_x = pltpu.make_async_copy(x_hbm, ux.at[1:X + 1, TOP:TOP + Y], isem.at[0])
    load_b = pltpu.make_async_copy(b_hbm, bb, isem.at[1])
    load_x.start()
    load_b.start()

    def others():
        out = []
        for b in range(ny - 1, -1, -1):
            for c in range(nz - 1, -1, -1):
                for a in range(nx):
                    if b or c:
                        first = jnp.where(at[0] < nx // 2, nx - 1 - a, a)
                    elif a:
                        first = lax.rem(at[0] + a, nx)
                    else:
                        continue
                    out.append((first, lax.rem(at[1] + b, ny), lax.rem(at[2] + c, nz)))
        return out

    barrier = pltpu.get_barrier_semaphore()
    for target in others():
        pl.semaphore_signal(barrier, inc=1, device_id=target, device_id_type=MESH)

    def outside(dim, side):
        for l in range(HALOED + 1):
            A, B = (groups if l == HALOED else dims[l][0]), (Y if l == HALOED else dims[l][1])
            d, ref = (1, gs) if l == HALOED else (DEPTH, fields[l])
            for k in range(STEPS):
                if dim == 0:
                    a = A + d if side else 0
                    ref[k, a:a + d, TOP - DEPTH:TOP + B + DEPTH, :] = jnp.zeros((d, B + 2 * DEPTH, LANES), jnp.float32)
                else:
                    a = TOP + B if side else TOP - DEPTH
                    ref[k, :, a:a + DEPTH, :] = jnp.zeros((A + 2 * d, DEPTH, LANES), jnp.float32)

    far = (zr0, zr1, zr2, zx, xf)

    def nothing_in(ref):
        ref[...] = jnp.zeros(ref.shape, jnp.float32)

    for side in (0, 1):
        for dim in range(2):
            @pl.when(jnp.logical_not((upper if side else lower)[dim]))
            def _(dim=dim, side=side):
                outside(dim, side)
                nothing_in((xg, yg)[dim].at[1 - side])
                for ref in far if dim else ():
                    head = (slice(None),) * (len(ref.shape) - 2)
                    a = ref.shape[-2] - DEPTH if side else 0
                    nothing_in(ref.at[head + (slice(a, a + DEPTH),)])
                if dim == 0:
                    nothing_in(zx.at[:, :, side])
                    nothing_in(xf.at[:, side])
        @pl.when(jnp.logical_not((upper if side else lower)[2]))
        def _(side=side):
            nothing_in(zi.at[side])
            for ref in far[:4]:
                nothing_in(ref.at[:, 1 - side])

    ux[:, TOP - 1:TOP, :] = jnp.zeros((X + 2, 1, LANES), jnp.float32)
    ux[:, TOP + Y:TOP + Y + 1, :] = jnp.zeros((X + 2, 1, LANES), jnp.float32)
    ux[0, TOP:TOP + Y, :] = jnp.zeros((Y, LANES), jnp.float32)
    ux[X + 1, TOP:TOP + Y, :] = jnp.zeros((Y, LANES), jnp.float32)
    wref[...] = jnp.zeros_like(wref)
    wide[...] = jnp.zeros_like(wide)

    def mask(rows, z, depth_z):
        y = iota((rows + 2 * DEPTH, LANES), 0) - DEPTH
        part = jnp.where(y < 0, inlow[1], jnp.where(y >= rows, inup[1], 1.0))
        return part * jnp.where(z < 0, inlow[2], jnp.where(z >= depth_z, inup[2], 1.0)) * (1.0 / 9.0)

    for l in range(HALOED):
        lane = iota((dims[l][1] + 2 * DEPTH, LANES), 1)
        masks[l][...] = mask(dims[l][1], lane if l == 0 else wrapped(lane), dims[l][2])
    CA, CB, CC = dims[HALOED]
    CD = dims[HALOED + 1][2]
    cells = CA * CB
    row, column = iota(pmat.shape, 0), iota(pmat.shape, 1)
    cell, device = column // n, column % n
    plane, line = row // ROWS, row % ROWS
    dx, dy = device // (ny * nz), device // nz % ny
    fits = (cell < cells) & (plane == dx * CA + cell // CB) & (line == dy * CB + cell % CB)
    fits = fits | ((cell == cells) & (plane == nx * CA + dx) & (line == dy))
    pmat[...] = jnp.where(fits, 1.0, 0.0)
    lane = iota((Y + 2 * DEPTH, LANES), 1) % SPAN
    ms[...] = mask(Y, jnp.where(lane < SPAN // 2, lane + Z - SPAN // 4, lane - 3 * SPAN // 4), Z)

    def face_copies():
        out = []
        for i, (d, s) in enumerate(FACES):
            target = list(at)
            target[d] = at[d] + s
            into = 1 if s > 0 else 0
            if d == 0:
                src, dst = ux.at[X if s > 0 else 1, TOP:TOP + Y], xg.at[into]
            elif d == 1:
                a = TOP + Y - 1 if s > 0 else TOP
                src, dst = ux.at[1:X + 1, a:a + 1], yg.at[into]
            else:
                src, dst = ze, zi.at[0 if s > 0 else 1]
            copy = pltpu.make_async_remote_copy(
                src_ref=src, dst_ref=dst, send_sem=xsend.at[0], recv_sem=xrecv.at[0],
                device_id=tuple(target), device_id_type=MESH,
            )
            out.append((copy, upper[d] if s > 0 else lower[d], lower[d] if s > 0 else upper[d]))
        return out

    def span(step, depth, start, own, other):
        if step > 0:
            return (start + own - depth, depth), (start - depth, depth)
        if step < 0:
            return (start, depth), (start + own, depth)
        return (start, own), (start, own)

    def around_copies(ref, k, depth, planes, rows, rsem):
        out = []
        for i, (dx, dy) in enumerate(AROUND):
            (sx, lx), (tx, _) = span(dx, depth, depth, planes, None)
            (sy, ly), (ty, _) = span(dy, DEPTH, TOP, rows, None)
            copy = pltpu.make_async_remote_copy(
                src_ref=ref.at[k, sx:sx + lx, sy:sy + ly], dst_ref=ref.at[k, tx:tx + lx, ty:ty + ly],
                send_sem=send.at[0], recv_sem=rsem.at[k],
                device_id=(at[0] + dx, at[1] + dy, at[2]), device_id_type=MESH,
            )
            to, fro = None, None
            for d, s in ((0, dx), (1, dy)):
                if s:
                    a, b = (upper[d], lower[d]) if s > 0 else (lower[d], upper[d])
                    to = a if to is None else jnp.logical_and(to, a)
                    fro = b if fro is None else jnp.logical_and(fro, b)
            out.append((copy, to, fro, lx * ly))
        return out

    def main_copies(k):
        return around_copies(g0, k, DEPTH, X, Y, mrecv)

    def rows_of(dy, rows):
        if dy > 0:
            return pl.ds(rows - DEPTH, DEPTH), pl.ds(0, DEPTH), DEPTH
        if dy < 0:
            return pl.ds(0, DEPTH), pl.ds(rows + DEPTH, DEPTH), DEPTH
        return pl.ds(0, rows), pl.ds(DEPTH, rows), rows

    def every(conds):
        out = None
        for cond in conds:
            out = cond if out is None else jnp.logical_and(out, cond)
        return out

    def far_copies(k):
        out = []
        for i, (dx, dy, dz) in enumerate(ALL):
            step = (dx, dy, dz)
            to = every([(upper if t > 0 else lower)[d] for d, t in enumerate(step) if t])
            fro = every([(lower if t > 0 else upper)[d] for d, t in enumerate(step) if t])
            from_x, into_x = (1, 0) if dx > 0 else (0, 1)
            side = 1 if dz > 0 else 0
            pairs = []
            if dz and dx:
                a, b, c = rows_of(dy, Y)
                pairs.append((es.at[k, from_x, a], zx.at[k, side, into_x, b], c))
            elif dz:
                for src, dst in ((zq0.at[k, side], zr0), (zq1.at[k], zr1), (zq2.at[k], zr2)):
                    a, b, c = rows_of(dy, src.shape[0])
                    pairs.append((src.at[a], dst.at[k, side, b], c))
            else:
                arrays = []
                if dx:
                    a, b, c = rows_of(dy, dims[1][1])
                    pairs.append((xs.at[k, from_x, :, a], xf.at[k, into_x, :, b], DEPTH * c))
                else:
                    arrays = [(gs, 1, groups, Y)]
                    arrays += [(fields[l], DEPTH, dims[l][0], dims[l][1]) for l in range(1, HALOED)]
                for ref, depth, planes, rows in arrays:
                    (sx, lx), (tx, _) = span(dx, depth, depth, planes, None)
                    (sy, ly), (ty, _) = span(dy, DEPTH, TOP, rows, None)
                    pairs.append((ref.at[k, sx:sx + lx, sy:sy + ly], ref.at[k, tx:tx + lx, ty:ty + ly], lx * ly))
            copies = [pltpu.make_async_remote_copy(
                src_ref=src, dst_ref=dst, send_sem=send.at[0], recv_sem=frecv.at[k],
                device_id=(at[0] + dx, at[1] + dy, at[2] + dz), device_id_type=MESH,
            ) for src, dst, _ in pairs]
            out.append((copies, to, fro, sum(c for _, _, c in pairs)))
        return out

    def bytes_done(count, sem):
        assert count <= blank.shape[0]
        part = blank.at[pl.ds(0, count)]
        pltpu.make_async_copy(part, part, sem).wait()

    def all_of(entries, sem, sign):
        def nest(d, have):
            if d == len(sizes):
                total = sum(c for step, c in entries if all(t == 0 or sign * t in have[i] for i, t in enumerate(step)))
                if total:
                    bytes_done(total, sem)
            elif sizes[d] == 1 or not any(step[d] for step, _ in entries):
                nest(d + 1, have + [()])
            else:
                pl.when(jnp.logical_not(lower[d]))(lambda: nest(d + 1, have + [(1,)]))
                pl.when(jnp.logical_not(upper[d]))(lambda: nest(d + 1, have + [(-1,)]))
                if sizes[d] > 2:
                    pl.when(jnp.logical_and(lower[d], upper[d]))(lambda: nest(d + 1, have + [(-1, 1)]))

        nest(0, [])

    def main_entries():
        return [((dx, dy, 0), entry[3]) for (dx, dy), entry in zip(AROUND, main_copies(0))]

    def far_entries():
        return [(step, entry[3]) for step, entry in zip(ALL, far_copies(0))]

    def face_entries():
        return [(tuple(s if i == d else 0 for i in range(3)), X if d == 1 else Y) for d, s in FACES]

    def start_all(copies):
        for copy, cond, *_ in copies:
            pl.when(cond)(copy.start)

    def start_far(k):
        for copies, to, _, _ in far_copies(k):
            @pl.when(to)
            def _(copies=copies):
                for copy in copies:
                    copy.start()

    def to_all(src, dst, s_sem, r_sem):
        for target in others():
            pltpu.make_async_remote_copy(
                src_ref=src, dst_ref=dst.at[me], send_sem=s_sem, recv_sem=r_sem,
                device_id=target, device_id_type=MESH,
            ).start()

    def all_done(dst, sem):
        part = dst.at[pl.ds(0, n - 1)]
        pltpu.make_async_copy(part, part, sem).wait()

    def fold_xy(field):
        A, B, _ = field.shape
        pairs = field.reshape(A // 2, 2, B, LANES)
        fold[0:A // 2, 0:B, :] = pairs[:, 0] + pairs[:, 1]
        return fold[0:A // 2, pl.ds(0, B // 2, 2), :] + fold[0:A // 2, pl.ds(1, B // 2, 2), :]

    def spread_y(field, into, first=0):
        A, B, _ = field.shape
        into[0:A, pl.ds(first, B, 2), :] = field
        into[0:A, pl.ds(first + 1, B, 2), :] = field

    def twice(field):
        A, B, _ = field.shape
        return jnp.broadcast_to(field[:, None], (A, 2, B, LANES)).reshape(2 * A, B, LANES)

    def own(ref, l, k=None):
        A, B, _ = dims[l]
        return ref[(k,) * (k is not None) + (slice(DEPTH, DEPTH + A), slice(TOP, TOP + B))]

    def update(src, rhs, dst, a, c, low, rows, scale):
        at_rows = slice(low, low + rows)
        mid = src[a:a + c, at_rows, :]
        total = src[a - 1:a - 1 + c, at_rows, :] + src[a + 1:a + 1 + c, at_rows, :]
        total = total + src[a:a + c, low - 1:low - 1 + rows, :] + src[a:a + c, low + 1:low + 1 + rows, :]
        total = total + turn(mid, 1) + turn(mid, -1)
        dst[a:a + c, at_rows, :] = rhs[a:a + c, at_rows, :] + (3.0 * mid + total) * scale

    def pieces(a, b):
        return [(p, min(4, b - p)) for p in range(a, b, 4)]

    def sweep(l, src, rhs, dst, k):
        A, B, _ = dims[l]
        low, rows = TOP - DEPTH, B + 2 * DEPTH
        m = masks[l][...]
        update(src, rhs, dst, k, DEPTH - k, low, rows, m * inlow[0])
        for a, c in pieces(DEPTH, DEPTH + A):
            update(src, rhs, dst, a, c, low, rows, m)
        update(src, rhs, dst, DEPTH + A, DEPTH - k, low, rows, m * inup[0])

    def sweep_inside(src, rhs, dst, k):
        for a, c in pieces(DEPTH + k, DEPTH + X - k):
            update(src, rhs, dst, a, c, TOP + k, Y - 2 * k, 1.0 / 9.0)

    def sweep_rim(src, rhs, dst, k):
        low, rows = TOP - DEPTH, Y + 2 * DEPTH
        m = m0[...]
        update(src, rhs, dst, k, DEPTH - k, low, rows, m * inlow[0])
        update(src, rhs, dst, DEPTH, k, low, rows, m)
        update(src, rhs, dst, DEPTH + X - k, k, low, rows, m)
        update(src, rhs, dst, DEPTH + X, DEPTH - k, low, rows, m * inup[0])
        for start in (0, Y):
            edge = m0[start:start + 2 * DEPTH, :]
            for a, c in pieces(DEPTH + k, DEPTH + X - k):
                update(src, rhs, dst, a, c, low + start, 2 * DEPTH, edge)

    def sweep_slab(src, rhs, dst):
        low, rows = TOP - DEPTH, Y + 2 * DEPTH
        lane = iota((rows, LANES), 1)
        m = ms[...]
        for g in range(groups + 2):
            mid = src[g, low:low + rows, :]
            total = src[g, low - 1:low - 1 + rows, :] + src[g, low + 1:low + 1 + rows, :]
            total = total + turn(mid, 1) + turn(mid, -1)
            before = mid if g == 0 else jnp.where(lane >= LANES - SPAN, src[g - 1, low:low + rows, :], mid)
            behind = mid if g == groups + 1 else jnp.where(lane < SPAN, src[g + 1, low:low + rows, :], mid)
            total = total + turn(before, SPAN) + turn(behind, -SPAN)
            scale = m * inlow[0] if g == 0 else m * inup[0] if g == groups + 1 else m
            dst[g, low:low + rows, :] = rhs[g, low:low + rows, :] + (3.0 * mid + total) * scale

    def smooth_whole(rhs, depth_y, depth_z, l):
        A, B, _ = rhs.shape
        lane, row = iota(rhs.shape, 2), iota(rhs.shape, 1)
        e = rhs
        for _ in range(SWEEPS - 1):
            px, py = jnp.zeros((1, B, LANES), jnp.float32), jnp.zeros((A, 1, LANES), jnp.float32)
            total = jnp.concatenate([px, e[:-1]], axis=0) + jnp.concatenate([e[1:], px], axis=0)
            total = total + jnp.concatenate([py, e[:, :-1]], axis=1) + jnp.concatenate([e[:, 1:], py], axis=1)
            total = total + jnp.where(lane == 0, 0.0, turn(e, 1))
            total = total + jnp.where(lane == depth_z - 1, 0.0, turn(e, -1))
            e = rhs + jnp.where(row < depth_y, (3.0 * e + total) * (1.0 / 9.0), 0.0)
        return e * (4.0 ** l / 9.0)

    half, quarter = SPAN // 2, SPAN // 4

    def pack_slab(k):
        lane = iota((Y, LANES), 1)
        line, spot = lane // SPAN, lane % SPAN
        low = high = jnp.zeros((Y, LANES), jnp.float32)
        for g in range(groups):
            both = jnp.zeros((Y, LANES), jnp.float32)
            for i in range(PER):
                field = g0[k, DEPTH + g * PER + i, TOP:TOP + Y, :]
                both = jnp.where((line == i) & (spot < half), turn(field, SPAN * i + quarter), both)
            gs[k, g + 1, TOP:TOP + Y, :] = jnp.where(
                spot < quarter, both, jnp.where(spot >= 3 * quarter, turn(both, half), 0.0))
            here = spot // DEPTH == g
            low = jnp.where(here, turn(both, DEPTH * g - quarter), low)
            high = jnp.where(here, turn(both, DEPTH * g - quarter + DEPTH), high)
        zq0[k, 0] = low
        zq0[k, 1] = high
        for side, j in ((0, 0), (1, groups - 1)):
            es[k, side] = put(0, low, j, 0) + put(0, high, j, 1)

    def pack_ends(k):
        low, rows = TOP - DEPTH, Y + 2 * DEPTH
        lane = iota((rows, LANES), 1)
        line, spot = lane // SPAN, lane % SPAN
        for g, p in ((0, 0), (groups + 1, DEPTH + X)):
            both = jnp.zeros((rows, LANES), jnp.float32)
            for i in range(PER):
                field = g0[k, p + i, low:low + rows, :]
                both = jnp.where((line == i) & (spot < half), turn(field, SPAN * i + quarter), both)
            gs[k, g, low:low + rows, :] = jnp.where(
                spot < quarter, both, jnp.where(spot >= 3 * quarter, turn(both, half), 0.0))

    def slots(l):
        return (0, 0, 0, dims[2][0] // DEPTH * 2)[l], dims[l][0] // DEPTH

    def put(l, x, source, target):
        lane = iota(x.shape, 1)
        return jnp.where(lane % SPAN // DEPTH == target, turn(x, DEPTH * (target - source)), 0.0)

    def pack_level(k, l):
        A, B, C = dims[l]
        base, many = slots(l)
        lane = iota((B, LANES), 1)
        line, slot = lane // SPAN, lane % SPAN // DEPTH
        out = jnp.zeros((B, LANES), jnp.float32)
        for i in range(A):
            field = fields[l][k, DEPTH + i, TOP:TOP + B, :]
            x, j = i % DEPTH, i // DEPTH
            lo, hi = base + j, base + many + j
            out = jnp.where((line == x) & (slot == lo), turn(field, SPAN * x + DEPTH * lo), out)
            out = jnp.where((line == x) & (slot == hi), turn(field, SPAN * x + DEPTH * hi - C + DEPTH), out)
        return out

    def pack_rest(k):
        one, two, three = [pack_level(k, l) for l in range(1, HALOED)]
        zq1[k] = one
        B1, B2, B3 = [dims[l][1] for l in range(1, HALOED)]
        zq2[k, 0:B2] = two
        for a in (0, B2 - B3):
            zq2[k, a:a + B3] = zq2[k, a:a + B3] + three
        for side in (0, 1):
            def edge(l, x):
                base, many = slots(l)
                j = many - 1 if side else 0
                return put(l, x, base + j, 2 * l) + put(l, x, base + many + j, 2 * l + 1)
            first, second, third = edge(1, one), edge(2, two), edge(3, three)
            for src, dst, size, part in (
                    (0, 0, B1 - DEPTH, first), (B1 - DEPTH, Y - DEPTH, DEPTH, first),
                    (0, 0, DEPTH, second), (B2 - DEPTH, Y - DEPTH, DEPTH, second),
                    (0, 0, DEPTH, third), (0, Y - DEPTH, DEPTH, third)):
                es[k, side, dst:dst + size] = es[k, side, dst:dst + size] + part[src:src + size]
            for x in range(DEPTH):
                p1, p2, p3 = [DEPTH + x + (dims[l][0] - DEPTH if side else 0) for l in range(1, HALOED)]
                xs[k, side, x] = g1[k, p1, TOP:TOP + B1, :]
                second = turn(g2[k, p2, TOP:TOP + B2, :], dims[1][2])
                third = turn(g3[k, p3, TOP:TOP + B3, :], dims[1][2] + dims[2][2])
                xs[k, side, x, 0:DEPTH] = xs[k, side, x, 0:DEPTH] + second[0:DEPTH] + third
                xs[k, side, x, B1 - DEPTH:B1] = xs[k, side, x, B1 - DEPTH:B1] + second[B2 - DEPTH:B2] + third

    def unpack_slab(k):
        low, rows = TOP - DEPTH, Y + 2 * DEPTH
        spot = iota((rows, LANES), 1) % SPAN
        for g in range(groups + 2):
            edge = 0 if g == 0 else 1 if g == groups + 1 else None
            if edge is None:
                above, below, up, down = zr0[k, 0], zr0[k, 1], g - 1, g - 1
            else:
                above, below, up, down = zx[k, 0, edge], zx[k, 1, edge], 0, 1
            held = gs[k, g, low:low + rows, :]
            held = jnp.where(spot // DEPTH == 2, turn(above, DEPTH * (2 - up)), held)
            hs[g, low:low + rows, :] = jnp.where(spot // DEPTH == 5, turn(below, DEPTH * (5 - down)), held)

    def unpack_level(k, l):
        A, B, C = dims[l]
        low, rows = TOP - DEPTH, B + 2 * DEPTH
        base, many = slots(l)
        lane = iota((rows, LANES), 1)

        def cut(ref, head):
            end = ref.shape[-2]
            tail = 0 if end == rows else (2 * DEPTH if B > DEPTH else DEPTH)
            a = ref[head + (slice(0, rows - tail),)]
            return jnp.concatenate([a, ref[head + (slice(end - tail, end),)]], axis=0) if tail else a

        ref = (None, zr1, zr2, zr2)[l]
        sides = [cut(ref, (k, 0)), cut(ref, (k, 1))]
        edges = [[cut(zx, (k, side, e)) for side in (0, 1)] for e in (0, 1)]
        start = sum(dims[i][2] for i in range(1, l))
        for p in range(A + 2 * DEPTH):
            edge = 0 if p < DEPTH else 1 if p >= DEPTH + A else None
            x, j = p % DEPTH, p // DEPTH - 1
            if edge is None:
                held = fields[l][k, p, low:low + rows, :]
                (above, below), up, down = sides, base + j, base + many + j
            else:
                held = jnp.where(lane < C, turn(cut(xf, (k, edge, x)), -start), 0.0)
                (above, below), up, down = edges[edge], 2 * l, 2 * l + 1
            held = jnp.where(lane // DEPTH == C // DEPTH, turn(above, C - SPAN * x - DEPTH * up), held)
            whole[l][p, low:low + rows, :] = jnp.where(
                lane >= LANES - DEPTH, turn(below, -DEPTH - SPAN * x - DEPTH * down), held)

    half_row = LANES // 2
    def own_row(k):
        lane = iota((1, LANES), 1)
        out, total = jnp.zeros((1, LANES), jnp.float32), None
        for i in range(CA):
            for j in range(CB):
                part = None
                for a in (0, 1):
                    for b in (0, 1):
                        y = TOP + 2 * j + b
                        one = fields[HALOED - 1][k, DEPTH + 2 * i + a, y:y + 1, :]
                        part = one if part is None else part + one
                part = halve(part, CC)
                out = jnp.where(lane // CC == i * CB + j, part, out)
                total = part if total is None else total + part
        return jnp.where((lane >= cells * CC) & (lane < cells * CC + CD), halve(total, CD), out)

    def coarse(k):
        rows = cr[k, :, 0, :]
        lane, row = iota((n, LANES), 1), iota((n, LANES), 0)
        parts = [jnp.where(lane // CC == row % nz, take(rows, cell * CC + lane % CC), 0.0) for cell in range(cells)]
        parts.append(jnp.where(lane // CD == row % nz, take(rows, cells * CC + lane % CD), 0.0))
        out = jnp.dot(pmat[...], jnp.concatenate(parts, axis=0), precision=HIGH, preferred_element_type=jnp.float32)
        out = out.reshape(-1, ROWS, LANES)
        last = smooth_whole(out[nx * CA:], ny, nz * CD, HALOED + 1)
        spread_y(last, spread)
        grown = take(spread[0:nx, 0:ROWS, :], iota((8, LANES), 1) // 2)
        wref[DEPTH // 2:DEPTH // 2 + nx * CA, :, :] = (
            twice(grown) + smooth_whole(out[:nx * CA], ny * CB, nz * CC, HALOED))

    def precondition(k, z, extra):
        start_all([main_copies(k)[i] for i, (dx, _) in enumerate(AROUND) if not dx])
        lane = iota((8, LANES), 1)
        sums = own(g0, 0, k)
        for l in range(1, HALOED):
            A, B, C = dims[l]
            sums = fold_xy(sums)
            sums = sums + turn(sums, -(1 << (l - 1)))
            coarser = jnp.where(lane[0:1][None] < C, take(sums, (1 << l) * (lane % C)) * 0.125 ** l, 0.0)
            fields[l][k, DEPTH:DEPTH + A, TOP:TOP + B, :] = coarser
        pack_slab(k)
        pack_rest(k)
        mine = own_row(k) if extra is None else jnp.where(iota((1, LANES), 1) < half_row, own_row(k), extra)
        cs[k] = mine
        cr[k, me] = mine
        start_far(k)
        to_all(cs.at[k], cr.at[k], csend.at[0], crecv.at[k])
        for s in range(1, SWEEPS):
            sweep_inside(after[0][s - 2] if s > 1 else g0.at[k], g0.at[k], after[0][s - 1], s)
        all_of(main_entries(), mrecv.at[k], -1)
        pack_ends(k)
        for s in range(1, SWEEPS):
            sweep_rim(after[0][s - 2] if s > 1 else g0.at[k], g0.at[k], after[0][s - 1], s)
        all_of(far_entries(), frecv.at[k], -1)
        unpack_slab(k)
        for l in range(1, HALOED):
            unpack_level(k, l)
        for s in range(1, SWEEPS):
            sweep_slab(after[HALOED][s - 2] if s > 1 else hs, hs, after[HALOED][s - 1])
            for l in range(1, HALOED):
                sweep(l, after[l][s - 2] if s > 1 else whole[l], whole[l], after[l][s - 1], s)
        all_done(cr.at[k], crecv.at[k])
        coarse(k)
        A, B, C = dims[HALOED - 1]
        spread_y(wref[pl.ds(at[0] * CA, CA + DEPTH)], wide, DEPTH)
        part = wide[:, 0:2 * ROWS, :]
        for j in range(1, ny):
            part = jnp.where(at[1] == j, wide[:, j * B:j * B + 2 * ROWS, :], part)
        source = (wrapped(lane) >> 1) + at[2] * CC
        inside = (source >= 0) & (source < CC * nz)
        part = take(part, jnp.where(inside, source, 0))
        part = jnp.where(inside[0:1][None], part, 0.0)
        part = twice(part)[DEPTH - 1:DEPTH + A + 1, 0:B + 2 * DEPTH]
        for l in range(HALOED - 1, 0, -1):
            A, B, C = dims[l]
            end = after[l][SWEEPS - 2][DEPTH - 1:DEPTH + A + 1, TOP - DEPTH:TOP + B + DEPTH, :]
            full = end * (4.0 ** l / 9.0) + part
            if l > 1:
                spread_y(take(full, (wrapped(lane) >> 1) & (LANES - 1)), spread)
                part = twice(spread[0:A + 2, DEPTH:DEPTH + 2 * B + 2 * DEPTH, :])[1:2 * A + 3]
            else:
                spread_y(take(full, lane // 2), pd)
                spread_y(take(full, jnp.where(lane == 0, LANES - 1, C)), pe)
        low, rows = TOP - DEPTH, Y + 2 * DEPTH
        slab = after[HALOED][SWEEPS - 2]
        spot = iota((rows, LANES), 1) % SPAN
        for g in range(groups + 2):
            s = slab[g, low:low + rows, :]
            sc[g] = jnp.where(spot < quarter, s, turn(s, -half))
            sd[g] = jnp.where(spot <= quarter, s, turn(s, quarter + 1 - (3 * quarter - 1)))
        lane = iota((rows, LANES), 1)
        near = (lane < DEPTH - 1) | (lane > LANES - DEPTH)
        end = after[0][SWEEPS - 2]
        for p in range(DEPTH - 1, DEPTH + X + 1):
            g, i = p // PER, p % PER
            f = jnp.where(near, turn(sc[g], -quarter - SPAN * i), end[p, low:low + rows, :])
            z[p, low:low + rows, :] = f * (1.0 / 9.0) + pd[(p - DEPTH + 2) // 2, low:low + rows, :]

    def around(ref, p):
        mid = ref[p, TOP:TOP + Y, :]
        total = ref[p - 1, TOP:TOP + Y, :] + ref[p + 1, TOP:TOP + Y, :]
        return mid, total + ref[p, TOP - 1:TOP - 1 + Y, :] + ref[p, TOP + 1:TOP + 1 + Y, :]

    lane = iota((Y, LANES), 1)
    first, last = lane == 0, lane == LANES - 1

    def operator(z, p):
        mid, total = around(z, p)
        g, i = p // PER, p % PER
        ghost = turn(sd[g, DEPTH:DEPTH + Y, :], LANES - 1 - quarter - SPAN * i) * (1.0 / 9.0)
        ghost = ghost + pe[(p - DEPTH + 2) // 2, TOP:TOP + Y, :]
        total = total + jnp.where(first, ghost, turn(mid, 1))
        total = total + jnp.where(last, ghost, turn(mid, -1))
        return mid, 6.0 * mid - total

    load_x.wait()
    out = jnp.zeros((Y, LANES), jnp.float32)
    for i in range(X):
        out = jnp.where(lane // 2 == i, turn(ux[1 + i, TOP:TOP + Y, :], 2 * i + 1), out)
    ze[...] = out
    pl.semaphore_wait(barrier, n - 1)
    start_all(face_copies())
    load_b.wait()
    for i in range(X):
        mid, total = around(ux, 1 + i)
        total = total + jnp.where(first, 0.0, turn(mid, 1))
        total = total + jnp.where(last, 0.0, turn(mid, -1))
        g0[0, DEPTH + i, TOP:TOP + Y, :] = bb[i] - (6.0 * mid - total)
    all_of(face_entries(), xrecv.at[0], -1)
    for i, side in ((0, 1), (X - 1, 0)):
        here = (0, DEPTH + i, slice(TOP, TOP + Y))
        g0[here] = g0[here] + xg[side]
    ghosts = jnp.where(lane % 2 == 0, turn(zi[1], -1), turn(zi[0], 1))

    def complete(a, b):
        for j, side in ((0, 1), (Y - 1, 0)):
            here = (0, slice(DEPTH + a, DEPTH + b), slice(TOP + j, TOP + j + 1))
            g0[here] = g0[here] + yg[side, a:b]
        for i in range(a, b):
            here = (0, DEPTH + i, slice(TOP, TOP + Y))
            g0[here] = g0[here] + jnp.where(first | last, turn(ghosts, -2 * i - 1), 0.0)

    def start_edges(k):
        start_all([main_copies(k)[i] for i, (dx, _) in enumerate(AROUND) if dx])

    complete(0, DEPTH)
    complete(X - DEPTH, X)
    start_edges(0)
    complete(DEPTH, X - DEPTH)

    def sums_of(a, b, width):
        lane = iota((1, LANES), 1)
        pair = jnp.concatenate([jnp.sum(a, axis=0, keepdims=True), jnp.sum(b, axis=0, keepdims=True)], axis=0)
        size = LANES // 2
        while size >= width:
            pair = pair + turn(pair, size)
            size //= 2
        return jnp.where(lane < LANES - width, pair[0:1], pair[1:2])

    def ratio(rows, width):
        lane = iota((1, LANES), 1)
        row = jnp.sum(rows, axis=0, keepdims=True)
        second = jnp.where(lane >= LANES - width, row, 0.0)
        first = jnp.where((lane >= LANES - 2 * width) & (lane < LANES - width), row, 0.0)
        return jnp.sum(first, axis=1, keepdims=True) / jnp.sum(second, axis=1, keepdims=True)

    nothing = jnp.zeros((Y, LANES), jnp.float32)
    precondition(0, z0, None)
    rz, zw = nothing, nothing
    inner = list(range(DEPTH, X - DEPTH))
    for i in [i for i in range(X) if i not in inner] + inner:
        if i == DEPTH:
            start_edges(1)
        mid, image = operator(z0, DEPTH + i)
        g0[1, DEPTH + i, TOP:TOP + Y, :] = image
        rz = rz + g0[0, DEPTH + i, TOP:TOP + Y, :] * mid
        zw = zw + mid * image
    precondition(1, z1, sums_of(rz, zw, LANES // 4))
    alpha = ratio(cr[1, :, 0, :], LANES // 4)
    rz, zw = nothing, nothing
    for i in range(X):
        mid, image = operator(z1, DEPTH + i)
        here = (DEPTH + i, slice(TOP, TOP + Y))
        before, w = z0[here], g0[(1,) + here]
        r = g0[(0,) + here] - alpha * w
        z = before - alpha * mid
        w = w - alpha * image
        rz = rz + r * z
        zw = zw + z * w
        w_ref[i] = w
    sums = sums_of(rz, zw, LANES // 2)
    ds[...] = sums
    dr[me] = sums
    to_all(ds, dr, dsend.at[0], drecv.at[0])
    for i in range(X):
        here = (DEPTH + i, slice(TOP, TOP + Y))
        before = z0[here]
        sol_ref[i] = ux[1 + i, TOP:TOP + Y, :] + alpha * before
        z_ref[i] = before - alpha * z1[here]
        res_ref[i] = g0[(0,) + here] - alpha * g0[(1,) + here]
    all_of(face_entries(), xsend.at[0], 1)
    all_of([(step, STEPS * c) for step, c in main_entries() + far_entries()], send.at[0], 1)
    part = cr.at[:, pl.ds(0, n - 1)]
    pltpu.make_async_copy(part, part, csend.at[0]).wait()
    all_done(dr, dsend.at[0])
    all_done(dr, drecv.at[0])
    alpha_ref[...] = jnp.broadcast_to(ratio(dr[:, 0, :], LANES // 2), alpha_ref.shape)


def finish(base, z, r, w, alpha, sol, res, sol_out, res_out, sem):
    X = base.shape[0]
    size = X // PARTS
    a = alpha[0:1, 0:1][None]
    copies = []
    for part in range(PARTS):
        here = slice(part * size, (part + 1) * size)
        sol_out[here] = base[here] + a * z[here]
        res_out[here] = r[here] - a * w[here]
        for i, (src, dst) in enumerate(((sol_out, sol), (res_out, res))):
            copies.append(pltpu.make_async_copy(src.at[here], dst.at[here], sem.at[i, part]))
            copies[-1].start()
    for copy in copies:
        copy.wait()


def solution(mesh):
    sizes = tuple(mesh.shape[a] for a in AXES)
    n = sizes[0] * sizes[1] * sizes[2]

    def run(right_side, guess):
        X, Y, Z = block = guess.shape
        assert Z == LANES and PER == DEPTH and X % PER == 0 and X * DEPTH <= LANES
        dims = [tuple(d >> l for d in block) for l in range(LEVELS)]
        f32 = jnp.float32
        vm = lambda *s: pltpu.VMEM(s, f32)
        ext = [(dims[l][0] + 2 * DEPTH, dims[l][1] + 2 * TOP, LANES) for l in range(HALOED)]
        slab = (X // PER + 2, Y + 2 * TOP, LANES)
        tall = [(dims[l][1] + 2 * DEPTH, LANES) for l in range(HALOED)]
        CA, CB, CC = dims[HALOED]
        assert dims[HALOED + 1][:2] == (1, 1) and sizes[1] * CB <= ROWS and CA * CB * CC + CC // 2 <= LANES // 2
        dma = lambda *s: pltpu.SemaphoreType.DMA(s)
        scratch = [
            vm(X + 2, Y + 2 * TOP, LANES), vm(*block),
            *(vm(STEPS, *e) for e in ext), vm(STEPS, *slab),
            *(vm(*e) for e in ext[1:]), vm(*slab),
            *(vm(*e) for e in ext + [slab] for _ in range(SWEEPS - 1)),
            vm(*ext[0]), vm(*ext[0]),
            vm(slab[0], *tall[0]), vm(slab[0], *tall[0]),
            vm(dims[1][0] + 2, 2 * tall[1][0], LANES), vm(dims[1][0] + 2, 2 * tall[1][0], LANES),
            *(vm(*t) for t in tall), vm(*tall[0]),
            vm((CA + 1) * sizes[0] * ROWS, (CA * CB + 1) * n),
            vm(CA * sizes[0] + DEPTH, ROWS, LANES),
            vm(CA + DEPTH, 4 * ROWS, LANES),
            vm(X // 2, Y, LANES), vm(X // 2, 2 * Y, LANES),
            vm(2, Y, LANES), vm(2, X, 1, LANES), vm(Y, LANES), vm(2, Y, LANES),
            vm(STEPS, 2, Y, LANES), vm(STEPS, dims[1][1], LANES), vm(STEPS, dims[2][1], LANES),
            *(vm(STEPS, 2, dims[l][1] + 2 * DEPTH, LANES) for l in range(HALOED - 1)),
            vm(STEPS, 2, Y, LANES), vm(STEPS, 2, 2, Y + 2 * DEPTH, LANES),
            vm(STEPS, 2, DEPTH, dims[1][1], LANES), vm(STEPS, 2, DEPTH, dims[1][1] + 2 * DEPTH, LANES),
            vm(STEPS, 1, LANES), vm(STEPS, n, 1, LANES),
            vm(1, LANES), vm(n, 1, LANES), vm(16 * STEPS * DEPTH * max(X, Y), LANES),
            dma(2), dma(1), dma(1), dma(STEPS), dma(1), dma(STEPS),
            dma(1), dma(STEPS), dma(1), dma(1),
        ]
        whole = pltpu.VMEM(block, f32)
        base, z, r, w, alpha = pl.pallas_call(
            functools.partial(kernel, sizes, block),
            out_shape=(whole, whole, whole, whole, pltpu.VMEM((8, LANES), f32)),
            in_specs=[pl.BlockSpec(memory_space=pl.ANY)] * 2,
            out_specs=[pl.BlockSpec(memory_space=pltpu.VMEM)] * 5,
            scratch_shapes=scratch,
            compiler_params=pltpu.CompilerParams(collective_id=0, has_side_effects=True),
        )(right_side, guess)
        inner = [pltpu.with_memory_space_constraint(v, pltpu.VMEM) for v in (base, z, r, w, alpha)]
        out = jax.ShapeDtypeStruct(block, f32)
        return tuple(pl.pallas_call(
            finish,
            out_shape=(out, out),
            in_specs=[pl.BlockSpec(memory_space=pltpu.VMEM)] * 5,
            out_specs=[pl.BlockSpec(memory_space=pl.ANY)] * 2,
            scratch_shapes=[vm(*block), vm(*block), dma(2, PARTS)],
        )(*inner))

    spec = P(*AXES)
    return jax.shard_map(run, mesh=mesh, in_specs=(spec, spec), out_specs=(spec, spec), check_vma=False)
```

```python
import functools

import jax
import jax.numpy as jnp
from jax import lax
from jax.experimental import pallas as pl
from jax.experimental.pallas import tpu as pltpu
from jax.sharding import PartitionSpec as P

LEVELS = 6
SWEEPS = 4
STEPS = 2
HALOED = 4
AXES = ("gx", "gy", "gz")
LANES = 128
TOP = 8
DEPTH = SWEEPS
SPAN = 8 * DEPTH
PER = LANES // SPAN
PARTS = 4
MESH = pl.DeviceIdType.MESH
HIGH = lax.Precision.HIGHEST
ROWS = 8
ALL = [(a, b, c) for a in (-1, 1, 0) for c in (0, -1, 1) for b in (0, -1, 1) if (a, b, c) != (0, 0, 0)]
AROUND = [(a, b) for a in (-1, 0, 1) for b in (-1, 0, 1) if (a, b) != (0, 0)]
FACES = [(d, s) for d in range(3) for s in (-1, 1)]


def iota(shape, dim):
    return lax.broadcasted_iota(jnp.int32, shape, dim)


def take(x, index):
    if x.ndim == 3:
        return jnp.stack([take(x[i], index) for i in range(x.shape[0])])
    rows = x.shape[0]
    more = -rows % 8
    if rows == 1:
        x = jnp.broadcast_to(x, (8, LANES))
    elif more:
        x = jnp.concatenate([x, jnp.zeros((more, LANES), x.dtype)], axis=0)
    index = jnp.broadcast_to(index[:1], x.shape)
    out = jnp.take_along_axis(x, index, axis=1, mode="promise_in_bounds")
    return out[:rows] if more else out


def wrapped(lane):
    return jnp.where(lane >= LANES - DEPTH, lane - LANES, lane)


def halve(x, width):
    lane = iota((8, LANES), 1)
    return take(x + turn(x, -1), 2 * (lane % width)) * 0.125


def turn(x, shift):
    shift = shift % LANES
    return pltpu.roll(x, shift, x.ndim - 1) if shift else x


def kernel(sizes, block, b_hbm, x_hbm, sol_ref, z_ref, res_ref, w_ref, alpha_ref, *rest):
    (ux, bb, g0, g1, g2, g3, gs, h1, h2, h3, hs, f0a, f0b, f0c, f1a, f1b, f1c, f2a, f2b, f2c, f3a, f3b, f3c, fsa, fsb, fsc,
     z0, z1, sc, sd, pd, pe, m0, m1, m2, m3, ms, pmat, wref, wide, fold, spread, xg, yg, ze, zi, zq0, zq1, zq2, zr0, zr1, zr2, es, zx, xs, xf, cs, cr, ds, dr, blank,
     isem, xsend, xrecv, frecv, send, mrecv, csend, crecv, dsend, drecv) = rest
    nx, ny, nz = sizes
    n = nx * ny * nz
    at = tuple(lax.axis_index(a) for a in AXES)
    me = (at[0] * ny + at[1]) * nz + at[2]
    dims = [tuple(d >> l for d in block) for l in range(LEVELS)]
    X, Y, Z = block
    fields = (g0, g1, g2, g3)
    after = ((f0a, f0b, f0c), (f1a, f1b, f1c), (f2a, f2b, f2c), (f3a, f3b, f3c), (fsa, fsb, fsc))
    masks = (m0, m1, m2, m3)
    whole = (None, h1, h2, h3, hs)
    groups = X // PER
    lower = [at[d] > 0 for d in range(3)]
    upper = [at[d] < sizes[d] - 1 for d in range(3)]
    inlow = [jnp.where(c, 1.0, 0.0) for c in lower]
    inup = [jnp.where(c, 1.0, 0.0) for c in upper]

    load_x = pltpu.make_async_copy(x_hbm, ux.at[1:X + 1, TOP:TOP + Y], isem.at[0])
    load_b = pltpu.make_async_copy(b_hbm, bb, isem.at[1])
    load_x.start()
    load_b.start()

    def others():
        out = []
        for b in range(ny - 1, -1, -1):
            for c in range(nz - 1, -1, -1):
                for a in range(nx):
                    if b or c:
                        first = jnp.where(at[0] < nx // 2, nx - 1 - a, a)
                    elif a:
                        first = lax.rem(at[0] + a, nx)
                    else:
                        continue
                    out.append((first, lax.rem(at[1] + b, ny), lax.rem(at[2] + c, nz)))
        return out

    barrier = pltpu.get_barrier_semaphore()
    for target in others():
        pl.semaphore_signal(barrier, inc=1, device_id=target, device_id_type=MESH)

    def outside(dim, side):
        for l in range(HALOED + 1):
            A, B = (groups if l == HALOED else dims[l][0]), (Y if l == HALOED else dims[l][1])
            d, ref = (1, gs) if l == HALOED else (DEPTH, fields[l])
            for k in range(STEPS):
                if dim == 0:
                    a = A + d if side else 0
                    ref[k, a:a + d, TOP - DEPTH:TOP + B + DEPTH, :] = jnp.zeros((d, B + 2 * DEPTH, LANES), jnp.float32)
                else:
                    a = TOP + B if side else TOP - DEPTH
                    ref[k, :, a:a + DEPTH, :] = jnp.zeros((A + 2 * d, DEPTH, LANES), jnp.float32)

    far = (zr0, zr1, zr2, zx, xf)

    def nothing_in(ref):
        ref[...] = jnp.zeros(ref.shape, jnp.float32)

    for side in (0, 1):
        for dim in range(2):
            @pl.when(jnp.logical_not((upper if side else lower)[dim]))
            def _(dim=dim, side=side):
                outside(dim, side)
                nothing_in((xg, yg)[dim].at[1 - side])
                for ref in far if dim else ():
                    head = (slice(None),) * (len(ref.shape) - 2)
                    a = ref.shape[-2] - DEPTH if side else 0
                    nothing_in(ref.at[head + (slice(a, a + DEPTH),)])
                if dim == 0:
                    nothing_in(zx.at[:, :, side])
                    nothing_in(xf.at[:, side])
        @pl.when(jnp.logical_not((upper if side else lower)[2]))
        def _(side=side):
            nothing_in(zi.at[side])
            for ref in far[:4]:
                nothing_in(ref.at[:, 1 - side])

    ux[:, TOP - 1:TOP, :] = jnp.zeros((X + 2, 1, LANES), jnp.float32)
    ux[:, TOP + Y:TOP + Y + 1, :] = jnp.zeros((X + 2, 1, LANES), jnp.float32)
    ux[0, TOP:TOP + Y, :] = jnp.zeros((Y, LANES), jnp.float32)
    ux[X + 1, TOP:TOP + Y, :] = jnp.zeros((Y, LANES), jnp.float32)
    wref[...] = jnp.zeros_like(wref)
    wide[...] = jnp.zeros_like(wide)

    def mask(rows, z, depth_z):
        y = iota((rows + 2 * DEPTH, LANES), 0) - DEPTH
        part = jnp.where(y < 0, inlow[1], jnp.where(y >= rows, inup[1], 1.0))
        return part * jnp.where(z < 0, inlow[2], jnp.where(z >= depth_z, inup[2], 1.0)) * (1.0 / 9.0)

    for l in range(HALOED):
        lane = iota((dims[l][1] + 2 * DEPTH, LANES), 1)
        masks[l][...] = mask(dims[l][1], lane if l == 0 else wrapped(lane), dims[l][2])
    CA, CB, CC = dims[HALOED]
    CD = dims[HALOED + 1][2]
    cells = CA * CB
    row, column = iota(pmat.shape, 0), iota(pmat.shape, 1)
    cell, device = column // n, column % n
    plane, line = row // ROWS, row % ROWS
    dx, dy = device // (ny * nz), device // nz % ny
    fits = (cell < cells) & (plane == dx * CA + cell // CB) & (line == dy * CB + cell % CB)
    fits = fits | ((cell == cells) & (plane == nx * CA + dx) & (line == dy))
    pmat[...] = jnp.where(fits, 1.0, 0.0)
    lane = iota((Y + 2 * DEPTH, LANES), 1) % SPAN
    ms[...] = mask(Y, jnp.where(lane < SPAN // 2, lane + Z - SPAN // 4, lane - 3 * SPAN // 4), Z)

    def face_copies():
        out = []
        for i, (d, s) in enumerate(FACES):
            target = list(at)
            target[d] = at[d] + s
            into = 1 if s > 0 else 0
            if d == 0:
                src, dst = ux.at[X if s > 0 else 1, TOP:TOP + Y], xg.at[into]
            elif d == 1:
                a = TOP + Y - 1 if s > 0 else TOP
                src, dst = ux.at[1:X + 1, a:a + 1], yg.at[into]
            else:
                src, dst = ze, zi.at[0 if s > 0 else 1]
            copy = pltpu.make_async_remote_copy(
                src_ref=src, dst_ref=dst, send_sem=xsend.at[0], recv_sem=xrecv.at[0],
                device_id=tuple(target), device_id_type=MESH,
            )
            out.append((copy, upper[d] if s > 0 else lower[d], lower[d] if s > 0 else upper[d]))
        return out

    def span(step, depth, start, own, other):
        if step > 0:
            return (start + own - depth, depth), (start - depth, depth)
        if step < 0:
            return (start, depth), (start + own, depth)
        return (start, own), (start, own)

    def around_copies(ref, k, depth, planes, rows, rsem):
        out = []
        for i, (dx, dy) in enumerate(AROUND):
            (sx, lx), (tx, _) = span(dx, depth, depth, planes, None)
            (sy, ly), (ty, _) = span(dy, DEPTH, TOP, rows, None)
            copy = pltpu.make_async_remote_copy(
                src_ref=ref.at[k, sx:sx + lx, sy:sy + ly], dst_ref=ref.at[k, tx:tx + lx, ty:ty + ly],
                send_sem=send.at[0], recv_sem=rsem.at[k],
                device_id=(at[0] + dx, at[1] + dy, at[2]), device_id_type=MESH,
            )
            to, fro = None, None
            for d, s in ((0, dx), (1, dy)):
                if s:
                    a, b = (upper[d], lower[d]) if s > 0 else (lower[d], upper[d])
                    to = a if to is None else jnp.logical_and(to, a)
                    fro = b if fro is None else jnp.logical_and(fro, b)
            out.append((copy, to, fro, lx * ly))
        return out

    def main_copies(k):
        return around_copies(g0, k, DEPTH, X, Y, mrecv)

    def rows_of(dy, rows):
        if dy > 0:
            return pl.ds(rows - DEPTH, DEPTH), pl.ds(0, DEPTH), DEPTH
        if dy < 0:
            return pl.ds(0, DEPTH), pl.ds(rows + DEPTH, DEPTH), DEPTH
        return pl.ds(0, rows), pl.ds(DEPTH, rows), rows

    def every(conds):
        out = None
        for cond in conds:
            out = cond if out is None else jnp.logical_and(out, cond)
        return out

    def far_copies(k):
        out = []
        for i, (dx, dy, dz) in enumerate(ALL):
            step = (dx, dy, dz)
            to = every([(upper if t > 0 else lower)[d] for d, t in enumerate(step) if t])
            fro = every([(lower if t > 0 else upper)[d] for d, t in enumerate(step) if t])
            from_x, into_x = (1, 0) if dx > 0 else (0, 1)
            side = 1 if dz > 0 else 0
            pairs = []
            if dz and dx:
                a, b, c = rows_of(dy, Y)
                pairs.append((es.at[k, from_x, a], zx.at[k, side, into_x, b], c))
            elif dz:
                for src, dst in ((zq0.at[k, side], zr0), (zq1.at[k], zr1), (zq2.at[k], zr2)):
                    a, b, c = rows_of(dy, src.shape[0])
                    pairs.append((src.at[a], dst.at[k, side, b], c))
            else:
                arrays = []
                if dx:
                    a, b, c = rows_of(dy, dims[1][1])
                    pairs.append((xs.at[k, from_x, :, a], xf.at[k, into_x, :, b], DEPTH * c))
                else:
                    arrays = [(gs, 1, groups, Y)]
                    arrays += [(fields[l], DEPTH, dims[l][0], dims[l][1]) for l in range(1, HALOED)]
                for ref, depth, planes, rows in arrays:
                    (sx, lx), (tx, _) = span(dx, depth, depth, planes, None)
                    (sy, ly), (ty, _) = span(dy, DEPTH, TOP, rows, None)
                    pairs.append((ref.at[k, sx:sx + lx, sy:sy + ly], ref.at[k, tx:tx + lx, ty:ty + ly], lx * ly))
            copies = [pltpu.make_async_remote_copy(
                src_ref=src, dst_ref=dst, send_sem=send.at[0], recv_sem=frecv.at[k],
                device_id=(at[0] + dx, at[1] + dy, at[2] + dz), device_id_type=MESH,
            ) for src, dst, _ in pairs]
            out.append((copies, to, fro, sum(c for _, _, c in pairs)))
        return out

    def bytes_done(count, sem):
        assert count <= blank.shape[0]
        part = blank.at[pl.ds(0, count)]
        pltpu.make_async_copy(part, part, sem).wait()

    def all_of(entries, sem, sign):
        def nest(d, have):
            if d == len(sizes):
                total = sum(c for step, c in entries if all(t == 0 or sign * t in have[i] for i, t in enumerate(step)))
                if total:
                    bytes_done(total, sem)
            elif sizes[d] == 1 or not any(step[d] for step, _ in entries):
                nest(d + 1, have + [()])
            else:
                pl.when(jnp.logical_not(lower[d]))(lambda: nest(d + 1, have + [(1,)]))
                pl.when(jnp.logical_not(upper[d]))(lambda: nest(d + 1, have + [(-1,)]))
                if sizes[d] > 2:
                    pl.when(jnp.logical_and(lower[d], upper[d]))(lambda: nest(d + 1, have + [(-1, 1)]))

        nest(0, [])

    def main_entries():
        return [((dx, dy, 0), entry[3]) for (dx, dy), entry in zip(AROUND, main_copies(0))]

    def far_entries():
        return [(step, entry[3]) for step, entry in zip(ALL, far_copies(0))]

    def face_entries():
        return [(tuple(s if i == d else 0 for i in range(3)), X if d == 1 else Y) for d, s in FACES]

    def start_all(copies):
        for copy, cond, *_ in copies:
            pl.when(cond)(copy.start)

    def start_far(k):
        for copies, to, _, _ in far_copies(k):
            @pl.when(to)
            def _(copies=copies):
                for copy in copies:
                    copy.start()

    def to_all(src, dst, s_sem, r_sem):
        for target in others():
            pltpu.make_async_remote_copy(
                src_ref=src, dst_ref=dst.at[me], send_sem=s_sem, recv_sem=r_sem,
                device_id=target, device_id_type=MESH,
            ).start()

    def all_done(dst, sem):
        part = dst.at[pl.ds(0, n - 1)]
        pltpu.make_async_copy(part, part, sem).wait()

    def fold_xy(field):
        A, B, _ = field.shape
        pairs = field.reshape(A // 2, 2, B, LANES)
        fold[0:A // 2, 0:B, :] = pairs[:, 0] + pairs[:, 1]
        return fold[0:A // 2, pl.ds(0, B // 2, 2), :] + fold[0:A // 2, pl.ds(1, B // 2, 2), :]

    def spread_y(field, into, first=0):
        A, B, _ = field.shape
        into[0:A, pl.ds(first, B, 2), :] = field
        into[0:A, pl.ds(first + 1, B, 2), :] = field

    def twice(field):
        A, B, _ = field.shape
        return jnp.broadcast_to(field[:, None], (A, 2, B, LANES)).reshape(2 * A, B, LANES)

    def own(ref, l, k=None):
        A, B, _ = dims[l]
        return ref[(k,) * (k is not None) + (slice(DEPTH, DEPTH + A), slice(TOP, TOP + B))]

    def update(src, rhs, dst, a, c, low, rows, scale):
        at_rows = slice(low, low + rows)
        mid = src[a:a + c, at_rows, :]
        total = src[a - 1:a - 1 + c, at_rows, :] + src[a + 1:a + 1 + c, at_rows, :]
        total = total + src[a:a + c, low - 1:low - 1 + rows, :] + src[a:a + c, low + 1:low + 1 + rows, :]
        total = total + turn(mid, 1) + turn(mid, -1)
        dst[a:a + c, at_rows, :] = rhs[a:a + c, at_rows, :] + (3.0 * mid + total) * scale

    def pieces(a, b):
        return [(p, min(4, b - p)) for p in range(a, b, 4)]

    def sweep(l, src, rhs, dst, k):
        A, B, _ = dims[l]
        low, rows = TOP - DEPTH, B + 2 * DEPTH
        m = masks[l][...]
        update(src, rhs, dst, k, DEPTH - k, low, rows, m * inlow[0])
        for a, c in pieces(DEPTH, DEPTH + A):
            update(src, rhs, dst, a, c, low, rows, m)
        update(src, rhs, dst, DEPTH + A, DEPTH - k, low, rows, m * inup[0])

    def sweep_inside(src, rhs, dst, k):
        for a, c in pieces(DEPTH + k, DEPTH + X - k):
            update(src, rhs, dst, a, c, TOP + k, Y - 2 * k, 1.0 / 9.0)

    def sweep_rim(src, rhs, dst, k):
        low, rows = TOP - DEPTH, Y + 2 * DEPTH
        m = m0[...]
        update(src, rhs, dst, k, DEPTH - k, low, rows, m * inlow[0])
        update(src, rhs, dst, DEPTH, k, low, rows, m)
        update(src, rhs, dst, DEPTH + X - k, k, low, rows, m)
        update(src, rhs, dst, DEPTH + X, DEPTH - k, low, rows, m * inup[0])
        for start in (0, Y):
            edge = m0[start:start + 2 * DEPTH, :]
            for a, c in pieces(DEPTH + k, DEPTH + X - k):
                update(src, rhs, dst, a, c, low + start, 2 * DEPTH, edge)

    def sweep_slab(src, rhs, dst):
        low, rows = TOP - DEPTH, Y + 2 * DEPTH
        lane = iota((rows, LANES), 1)
        m = ms[...]
        for g in range(groups + 2):
            mid = src[g, low:low + rows, :]
            total = src[g, low - 1:low - 1 + rows, :] + src[g, low + 1:low + 1 + rows, :]
            total = total + turn(mid, 1) + turn(mid, -1)
            before = mid if g == 0 else jnp.where(lane >= LANES - SPAN, src[g - 1, low:low + rows, :], mid)
            behind = mid if g == groups + 1 else jnp.where(lane < SPAN, src[g + 1, low:low + rows, :], mid)
            total = total + turn(before, SPAN) + turn(behind, -SPAN)
            scale = m * inlow[0] if g == 0 else m * inup[0] if g == groups + 1 else m
            dst[g, low:low + rows, :] = rhs[g, low:low + rows, :] + (3.0 * mid + total) * scale

    def smooth_whole(rhs, depth_y, depth_z, l):
        A, B, _ = rhs.shape
        lane, row = iota(rhs.shape, 2), iota(rhs.shape, 1)
        e = rhs
        for _ in range(SWEEPS - 1):
            px, py = jnp.zeros((1, B, LANES), jnp.float32), jnp.zeros((A, 1, LANES), jnp.float32)
            total = jnp.concatenate([px, e[:-1]], axis=0) + jnp.concatenate([e[1:], px], axis=0)
            total = total + jnp.concatenate([py, e[:, :-1]], axis=1) + jnp.concatenate([e[:, 1:], py], axis=1)
            total = total + jnp.where(lane == 0, 0.0, turn(e, 1))
            total = total + jnp.where(lane == depth_z - 1, 0.0, turn(e, -1))
            e = rhs + jnp.where(row < depth_y, (3.0 * e + total) * (1.0 / 9.0), 0.0)
        return e * (4.0 ** l / 9.0)

    half, quarter = SPAN // 2, SPAN // 4

    def pack_slab(k):
        lane = iota((Y, LANES), 1)
        line, spot = lane // SPAN, lane % SPAN
        low = high = jnp.zeros((Y, LANES), jnp.float32)
        for g in range(groups):
            both = jnp.zeros((Y, LANES), jnp.float32)
            for i in range(PER):
                field = g0[k, DEPTH + g * PER + i, TOP:TOP + Y, :]
                both = jnp.where((line == i) & (spot < half), turn(field, SPAN * i + quarter), both)
            gs[k, g + 1, TOP:TOP + Y, :] = jnp.where(
                spot < quarter, both, jnp.where(spot >= 3 * quarter, turn(both, half), 0.0))
            here = spot // DEPTH == g
            low = jnp.where(here, turn(both, DEPTH * g - quarter), low)
            high = jnp.where(here, turn(both, DEPTH * g - quarter + DEPTH), high)
        zq0[k, 0] = low
        zq0[k, 1] = high
        for side, j in ((0, 0), (1, groups - 1)):
            es[k, side] = put(0, low, j, 0) + put(0, high, j, 1)

    def pack_ends(k):
        low, rows = TOP - DEPTH, Y + 2 * DEPTH
        lane = iota((rows, LANES), 1)
        line, spot = lane // SPAN, lane % SPAN
        for g, p in ((0, 0), (groups + 1, DEPTH + X)):
            both = jnp.zeros((rows, LANES), jnp.float32)
            for i in range(PER):
                field = g0[k, p + i, low:low + rows, :]
                both = jnp.where((line == i) & (spot < half), turn(field, SPAN * i + quarter), both)
            gs[k, g, low:low + rows, :] = jnp.where(
                spot < quarter, both, jnp.where(spot >= 3 * quarter, turn(both, half), 0.0))

    def slots(l):
        return (0, 0, 0, dims[2][0] // DEPTH * 2)[l], dims[l][0] // DEPTH

    def put(l, x, source, target):
        lane = iota(x.shape, 1)
        return jnp.where(lane % SPAN // DEPTH == target, turn(x, DEPTH * (target - source)), 0.0)

    def pack_level(k, l):
        A, B, C = dims[l]
        base, many = slots(l)
        lane = iota((B, LANES), 1)
        line, slot = lane // SPAN, lane % SPAN // DEPTH
        out = jnp.zeros((B, LANES), jnp.float32)
        for i in range(A):
            field = fields[l][k, DEPTH + i, TOP:TOP + B, :]
            x, j = i % DEPTH, i // DEPTH
            lo, hi = base + j, base + many + j
            out = jnp.where((line == x) & (slot == lo), turn(field, SPAN * x + DEPTH * lo), out)
            out = jnp.where((line == x) & (slot == hi), turn(field, SPAN * x + DEPTH * hi - C + DEPTH), out)
        return out

    def pack_rest(k):
        one, two, three = [pack_level(k, l) for l in range(1, HALOED)]
        zq1[k] = one
        B1, B2, B3 = [dims[l][1] for l in range(1, HALOED)]
        zq2[k, 0:B2] = two
        for a in (0, B2 - B3):
            zq2[k, a:a + B3] = zq2[k, a:a + B3] + three
        for side in (0, 1):
            def edge(l, x):
                base, many = slots(l)
                j = many - 1 if side else 0
                return put(l, x, base + j, 2 * l) + put(l, x, base + many + j, 2 * l + 1)
            first, second, third = edge(1, one), edge(2, two), edge(3, three)
            for src, dst, size, part in (
                    (0, 0, B1 - DEPTH, first), (B1 - DEPTH, Y - DEPTH, DEPTH, first),
                    (0, 0, DEPTH, second), (B2 - DEPTH, Y - DEPTH, DEPTH, second),
                    (0, 0, DEPTH, third), (0, Y - DEPTH, DEPTH, third)):
                es[k, side, dst:dst + size] = es[k, side, dst:dst + size] + part[src:src + size]
            for x in range(DEPTH):
                p1, p2, p3 = [DEPTH + x + (dims[l][0] - DEPTH if side else 0) for l in range(1, HALOED)]
                xs[k, side, x] = g1[k, p1, TOP:TOP + B1, :]
                second = turn(g2[k, p2, TOP:TOP + B2, :], dims[1][2])
                third = turn(g3[k, p3, TOP:TOP + B3, :], dims[1][2] + dims[2][2])
                xs[k, side, x, 0:DEPTH] = xs[k, side, x, 0:DEPTH] + second[0:DEPTH] + third
                xs[k, side, x, B1 - DEPTH:B1] = xs[k, side, x, B1 - DEPTH:B1] + second[B2 - DEPTH:B2] + third

    def unpack_slab(k):
        low, rows = TOP - DEPTH, Y + 2 * DEPTH
        spot = iota((rows, LANES), 1) % SPAN
        for g in range(groups + 2):
            edge = 0 if g == 0 else 1 if g == groups + 1 else None
            if edge is None:
                above, below, up, down = zr0[k, 0], zr0[k, 1], g - 1, g - 1
            else:
                above, below, up, down = zx[k, 0, edge], zx[k, 1, edge], 0, 1
            held = gs[k, g, low:low + rows, :]
            held = jnp.where(spot // DEPTH == 2, turn(above, DEPTH * (2 - up)), held)
            hs[g, low:low + rows, :] = jnp.where(spot // DEPTH == 5, turn(below, DEPTH * (5 - down)), held)

    def unpack_level(k, l):
        A, B, C = dims[l]
        low, rows = TOP - DEPTH, B + 2 * DEPTH
        base, many = slots(l)
        lane = iota((rows, LANES), 1)

        def cut(ref, head):
            end = ref.shape[-2]
            tail = 0 if end == rows else (2 * DEPTH if B > DEPTH else DEPTH)
            a = ref[head + (slice(0, rows - tail),)]
            return jnp.concatenate([a, ref[head + (slice(end - tail, end),)]], axis=0) if tail else a

        ref = (None, zr1, zr2, zr2)[l]
        sides = [cut(ref, (k, 0)), cut(ref, (k, 1))]
        edges = [[cut(zx, (k, side, e)) for side in (0, 1)] for e in (0, 1)]
        start = sum(dims[i][2] for i in range(1, l))
        for p in range(A + 2 * DEPTH):
            edge = 0 if p < DEPTH else 1 if p >= DEPTH + A else None
            x, j = p % DEPTH, p // DEPTH - 1
            if edge is None:
                held = fields[l][k, p, low:low + rows, :]
                (above, below), up, down = sides, base + j, base + many + j
            else:
                held = jnp.where(lane < C, turn(cut(xf, (k, edge, x)), -start), 0.0)
                (above, below), up, down = edges[edge], 2 * l, 2 * l + 1
            held = jnp.where(lane // DEPTH == C // DEPTH, turn(above, C - SPAN * x - DEPTH * up), held)
            whole[l][p, low:low + rows, :] = jnp.where(
                lane >= LANES - DEPTH, turn(below, -DEPTH - SPAN * x - DEPTH * down), held)

    half_row = LANES // 2
    def own_row(k):
        lane = iota((1, LANES), 1)
        out, total = jnp.zeros((1, LANES), jnp.float32), None
        for i in range(CA):
            for j in range(CB):
                part = None
                for a in (0, 1):
                    for b in (0, 1):
                        y = TOP + 2 * j + b
                        one = fields[HALOED - 1][k, DEPTH + 2 * i + a, y:y + 1, :]
                        part = one if part is None else part + one
                part = halve(part, CC)
                out = jnp.where(lane // CC == i * CB + j, part, out)
                total = part if total is None else total + part
        return jnp.where((lane >= cells * CC) & (lane < cells * CC + CD), halve(total, CD), out)

    def coarse(k):
        rows = cr[k, :, 0, :]
        lane, row = iota((n, LANES), 1), iota((n, LANES), 0)
        parts = [jnp.where(lane // CC == row % nz, take(rows, cell * CC + lane % CC), 0.0) for cell in range(cells)]
        parts.append(jnp.where(lane // CD == row % nz, take(rows, cells * CC + lane % CD), 0.0))
        out = jnp.dot(pmat[...], jnp.concatenate(parts, axis=0), precision=HIGH, preferred_element_type=jnp.float32)
        out = out.reshape(-1, ROWS, LANES)
        last = smooth_whole(out[nx * CA:], ny, nz * CD, HALOED + 1)
        spread_y(last, spread)
        grown = take(spread[0:nx, 0:ROWS, :], iota((8, LANES), 1) // 2)
        wref[DEPTH // 2:DEPTH // 2 + nx * CA, :, :] = (
            twice(grown) + smooth_whole(out[:nx * CA], ny * CB, nz * CC, HALOED))

    def precondition(k, z, extra):
        start_all([main_copies(k)[i] for i, (dx, _) in enumerate(AROUND) if not dx])
        lane = iota((8, LANES), 1)
        sums = own(g0, 0, k)
        for l in range(1, HALOED):
            A, B, C = dims[l]
            sums = fold_xy(sums)
            sums = sums + turn(sums, -(1 << (l - 1)))
            coarser = jnp.where(lane[0:1][None] < C, take(sums, (1 << l) * (lane % C)) * 0.125 ** l, 0.0)
            fields[l][k, DEPTH:DEPTH + A, TOP:TOP + B, :] = coarser
        pack_slab(k)
        pack_rest(k)
        mine = own_row(k) if extra is None else jnp.where(iota((1, LANES), 1) < half_row, own_row(k), extra)
        cs[k] = mine
        cr[k, me] = mine
        start_far(k)
        to_all(cs.at[k], cr.at[k], csend.at[0], crecv.at[k])
        for s in range(1, SWEEPS):
            sweep_inside(after[0][s - 2] if s > 1 else g0.at[k], g0.at[k], after[0][s - 1], s)
        all_of(main_entries(), mrecv.at[k], -1)
        pack_ends(k)
        for s in range(1, SWEEPS):
            sweep_rim(after[0][s - 2] if s > 1 else g0.at[k], g0.at[k], after[0][s - 1], s)
        all_of(far_entries(), frecv.at[k], -1)
        unpack_slab(k)
        for l in range(1, HALOED):
            unpack_level(k, l)
        for s in range(1, SWEEPS):
            sweep_slab(after[HALOED][s - 2] if s > 1 else hs, hs, after[HALOED][s - 1])
            for l in range(1, HALOED):
                sweep(l, after[l][s - 2] if s > 1 else whole[l], whole[l], after[l][s - 1], s)
        all_done(cr.at[k], crecv.at[k])
        coarse(k)
        A, B, C = dims[HALOED - 1]
        spread_y(wref[pl.ds(at[0] * CA, CA + DEPTH)], wide, DEPTH)
        part = wide[:, 0:2 * ROWS, :]
        for j in range(1, ny):
            part = jnp.where(at[1] == j, wide[:, j * B:j * B + 2 * ROWS, :], part)
        source = (wrapped(lane) >> 1) + at[2] * CC
        inside = (source >= 0) & (source < CC * nz)
        part = take(part, jnp.where(inside, source, 0))
        part = jnp.where(inside[0:1][None], part, 0.0)
        part = twice(part)[DEPTH - 1:DEPTH + A + 1, 0:B + 2 * DEPTH]
        for l in range(HALOED - 1, 0, -1):
            A, B, C = dims[l]
            end = after[l][SWEEPS - 2][DEPTH - 1:DEPTH + A + 1, TOP - DEPTH:TOP + B + DEPTH, :]
            full = end * (4.0 ** l / 9.0) + part
            if l > 1:
                spread_y(take(full, (wrapped(lane) >> 1) & (LANES - 1)), spread)
                part = twice(spread[0:A + 2, DEPTH:DEPTH + 2 * B + 2 * DEPTH, :])[1:2 * A + 3]
            else:
                spread_y(take(full, lane // 2), pd)
                spread_y(take(full, jnp.where(lane == 0, LANES - 1, C)), pe)
        low, rows = TOP - DEPTH, Y + 2 * DEPTH
        slab = after[HALOED][SWEEPS - 2]
        spot = iota((rows, LANES), 1) % SPAN
        for g in range(groups + 2):
            s = slab[g, low:low + rows, :]
            sc[g] = jnp.where(spot < quarter, s, turn(s, -half))
            sd[g] = jnp.where(spot <= quarter, s, turn(s, quarter + 1 - (3 * quarter - 1)))
        lane = iota((rows, LANES), 1)
        near = (lane < DEPTH - 1) | (lane > LANES - DEPTH)
        end = after[0][SWEEPS - 2]
        for p in range(DEPTH - 1, DEPTH + X + 1):
            g, i = p // PER, p % PER
            f = jnp.where(near, turn(sc[g], -quarter - SPAN * i), end[p, low:low + rows, :])
            z[p, low:low + rows, :] = f * (1.0 / 9.0) + pd[(p - DEPTH + 2) // 2, low:low + rows, :]

    def around(ref, p):
        mid = ref[p, TOP:TOP + Y, :]
        total = ref[p - 1, TOP:TOP + Y, :] + ref[p + 1, TOP:TOP + Y, :]
        return mid, total + ref[p, TOP - 1:TOP - 1 + Y, :] + ref[p, TOP + 1:TOP + 1 + Y, :]

    lane = iota((Y, LANES), 1)
    first, last = lane == 0, lane == LANES - 1

    def operator(z, p):
        mid, total = around(z, p)
        g, i = p // PER, p % PER
        ghost = turn(sd[g, DEPTH:DEPTH + Y, :], LANES - 1 - quarter - SPAN * i) * (1.0 / 9.0)
        ghost = ghost + pe[(p - DEPTH + 2) // 2, TOP:TOP + Y, :]
        total = total + jnp.where(first, ghost, turn(mid, 1))
        total = total + jnp.where(last, ghost, turn(mid, -1))
        return mid, 6.0 * mid - total

    load_x.wait()
    out = jnp.zeros((Y, LANES), jnp.float32)
    for i in range(X):
        out = jnp.where(lane // 2 == i, turn(ux[1 + i, TOP:TOP + Y, :], 2 * i + 1), out)
    ze[...] = out
    pl.semaphore_wait(barrier, n - 1)
    start_all(face_copies())
    load_b.wait()
    for i in range(X):
        mid, total = around(ux, 1 + i)
        total = total + jnp.where(first, 0.0, turn(mid, 1))
        total = total + jnp.where(last, 0.0, turn(mid, -1))
        g0[0, DEPTH + i, TOP:TOP + Y, :] = bb[i] - (6.0 * mid - total)
    all_of(face_entries(), xrecv.at[0], -1)
    for i, side in ((0, 1), (X - 1, 0)):
        here = (0, DEPTH + i, slice(TOP, TOP + Y))
        g0[here] = g0[here] + xg[side]
    ghosts = jnp.where(lane % 2 == 0, turn(zi[1], -1), turn(zi[0], 1))

    def complete(a, b):
        for j, side in ((0, 1), (Y - 1, 0)):
            here = (0, slice(DEPTH + a, DEPTH + b), slice(TOP + j, TOP + j + 1))
            g0[here] = g0[here] + yg[side, a:b]
        for i in range(a, b):
            here = (0, DEPTH + i, slice(TOP, TOP + Y))
            g0[here] = g0[here] + jnp.where(first | last, turn(ghosts, -2 * i - 1), 0.0)

    def start_edges(k):
        start_all([main_copies(k)[i] for i, (dx, _) in enumerate(AROUND) if dx])

    complete(0, DEPTH)
    complete(X - DEPTH, X)
    start_edges(0)
    complete(DEPTH, X - DEPTH)

    def sums_of(a, b, width):
        lane = iota((1, LANES), 1)
        pair = jnp.concatenate([jnp.sum(a, axis=0, keepdims=True), jnp.sum(b, axis=0, keepdims=True)], axis=0)
        size = LANES // 2
        while size >= width:
            pair = pair + turn(pair, size)
            size //= 2
        return jnp.where(lane < LANES - width, pair[0:1], pair[1:2])

    def ratio(rows, width):
        lane = iota((1, LANES), 1)
        row = jnp.sum(rows, axis=0, keepdims=True)
        second = jnp.where(lane >= LANES - width, row, 0.0)
        first = jnp.where((lane >= LANES - 2 * width) & (lane < LANES - width), row, 0.0)
        return jnp.sum(first, axis=1, keepdims=True) / jnp.sum(second, axis=1, keepdims=True)

    nothing = jnp.zeros((Y, LANES), jnp.float32)
    precondition(0, z0, None)
    rz, zw = nothing, nothing
    inner = list(range(DEPTH, X - DEPTH))
    for i in [i for i in range(X) if i not in inner] + inner:
        if i == DEPTH:
            start_edges(1)
        mid, image = operator(z0, DEPTH + i)
        g0[1, DEPTH + i, TOP:TOP + Y, :] = image
        rz = rz + g0[0, DEPTH + i, TOP:TOP + Y, :] * mid
        zw = zw + mid * image
    precondition(1, z1, sums_of(rz, zw, LANES // 4))
    alpha = ratio(cr[1, :, 0, :], LANES // 4)
    rz, zw = nothing, nothing
    for i in range(X):
        mid, image = operator(z1, DEPTH + i)
        here = (DEPTH + i, slice(TOP, TOP + Y))
        before, w = z0[here], g0[(1,) + here]
        r = g0[(0,) + here] - alpha * w
        z = before - alpha * mid
        w = w - alpha * image
        rz = rz + r * z
        zw = zw + z * w
        w_ref[i] = w
    sums = sums_of(rz, zw, LANES // 2)
    ds[...] = sums
    dr[me] = sums
    to_all(ds, dr, dsend.at[0], drecv.at[0])
    for i in range(X):
        here = (DEPTH + i, slice(TOP, TOP + Y))
        before = z0[here]
        sol_ref[i] = ux[1 + i, TOP:TOP + Y, :] + alpha * before
        z_ref[i] = before - alpha * z1[here]
        res_ref[i] = g0[(0,) + here] - alpha * g0[(1,) + here]
    all_of(face_entries(), xsend.at[0], 1)
    all_of([(step, STEPS * c) for step, c in main_entries() + far_entries()], send.at[0], 1)
    part = cr.at[:, pl.ds(0, n - 1)]
    pltpu.make_async_copy(part, part, csend.at[0]).wait()
    all_done(dr, dsend.at[0])
    all_done(dr, drecv.at[0])
    alpha_ref[...] = jnp.broadcast_to(ratio(dr[:, 0, :], LANES // 2), alpha_ref.shape)


def finish(base, z, r, w, alpha, sol, res, sol_out, res_out, sem):
    X = base.shape[0]
    size = X // PARTS
    a = alpha[0:1, 0:1][None]
    copies = []
    for part in range(PARTS):
        here = slice(part * size, (part + 1) * size)
        sol_out[here] = base[here] + a * z[here]
        res_out[here] = r[here] - a * w[here]
        for i, (src, dst) in enumerate(((sol_out, sol), (res_out, res))):
            copies.append(pltpu.make_async_copy(src.at[here], dst.at[here], sem.at[i, part]))
            copies[-1].start()
    for copy in copies:
        copy.wait()


def solution(mesh):
    sizes = tuple(mesh.shape[a] for a in AXES)
    n = sizes[0] * sizes[1] * sizes[2]

    def run(right_side, guess):
        X, Y, Z = block = guess.shape
        assert Z == LANES and PER == DEPTH and X % PER == 0 and X * DEPTH <= LANES
        dims = [tuple(d >> l for d in block) for l in range(LEVELS)]
        f32 = jnp.float32
        vm = lambda *s: pltpu.VMEM(s, f32)
        ext = [(dims[l][0] + 2 * DEPTH, dims[l][1] + 2 * TOP, LANES) for l in range(HALOED)]
        slab = (X // PER + 2, Y + 2 * TOP, LANES)
        tall = [(dims[l][1] + 2 * DEPTH, LANES) for l in range(HALOED)]
        CA, CB, CC = dims[HALOED]
        assert dims[HALOED + 1][:2] == (1, 1) and sizes[1] * CB <= ROWS and CA * CB * CC + CC // 2 <= LANES // 2
        dma = lambda *s: pltpu.SemaphoreType.DMA(s)
        scratch = [
            vm(X + 2, Y + 2 * TOP, LANES), vm(*block),
            *(vm(STEPS, *e) for e in ext), vm(STEPS, *slab),
            *(vm(*e) for e in ext[1:]), vm(*slab),
            *(vm(*e) for e in ext + [slab] for _ in range(SWEEPS - 1)),
            vm(*ext[0]), vm(*ext[0]),
            vm(slab[0], *tall[0]), vm(slab[0], *tall[0]),
            vm(dims[1][0] + 2, 2 * tall[1][0], LANES), vm(dims[1][0] + 2, 2 * tall[1][0], LANES),
            *(vm(*t) for t in tall), vm(*tall[0]),
            vm((CA + 1) * sizes[0] * ROWS, (CA * CB + 1) * n),
            vm(CA * sizes[0] + DEPTH, ROWS, LANES),
            vm(CA + DEPTH, 4 * ROWS, LANES),
            vm(X // 2, Y, LANES), vm(X // 2, 2 * Y, LANES),
            vm(2, Y, LANES), vm(2, X, 1, LANES), vm(Y, LANES), vm(2, Y, LANES),
            vm(STEPS, 2, Y, LANES), vm(STEPS, dims[1][1], LANES), vm(STEPS, dims[2][1], LANES),
            *(vm(STEPS, 2, dims[l][1] + 2 * DEPTH, LANES) for l in range(HALOED - 1)),
            vm(STEPS, 2, Y, LANES), vm(STEPS, 2, 2, Y + 2 * DEPTH, LANES),
            vm(STEPS, 2, DEPTH, dims[1][1], LANES), vm(STEPS, 2, DEPTH, dims[1][1] + 2 * DEPTH, LANES),
            vm(STEPS, 1, LANES), vm(STEPS, n, 1, LANES),
            vm(1, LANES), vm(n, 1, LANES), vm(16 * STEPS * DEPTH * max(X, Y), LANES),
            dma(2), dma(1), dma(1), dma(STEPS), dma(1), dma(STEPS),
            dma(1), dma(STEPS), dma(1), dma(1),
        ]
        whole = pltpu.VMEM(block, f32)
        base, z, r, w, alpha = pl.pallas_call(
            functools.partial(kernel, sizes, block),
            out_shape=(whole, whole, whole, whole, pltpu.VMEM((8, LANES), f32)),
            in_specs=[pl.BlockSpec(memory_space=pl.ANY)] * 2,
            out_specs=[pl.BlockSpec(memory_space=pltpu.VMEM)] * 5,
            scratch_shapes=scratch,
            compiler_params=pltpu.CompilerParams(collective_id=0, has_side_effects=True),
        )(right_side, guess)
        inner = [pltpu.with_memory_space_constraint(v, pltpu.VMEM) for v in (base, z, r, w, alpha)]
        out = jax.ShapeDtypeStruct(block, f32)
        return tuple(pl.pallas_call(
            finish,
            out_shape=(out, out),
            in_specs=[pl.BlockSpec(memory_space=pltpu.VMEM)] * 5,
            out_specs=[pl.BlockSpec(memory_space=pl.ANY)] * 2,
            scratch_shapes=[vm(*block), vm(*block), dma(2, PARTS)],
        )(*inner))

    spec = P(*AXES)
    return jax.shard_map(run, mesh=mesh, in_specs=(spec, spec), out_specs=(spec, spec), check_vma=False)
```
